8 devices in a mesh: tp: 4 (over z, y, x), ep: 2 (over core).
Axes of the slice: x: 2, y: 2, z: 1, core: 2. Of those that a mesh axis runs over, the one named last changes fastest.
Arguments:
- x: bfloat16 [2048, 2048], P(('ep', 'tp'))
- idx: int32 [2048, 2], P(('ep', 'tp'))
- g: float32 [2048, 2], P(('ep', 'tp'))
- cap: int32 [8], replicated
- w1: bfloat16 [8, 2048, 5632], P('ep', None, 'tp')
- w3: bfloat16 [8, 2048, 5632], P('ep', None, 'tp')
- w2: bfloat16 [8, 5632, 2048], P('ep', 'tp')
Outputs:
- output: bfloat16 [2048, 2048], P(('ep', 'tp'))
All inputs are finite; a program needn't handle non-finite values.
Results may differ from the reference program's by a relative error of at most 0.00147.
Values are sent between devices in bfloat16 or wider.
A program may use at most 1 GiB of HBM per device.

```python
import jax
import jax.numpy as jnp
from jax import lax

D = 2048
FF = 5632
EXPERTS = 8
TOP = 2
TOKENS_DEV = 256
DEVICES = 8
CAP = 160


def setup_inputs(seed: int = 0) -> dict:
    key = jax.random.key(seed)
    kx, kp, ki, kg, kc, k1, k3, k2 = jax.random.split(key, 8)
    t = TOKENS_DEV * DEVICES
    x = jax.random.normal(kx, (t, D), jnp.float32).astype(jnp.bfloat16)
    rank = jax.random.permutation(kp, EXPERTS)
    logw = jnp.where(rank < EXPERTS // 4, jnp.log(4.0), 0.0).astype(jnp.float32)
    noise = jax.random.gumbel(ki, (t, EXPERTS), jnp.float32)
    idx = lax.top_k(logw[None, :] + noise, TOP)[1].astype(jnp.int32)
    g = jax.nn.softmax(jax.random.normal(kg, (t, TOP), jnp.float32), axis=-1)
    cap = jax.random.randint(kc, (EXPERTS,), (3 * CAP) // 4, CAP + 1, jnp.int32)
    w1 = (jax.random.normal(k1, (EXPERTS, D, FF), jnp.float32) * D ** -0.5).astype(jnp.bfloat16)
    w3 = (jax.random.normal(k3, (EXPERTS, D, FF), jnp.float32) * D ** -0.5).astype(jnp.bfloat16)
    w2 = (jax.random.normal(k2, (EXPERTS, FF, D), jnp.float32) * FF ** -0.5).astype(jnp.bfloat16)
    return {"x": x, "idx": idx, "g": g, "cap": cap, "w1": w1, "w3": w3, "w2": w2}


def reference(x, idx, g, cap, w1, w3, w2):
    xs = x.reshape(DEVICES, TOKENS_DEV, D)
    ids = idx.reshape(DEVICES, TOKENS_DEV * TOP)
    gs = g.reshape(DEVICES, TOKENS_DEV * TOP)
    tok = jnp.arange(TOKENS_DEV * TOP) // TOP

    def slot_ids(ids_d):
        oh = (ids_d[:, None] == jnp.arange(EXPERTS, dtype=jnp.int32)[None, :]).astype(jnp.int32)
        pos = jnp.sum(jnp.cumsum(oh, axis=0) * oh, axis=1) - 1
        return jnp.where(pos < cap[ids_d], ids_d * CAP + pos, EXPERTS * CAP)

    sid = lax.map(slot_ids, ids)

    def place(a):
        xd, sd = a
        buf = jnp.zeros((EXPERTS * CAP + 1, D), jnp.bfloat16).at[sd].set(xd[tok])
        return buf[: EXPERTS * CAP]

    slots = lax.map(place, (xs, sid))
    slots = slots.reshape(DEVICES, EXPERTS, CAP, D).transpose(1, 0, 2, 3).reshape(EXPERTS, DEVICES * CAP, D)

    def expert(a):
        xe, a1, a3, a2 = a
        h1 = jnp.dot(xe, a1, preferred_element_type=jnp.float32)
        h3 = jnp.dot(xe, a3, preferred_element_type=jnp.float32)
        h = (jax.nn.silu(h1) * h3).astype(jnp.bfloat16)
        return jnp.dot(h, a2, preferred_element_type=jnp.float32).astype(jnp.bfloat16)

    ys = lax.map(expert, (slots, w1, w3, w2))
    ys = ys.reshape(EXPERTS, DEVICES, CAP, D).transpose(1, 0, 2, 3).reshape(DEVICES, EXPERTS * CAP, D)
    ys = jnp.pad(ys, ((0, 0), (0, 1), (0, 0)))

    def combine(a):
        yd, sd, gd = a
        yc = yd[sd].astype(jnp.float32) * gd[:, None]
        return jnp.sum(yc.reshape(TOKENS_DEV, TOP, D), axis=1).astype(jnp.bfloat16)

    out = lax.map(combine, (ys, sid, gs))
    return out.reshape(DEVICES * TOKENS_DEV, D)
```

```python
import functools

import jax
import jax.numpy as jnp
from jax import lax
from jax.experimental import pallas as pl
from jax.experimental.pallas import tpu as pltpu
from jax.sharding import PartitionSpec as P


F32 = jnp.float32
BF16 = jnp.bfloat16


def _meta_kernel(chips, idx_ref, cap_ref, pos_ref, off_ref, cnt_ref):
    blocks, _, t = idx_ref.shape
    e_all = cap_ref.shape[0]
    ids = lax.broadcasted_iota(jnp.int32, (e_all, t), 0)
    cap = jnp.broadcast_to(cap_ref[...], (e_all, t))
    before = (
        lax.broadcasted_iota(jnp.int32, (t, t), 0) < lax.broadcasted_iota(jnp.int32, (t, t), 1)
    ).astype(F32).astype(BF16)
    hits, earlier, counts = [], [], []
    for b in range(blocks):
        hit = (idx_ref[b, 0:1, :] == ids) | (idx_ref[b, 1:2, :] == ids)
        one = hit.astype(F32)
        rank = jnp.dot(one.astype(BF16), before, preferred_element_type=F32).astype(jnp.int32)
        total = jnp.sum(one, axis=1, keepdims=True).astype(jnp.int32)
        hits.append(hit)
        earlier.append(rank)
        counts.append(jnp.minimum(jnp.broadcast_to(total, (e_all, t)), cap))
    for c in range(chips):
        both = counts[c] + counts[c + chips]
        first = jnp.zeros_like(both)
        for e in range(e_all - 1):
            first = first + jnp.where(ids > e, jnp.broadcast_to(both[e : e + 1, :], both.shape), 0)
        off_ref[c] = first[:, :128]
        cnt_ref[c] = both[:, :128]
        for b, start in ((c, first), (c + chips, first + counts[c])):
            kept = hits[b] & (earlier[b] < cap)
            pos_ref[b] = jnp.where(kept, start + earlier[b], -1)


def _expert_kernel(sizes, s_ref, pos_ref, xa_ref, xb_ref, w1_ref, w3_ref, w2_ref, keep_ref, send_ref, acc, sem):
    e = pl.program_id(0)
    e_loc = pl.num_programs(0)
    rows = acc.shape[0]
    core, chip = s_ref[0], s_ref[1]
    chips = pos_ref.shape[0] // 2
    expert = core * e_loc + e
    off = s_ref[2 + chip * 8 + expert]
    cnt = s_ref[2 + 32 + chip * 8 + expert]
    base16 = off // 16 * 16

    @pl.when(e == 0)
    def _():
        acc[...] = jnp.zeros_like(acc)

    def run(m):
        base = pl.multiple_of(jnp.minimum(base16, rows - m), 16)
        t = xa_ref.shape[0]
        row = lax.broadcasted_iota(jnp.int32, (m, t), 0) + base
        pa = pos_ref[chip + core * chips, pl.ds(expert, 1), :]
        pb = pos_ref[chip + (1 - core) * chips, pl.ds(expert, 1), :]
        ha = (row == pa).astype(F32).astype(BF16)
        hb = (row == pb).astype(F32).astype(BF16)
        xs = jnp.dot(ha, xa_ref[...], preferred_element_type=F32) + jnp.dot(hb, xb_ref[...], preferred_element_type=F32)
        xs = xs.astype(BF16)
        h1 = jnp.dot(xs, w1_ref[...], preferred_element_type=F32)
        h3 = jnp.dot(xs, w3_ref[...], preferred_element_type=F32)
        h = (jax.nn.silu(h1) * h3).astype(BF16)
        acc[pl.ds(base, m), :] += jnp.dot(h, w2_ref[...], preferred_element_type=F32)

    need = off - base16 + cnt
    lo = 0
    for m in sizes:
        pl.when((need > lo) & (need <= m) & (cnt > 0))(functools.partial(run, m))
        lo = m

    @pl.when(e == e_loc - 1)
    def _():
        half = rows // 2
        mine = pl.multiple_of(core * half, half)
        other = pl.multiple_of((1 - core) * half, half)
        a = pltpu.make_async_copy(acc.at[pl.ds(other, half), :], send_ref, sem.at[0])
        b = pltpu.make_async_copy(acc.at[pl.ds(mine, half), :], keep_ref, sem.at[1])
        a.start()
        b.start()
        a.wait()
        b.wait()


def _combine_kernel(chips, s_ref, pos_ref, idx_ref, g_ref, ym_ref, yo_ref, out_ref):
    core, chip = s_ref[0], s_ref[1]
    half, _ = ym_ref.shape
    t = idx_ref.shape[1]
    pos = pos_ref[chip + core * chips]
    ids = lax.broadcasted_iota(jnp.int32, pos.shape, 0)
    row = lax.broadcasted_iota(jnp.int32, (half, t), 0)
    total = None
    for j in range(2):
        pj = jnp.max(jnp.where(idx_ref[j : j + 1, :] == ids, pos, -1), axis=0, keepdims=True)
        hm = (row + core * half == pj).astype(F32).astype(BF16)
        ho = (row + (1 - core) * half == pj).astype(F32).astype(BF16)
        dims = (((0,), (0,)), ((), ()))
        y = lax.dot_general(hm, ym_ref[...], dims, preferred_element_type=F32)
        y = y + lax.dot_general(ho, yo_ref[...], dims, preferred_element_type=F32)
        y = y * g_ref[:, j : j + 1]
        total = y if total is None else total + y
    out_ref[...] = total.astype(out_ref.dtype)


def solution(mesh):
    chips = mesh.shape["tp"]
    vmem = pl.BlockSpec(memory_space=pltpu.VMEM)
    anym = pl.BlockSpec(memory_space=pl.ANY)
    smem = pl.BlockSpec(memory_space=pltpu.SMEM)

    def local(x, idx, g, cap, w1, w3, w2):
        t_loc, d = x.shape
        top = idx.shape[1]
        e_all = cap.shape[0]
        e_loc, _, ff = w1.shape
        c = (5 * top * t_loc // (2 * e_all) + 7) // 8 * 8
        rows = 2 * top * t_loc
        core, me = lax.axis_index("ep"), lax.axis_index("tp")

        def swap(a):
            return lax.ppermute(a, "ep", [(0, 1), (1, 0)])

        def shift(a, r):
            return lax.ppermute(a, "tp", [(i, i ^ r) for i in range(chips)])

        idx_all = lax.all_gather(idx.T, ("ep", "tp"), axis=0)
        pos, off, cnt = pl.pallas_call(
            functools.partial(_meta_kernel, chips),
            out_shape=[
                jax.ShapeDtypeStruct((2 * chips, e_all, t_loc), jnp.int32),
                jax.ShapeDtypeStruct((chips, e_all, 128), jnp.int32),
                jax.ShapeDtypeStruct((chips, e_all, 128), jnp.int32),
            ],
            in_specs=[vmem] * 2,
            out_specs=[vmem] * 3,
            name="meta",
        )(idx_all, cap[:, None])
        tables = jnp.concatenate([off[:, :, 0].reshape(-1), cnt[:, :, 0].reshape(-1)])

        sizes = (144, (2 * c + 15 + 15) // 16 * 16)

        def stage(r, xa, xb):
            chip = me ^ r
            s = jnp.concatenate([jnp.stack([core, chip]).astype(jnp.int32), tables])
            flops = 2 * 3 * rows // 2 * d * ff
            return pl.pallas_call(
                functools.partial(_expert_kernel, sizes),
                out_shape=[jax.ShapeDtypeStruct((rows // 2, d), F32)] * 2,
                grid_spec=pltpu.PrefetchScalarGridSpec(
                    num_scalar_prefetch=1,
                    grid=(e_loc,),
                    in_specs=[
                        vmem,
                        vmem,
                        vmem,
                        pl.BlockSpec((None, d, ff), lambda e, s: (e, 0, 0)),
                        pl.BlockSpec((None, d, ff), lambda e, s: (e, 0, 0)),
                        pl.BlockSpec((None, ff, d), lambda e, s: (e, 0, 0)),
                    ],
                    out_specs=[anym, anym],
                    scratch_shapes=[pltpu.VMEM((rows, d), F32), pltpu.SemaphoreType.DMA((2,))],
                ),
                compiler_params=pltpu.CompilerParams(vmem_limit_bytes=67_043_328, dimension_semantics=("arbitrary",)),
                cost_estimate=pl.CostEstimate(flops=flops, bytes_accessed=6 * e_loc * d * ff + 4 * rows * d, transcendentals=0),
                name=f"experts{r}",
            )(s, pos, xa, xb, w1, w3, w2)

        xs = {3: shift(x, 3), 1: shift(x, 1), 2: shift(x, 2), 0: x}
        total = None
        order = (0, 3, 1, 2)
        got = []
        for r in order:
            keep, send = stage(r, xs[r], swap(xs[r]))
            merged = keep + swap(send)
            got.append(merged if r == 0 else shift(merged, r))
        total = got[0]
        for a in got[1:]:
            total = total + a
        y = total.astype(BF16)
        return pl.pallas_call(
            functools.partial(_combine_kernel, chips),
            out_shape=jax.ShapeDtypeStruct((t_loc, d), BF16),
            in_specs=[smem] + [vmem] * 5,
            out_specs=vmem,
            compiler_params=pltpu.CompilerParams(vmem_limit_bytes=60_000_000),
            name="combine",
        )(jnp.stack([core, me]).astype(jnp.int32), pos, idx.T, g, y, swap(y))

    rows = P(("ep", "tp"), None)
    return jax.shard_map(
        local,
        mesh=mesh,
        in_specs=(rows, rows, rows, P(None), P("ep", None, "tp"), P("ep", None, "tp"), P("ep", "tp", None)),
        out_specs=rows,
        check_vma=False,
    )
```

```python
import functools

import jax
import jax.numpy as jnp
from jax import lax
from jax.experimental import pallas as pl
from jax.experimental.pallas import tpu as pltpu
from jax.sharding import PartitionSpec as P


F32 = jnp.float32
BF16 = jnp.bfloat16


def _meta_kernel(chips, idx_ref, cap_ref, pos_ref, off_ref, cnt_ref):
    blocks, _, t = idx_ref.shape
    e_all = cap_ref.shape[0]
    ids = lax.broadcasted_iota(jnp.int32, (e_all, t), 0)
    cap = jnp.broadcast_to(cap_ref[...], (e_all, t))
    before = (
        lax.broadcasted_iota(jnp.int32, (t, t), 0) < lax.broadcasted_iota(jnp.int32, (t, t), 1)
    ).astype(F32).astype(BF16)
    hits, earlier, counts = [], [], []
    for b in range(blocks):
        hit = (idx_ref[b, 0:1, :] == ids) | (idx_ref[b, 1:2, :] == ids)
        one = hit.astype(F32)
        rank = jnp.dot(one.astype(BF16), before, preferred_element_type=F32).astype(jnp.int32)
        total = jnp.sum(one, axis=1, keepdims=True).astype(jnp.int32)
        hits.append(hit)
        earlier.append(rank)
        counts.append(jnp.minimum(jnp.broadcast_to(total, (e_all, t)), cap))
    for c in range(chips):
        both = counts[c] + counts[c + chips]
        first = jnp.zeros_like(both)
        for e in range(e_all - 1):
            first = first + jnp.where(ids > e, jnp.broadcast_to(both[e : e + 1, :], both.shape), 0)
        off_ref[c] = first[:, :128]
        cnt_ref[c] = both[:, :128]
        for b, start in ((c, first), (c + chips, first + counts[c])):
            kept = hits[b] & (earlier[b] < cap)
            pos_ref[b] = jnp.where(kept, start + earlier[b], -1)


def _expert_kernel(turns, small, tile, cut, *refs):
    n = len(turns)
    off_ref, cnt_ref, pos_ref = refs[:3]
    x_hbm = refs[3 : 3 + 2 * n]
    w1_hbm, w3_hbm, w2_hbm = refs[3 + 2 * n : 6 + 2 * n]
    outs = refs[6 + 2 * n : 6 + 6 * n]
    acc, xbuf, xs, hs, w1a, w3a, w1b, w3b, w2s, wsem, osem, xsem = refs[6 + 6 * n :]
    e_loc, d, ff = w1_hbm.shape
    t = xbuf.shape[2]
    quarter, half_d = t, d // 2
    span = xs.shape[0] // n
    core, me = lax.axis_index("ep"), lax.axis_index("tp")
    chips = pos_ref.shape[0] // 2

    def chunk(k, e):
        if k == 0:
            return [
                pltpu.make_async_copy(w1_hbm.at[e, :, pl.ds(0, cut)], w1a, wsem.at[0]),
                pltpu.make_async_copy(w3_hbm.at[e, :, pl.ds(0, cut)], w3a, wsem.at[1]),
            ]
        if k == 1:
            return [
                pltpu.make_async_copy(w1_hbm.at[e, :, pl.ds(cut, ff - cut)], w1b, wsem.at[2]),
                pltpu.make_async_copy(w3_hbm.at[e, :, pl.ds(cut, ff - cut)], w3b, wsem.at[3]),
            ]
        h = k - 2
        return [pltpu.make_async_copy(w2_hbm.at[e, :, pl.ds(h * half_d, half_d)], w2s.at[h], wsem.at[2 + k])]

    def start(k, e):
        for c in chunk(k, e):
            c.start()

    def finish(k, e):
        for c in chunk(k, e):
            c.wait()

    def following(k, e):
        @pl.when(e + 1 < e_loc)
        def _():
            start(k, e + 1)

    def out_copies(h):
        copies = []
        for s in range(n):
            for q in range(4):
                side = core if q < 2 else 1 - core
                first = pl.multiple_of(side * (2 * quarter) + (q % 2) * quarter, quarter)
                copies.append(
                    pltpu.make_async_copy(
                        acc.at[s, pl.ds(first, quarter), pl.ds(h * half_d, half_d)],
                        outs[4 * s + q].at[:, pl.ds(h * half_d, half_d)],
                        osem.at[h, 4 * s + q],
                    )
                )
        return copies

    tokens = [pltpu.make_async_copy(x_hbm[i], xbuf.at[i // 2, i % 2], xsem.at[i]) for i in range(2 * n)]
    for c in tokens:
        c.start()
    for k in range(4):
        start(k, 0)
    acc[...] = jnp.zeros_like(acc)
    for c in tokens:
        c.wait()

    def step(e, carry):
        expert = core * e_loc + e

        def each(body):
            def source(s, carry):
                turn = turns[0] if n == 1 else jnp.where(s == 0, turns[0], turns[1])
                chip = jnp.bitwise_xor(me, turn)
                off, cnt = off_ref[chip, expert, 0], cnt_ref[chip, expert, 0]
                base = off // 8 * 8
                need = jnp.where(cnt > 0, off - base + cnt, 0)

                @pl.when((need > 0) & (need <= small))
                def _():
                    body(s, chip, small, base, 0)

                @pl.when(need > small)
                def _():
                    def one(i, carry):
                        body(s, chip, tile, base, pl.multiple_of(i * tile, 16))
                        return carry

                    lax.fori_loop(0, (need + tile - 1) // tile, one, 0)

                return carry

            if n == 1:
                source(0, 0)
            else:
                lax.fori_loop(0, n, source, 0)

        def dispatch(s, chip, m, base, first):
            row = lax.broadcasted_iota(jnp.int32, (m, t), 0) + (base + first)
            pa = pos_ref[chip + core * chips, pl.ds(expert, 1), :]
            pb = pos_ref[chip + (1 - core) * chips, pl.ds(expert, 1), :]
            ha = (row == pa).astype(F32).astype(BF16)
            hb = (row == pb).astype(F32).astype(BF16)
            part = jnp.dot(ha, xbuf[s, 0], preferred_element_type=F32)
            part = part + jnp.dot(hb, xbuf[s, 1], preferred_element_type=F32)
            xs[pl.ds(pl.multiple_of(s * span + first, 16), m), :] = part.astype(BF16)

        def hidden(wa, wb, lo, width):
            def body(s, chip, m, base, first):
                at = pl.ds(pl.multiple_of(s * span + first, 16), m)
                h1 = jnp.dot(xs[at, :], wa[...], preferred_element_type=F32)
                h3 = jnp.dot(xs[at, :], wb[...], preferred_element_type=F32)
                hs[at, lo : lo + width] = (jax.nn.silu(h1) * h3).astype(BF16)

            return body

        def project(k):
            def body(s, chip, m, base, first):
                at = pl.ds(pl.multiple_of(s * span + first, 16), m)
                p = jnp.dot(hs[at, :], w2s[k], preferred_element_type=F32)
                acc[s, pl.ds(pl.multiple_of(base + first, 8), m), k * half_d : (k + 1) * half_d] += p

            return body

        each(dispatch)
        finish(0, e)
        each(hidden(w1a, w3a, 0, cut))
        following(0, e)
        finish(1, e)
        each(hidden(w1b, w3b, cut, ff - cut))
        following(1, e)
        for k in range(2):
            finish(2 + k, e)
            each(project(k))
            following(2 + k, e)
            if k == 0:

                @pl.when(e == e_loc - 1)
                def _():
                    for c in out_copies(0):
                        c.start()

        return carry

    lax.fori_loop(0, e_loc, step, 0)
    for c in out_copies(1):
        c.start()
    for c in out_copies(0) + out_copies(1):
        c.wait()


def _combine_kernel(chips, pos_ref, idx_ref, g_ref, ma_ref, mb_ref, oa_ref, ob_ref, out_ref):
    core, me = lax.axis_index("ep"), lax.axis_index("tp")
    quarter, _ = ma_ref.shape
    t = idx_ref.shape[1]
    pos = pos_ref[me + core * chips]
    ids = lax.broadcasted_iota(jnp.int32, pos.shape, 0)
    row = lax.broadcasted_iota(jnp.int32, (quarter, t), 0)
    dims = (((0,), (0,)), ((), ()))
    total = None
    for j in range(2):
        pj = jnp.max(jnp.where(idx_ref[j : j + 1, :] == ids, pos, -1), axis=0, keepdims=True)
        y = None
        for ref, first in (
            (ma_ref, core * 2 * quarter),
            (mb_ref, core * 2 * quarter + quarter),
            (oa_ref, (1 - core) * 2 * quarter),
            (ob_ref, (1 - core) * 2 * quarter + quarter),
        ):
            hit = (row + first == pj).astype(F32).astype(BF16)
            part = lax.dot_general(hit, ref[...], dims, preferred_element_type=F32)
            y = part if y is None else y + part
        y = y * g_ref[:, j : j + 1]
        total = y if total is None else total + y
    out_ref[...] = total.astype(out_ref.dtype)


def solution(mesh):
    chips = mesh.shape["tp"]
    vmem = pl.BlockSpec(memory_space=pltpu.VMEM)
    anym = pl.BlockSpec(memory_space=pl.ANY)
    smem = pl.BlockSpec(memory_space=pltpu.SMEM)

    def layer(x, idx, g, cap, w1, w3, w2):
        t_loc, d = x.shape
        top = idx.shape[1]
        e_all = cap.shape[0]
        e_loc, _, ff = w1.shape
        c = (5 * top * t_loc // (2 * e_all) + 7) // 8 * 8
        rows = 2 * top * t_loc
        quarter = rows // 4
        cut = 512

        def swap(a):
            return lax.ppermute(a, "ep", [(0, 1), (1, 0)])

        def shift(a, r):
            return lax.ppermute(a, "tp", [(i, i ^ r) for i in range(chips)])

        def after(a, *first):
            return lax.optimization_barrier((a, *first))[0]

        idx_all = lax.all_gather(idx.T, ("ep", "tp"), axis=0)
        pos, off, cnt = pl.pallas_call(
            functools.partial(_meta_kernel, chips),
            out_shape=[
                jax.ShapeDtypeStruct((2 * chips, e_all, t_loc), jnp.int32),
                jax.ShapeDtypeStruct((chips, e_all, 128), jnp.int32),
                jax.ShapeDtypeStruct((chips, e_all, 128), jnp.int32),
            ],
            in_specs=[vmem] * 2,
            out_specs=[vmem] * 3,
            name="meta",
        )(idx_all, cap[:, None])

        small, tile = 96, 144
        span = (2 * c + 7 + tile - 1) // tile * tile

        def stage_call(turns, xs):
            n = len(turns)
            return pl.pallas_call(
                functools.partial(_expert_kernel, turns, small, tile, cut),
                out_shape=[jax.ShapeDtypeStruct((quarter, d), F32)] * (4 * n),
                in_specs=[smem, smem, vmem] + [anym] * (2 * n + 3),
                out_specs=[anym] * (4 * n),
                scratch_shapes=[
                    pltpu.VMEM((n, rows + tile, d), F32),
                    pltpu.VMEM((n, 2, t_loc, d), BF16),
                    pltpu.VMEM((n * span, d), BF16),
                    pltpu.VMEM((n * span, ff), BF16),
                    pltpu.VMEM((d, cut), BF16),
                    pltpu.VMEM((d, cut), BF16),
                    pltpu.VMEM((d, ff - cut), BF16),
                    pltpu.VMEM((d, ff - cut), BF16),
                    pltpu.VMEM((2, ff, d // 2), BF16),
                    pltpu.SemaphoreType.DMA((6,)),
                    pltpu.SemaphoreType.DMA((2, 4 * n)),
                    pltpu.SemaphoreType.DMA((2 * n,)),
                ],
                compiler_params=pltpu.CompilerParams(vmem_limit_bytes=67_043_328),
                cost_estimate=pl.CostEstimate(
                    flops=n * 3 * rows * d * ff, bytes_accessed=6 * e_loc * d * ff + 4 * n * rows * d, transcendentals=0
                ),
            )(off, cnt, pos, *xs, w1, w3, w2)

        def merge(parts):
            return [parts[q] + swap(parts[2 + q]) for q in range(2)]

        x_first = after(x, idx_all)
        x_d, x_x, x_y = shift(x_first, 3), shift(x_first, 1), shift(x_first, 2)

        diag = merge(stage_call((3,), (x_d, swap(x_d))))
        via_x, via_y = shift(diag[0], 1), shift(diag[1], 2)
        x_x, x_y = after(x_x, *diag), after(x_y, *diag)
        both = stage_call((1, 2), (x_x, swap(x_x), x_y, swap(x_y)))
        for_x, for_y = merge(both[:4]), merge(both[4:])
        near_a, near_b = shift(for_x[0], 1), shift(for_y[1], 2)
        far_a, far_b = for_y[0] + via_x, for_x[1] + via_y
        got_a, got_b = shift(far_a, 2), shift(far_b, 1)
        x_o = after(x, *for_x, *for_y)
        own = merge(stage_call((0,), (x_o, swap(x_o))))
        y_a = (own[0] + near_a + got_a).astype(BF16)
        y_b = (own[1] + near_b + got_b).astype(BF16)
        return pl.pallas_call(
            functools.partial(_combine_kernel, chips),
            out_shape=jax.ShapeDtypeStruct((t_loc, d), BF16),
            in_specs=[vmem] * 7,
            out_specs=vmem,
            compiler_params=pltpu.CompilerParams(vmem_limit_bytes=60_000_000),
            name="combine",
        )(pos, idx.T, g, y_a, y_b, swap(y_a), swap(y_b))

    rows = P(("ep", "tp"), None)
    return jax.shard_map(
        layer,
        mesh=mesh,
        in_specs=(rows, rows, rows, P(None), P("ep", None, "tp"), P("ep", None, "tp"), P("ep", "tp", None)),
        out_specs=rows,
        check_vma=False,
    )
```

```python
import functools

import jax
import jax.numpy as jnp
from jax import lax
from jax.experimental import pallas as pl
from jax.experimental.pallas import tpu as pltpu
from jax.sharding import PartitionSpec as P


F32 = jnp.float32
BF16 = jnp.bfloat16
VMEM_BYTES = 67_043_328


def _route_kernel(chips, idx_ref, g_ref, cap_ref, pos_ref, off_ref, cnt_ref, mine_ref, ids_all, send_sem, recv_sem):
    core, me = lax.axis_index("ep"), lax.axis_index("tp")
    blocks, top, t = ids_all.shape
    e_all = cap_ref.shape[0]
    here = core * chips + me
    peers = [
        (k, {"ep": jnp.bitwise_xor(core, k // chips), "tp": jnp.bitwise_xor(me, k % chips)}) for k in range(1, blocks)
    ]
    barrier = pltpu.get_barrier_semaphore()
    for _, peer in peers:
        pl.semaphore_signal(barrier, inc=1, device_id=peer, device_id_type=pl.DeviceIdType.MESH)
    pl.semaphore_wait(barrier, blocks - 1)
    copies = [
        pltpu.make_async_remote_copy(
            src_ref=idx_ref,
            dst_ref=ids_all.at[here],
            send_sem=send_sem.at[k],
            recv_sem=recv_sem.at[k],
            device_id=peer,
            device_id_type=pl.DeviceIdType.MESH,
        )
        for k, peer in peers
    ]
    for c in copies:
        c.start()
    ids_all[pl.ds(here, 1)] = idx_ref[...][None]
    before = (
        lax.broadcasted_iota(jnp.int32, (t, t), 0) < lax.broadcasted_iota(jnp.int32, (t, t), 1)
    ).astype(F32).astype(BF16)
    ids = lax.broadcasted_iota(jnp.int32, (e_all, t), 0)
    cap = jnp.broadcast_to(cap_ref[...], (e_all, t))
    for c in copies:
        c.wait()

    for b in range(blocks):
        hit = (ids_all[b, 0:1, :] == ids) | (ids_all[b, 1:2, :] == ids)
        one = hit.astype(F32)
        rank = jnp.dot(one.astype(BF16), before, preferred_element_type=F32).astype(jnp.int32)
        total = jnp.sum(one, axis=1, keepdims=True).astype(jnp.int32)
        count = jnp.minimum(jnp.broadcast_to(total, (e_all, t)), cap)
        first = jnp.zeros_like(count)
        for e in range(e_all - 1):
            first = first + jnp.where(ids > e, jnp.broadcast_to(count[e : e + 1, :], count.shape), 0)
        off_ref[b] = first[:, :128]
        cnt_ref[b] = count[:, :128]
        pos_ref[b] = jnp.where(hit & (rank < cap), first + rank, -1)
    pos = pos_ref[here]
    lines = [
        jnp.max(jnp.where(idx_ref[j : j + 1, :] == ids, pos, -1), axis=0, keepdims=True).astype(F32) for j in range(top)
    ]
    lines += [g_ref[j : j + 1, :] for j in range(top)]
    table = jnp.concatenate(lines + [jnp.zeros((8 - 2 * top, t), F32)], axis=0)
    mine_ref[...] = jnp.transpose(table)


def _expert_kernel(
    turns, sizes, cut, off_ref, cnt_ref, pos_ref, xm_hbm, xo_hbm, w1_hbm, w3_hbm, w2_hbm, *refs
):
    outs = refs[:4]
    acc, xbuf, w1a, w3a, w1b, w3b, w2s, wsem, osem, xsem = refs[4:]
    e_loc, d, ff = w1_hbm.shape
    _, rows, _ = acc.shape
    t = xbuf.shape[1]
    half_d, half = d // 2, rows // 2
    core, me = lax.axis_index("ep"), lax.axis_index("tp")
    chips = pos_ref.shape[0] // 2
    blocks = []
    for c in (core, 1 - core):
        turn = jnp.where(c == 0, turns[0], turns[1])
        blocks.append(c * chips + jnp.bitwise_xor(me, turn))

    def chunk(k, e):
        if k == 0:
            return [
                pltpu.make_async_copy(w1_hbm.at[e, :, pl.ds(0, cut)], w1a, wsem.at[0]),
                pltpu.make_async_copy(w3_hbm.at[e, :, pl.ds(0, cut)], w3a, wsem.at[1]),
            ]
        if k == 1:
            return [
                pltpu.make_async_copy(w1_hbm.at[e, :, pl.ds(cut, ff - cut)], w1b, wsem.at[2]),
                pltpu.make_async_copy(w3_hbm.at[e, :, pl.ds(cut, ff - cut)], w3b, wsem.at[3]),
            ]
        h = k - 2
        return [pltpu.make_async_copy(w2_hbm.at[e, :, pl.ds(h * half_d, half_d)], w2s.at[h], wsem.at[2 + k])]

    def start(k, e):
        for c in chunk(k, e):
            c.start()

    def finish(k, e):
        for c in chunk(k, e):
            c.wait()

    def following(k, e):
        @pl.when(e + 1 < e_loc)
        def _():
            start(k, e + 1)

    def out_copies(h):
        cols = pl.ds(h * half_d, half_d)
        return [
            pltpu.make_async_copy(
                acc.at[1 - i // 2, pl.ds((i % 2) * half, half), cols], outs[i].at[:, cols], osem.at[h, i]
            )
            for i in range(4)
        ]

    tokens = [
        pltpu.make_async_copy(xm_hbm, xbuf.at[0], xsem.at[0]),
        pltpu.make_async_copy(xo_hbm, xbuf.at[1], xsem.at[1]),
    ]
    for c in tokens:
        c.start()
    for k in range(4):
        start(k, 0)
    acc[...] = jnp.zeros_like(acc)
    for c in tokens:
        c.wait()

    def step(e, carry):
        expert = core * e_loc + e
        offs = [off_ref[b, expert, 0] for b in blocks]
        cnts = [cnt_ref[b, expert, 0] for b in blocks]
        need = functools.reduce(jnp.maximum, [jnp.where(k > 0, o - o // 8 * 8 + k, 0) for o, k in zip(offs, cnts)])

        def last(k):
            if k == 0:

                @pl.when(e == e_loc - 1)
                def _():
                    for c in out_copies(0):
                        c.start()

        def run(m):
            bases = [pl.multiple_of(jnp.minimum(o // 8 * 8, rows - m), 8) for o in offs]
            parts = []
            for s in range(2):
                row = lax.broadcasted_iota(jnp.int32, (m, t), 0) + bases[s]
                hit = (row == pos_ref[blocks[s], pl.ds(expert, 1), :]).astype(F32).astype(BF16)
                parts.append(jnp.dot(hit, xbuf[s], preferred_element_type=F32))
            xs = jnp.concatenate(parts, axis=0).astype(BF16)
            hs = []
            for k, (wa, wb) in enumerate(((w1a, w3a), (w1b, w3b))):
                finish(k, e)
                h1 = jnp.dot(xs, wa[...], preferred_element_type=F32)
                h3 = jnp.dot(xs, wb[...], preferred_element_type=F32)
                hs.append((jax.nn.silu(h1) * h3).astype(BF16))
                following(k, e)
            h = jnp.concatenate(hs, axis=1)
            for k in range(2):
                finish(2 + k, e)
                p = jnp.dot(h, w2s[k], preferred_element_type=F32)
                for s in range(2):
                    acc[s, pl.ds(bases[s], m), k * half_d : (k + 1) * half_d] += p[s * m : (s + 1) * m]
                following(2 + k, e)
                last(k)

        @pl.when(need == 0)
        def _():
            for k in range(4):
                finish(k, e)
                following(k, e)
                last(k - 2)

        lo = 0
        for m in sizes:
            pl.when((need > lo) & (need <= m))(functools.partial(run, m))
            lo = m
        return carry

    lax.fori_loop(0, e_loc, step, 0)
    for c in out_copies(1):
        c.start()
    for c in out_copies(0) + out_copies(1):
        c.wait()


def _combine_kernel(mine_ref, s0_ref, s1_ref, f0_ref, f1_ref, out_ref, hit):
    top, t, rows = hit.shape

    @pl.when(pl.program_id(0) == 0)
    def _():
        row = lax.broadcasted_iota(jnp.int32, (t, rows), 1)
        for j in range(top):
            hit[j] = (row == mine_ref[:, j : j + 1].astype(jnp.int32)).astype(F32).astype(BF16)

    y = jnp.concatenate([s0_ref[...] + f0_ref[...], s1_ref[...] + f1_ref[...]], axis=0).astype(BF16)
    total = None
    for j in range(top):
        part = jnp.dot(hit[j], y, preferred_element_type=F32) * mine_ref[:, top + j : top + j + 1]
        total = part if total is None else total + part
    out_ref[...] = total.astype(out_ref.dtype)


def solution(mesh):
    chips = mesh.shape["tp"]
    vmem = pl.BlockSpec(memory_space=pltpu.VMEM)
    anym = pl.BlockSpec(memory_space=pl.ANY)
    smem = pl.BlockSpec(memory_space=pltpu.SMEM)

    def layer(x, idx, g, cap, w1, w3, w2):
        t_loc, d = x.shape
        top = idx.shape[1]
        e_all = cap.shape[0]
        e_loc, _, ff = w1.shape
        c = (5 * top * t_loc // (2 * e_all) + 7) // 8 * 8
        rows = top * t_loc
        half = rows // 2
        cut = 512
        blocks = 2 * chips

        def swap(a):
            return lax.ppermute(a, "ep", [(0, 1), (1, 0)])

        def shift(a, turns):
            pairs = [(2 * k + i, 2 * (k ^ turns[i]) + i) for k in range(chips) for i in range(2)]
            return lax.ppermute(a, ("tp", "ep"), pairs)

        def after(a, *first):
            return lax.optimization_barrier((a, *first))[0]

        x_d = shift(x, (3, 3))
        pos, off, cnt, mine = pl.pallas_call(
            functools.partial(_route_kernel, chips),
            out_shape=[
                jax.ShapeDtypeStruct((blocks, e_all, t_loc), jnp.int32),
                jax.ShapeDtypeStruct((blocks, e_all, 128), jnp.int32),
                jax.ShapeDtypeStruct((blocks, e_all, 128), jnp.int32),
                jax.ShapeDtypeStruct((t_loc, 8), F32),
            ],
            in_specs=[vmem] * 3,
            out_specs=[vmem] * 4,
            scratch_shapes=[
                pltpu.VMEM((blocks, top, t_loc), jnp.int32),
                pltpu.SemaphoreType.DMA((blocks,)),
                pltpu.SemaphoreType.DMA((blocks,)),
            ],
            compiler_params=pltpu.CompilerParams(collective_id=0, has_side_effects=True, vmem_limit_bytes=VMEM_BYTES),
            name="route",
        )(idx.T, g.T, cap[:, None])

        sizes = (64, (c + 7 + 7) // 8 * 8)

        def stage(turns, mine, other, sizes=sizes):
            return pl.pallas_call(
                functools.partial(_expert_kernel, turns, sizes, cut),
                out_shape=[jax.ShapeDtypeStruct((half, d), F32)] * 4,
                in_specs=[smem, smem, vmem] + [anym] * 5,
                out_specs=[anym] * 4,
                scratch_shapes=[
                    pltpu.VMEM((2, rows, d), F32),
                    pltpu.VMEM((2, t_loc, d), BF16),
                    pltpu.VMEM((d, cut), BF16),
                    pltpu.VMEM((d, cut), BF16),
                    pltpu.VMEM((d, ff - cut), BF16),
                    pltpu.VMEM((d, ff - cut), BF16),
                    pltpu.VMEM((2, ff, d // 2), BF16),
                    pltpu.SemaphoreType.DMA((6,)),
                    pltpu.SemaphoreType.DMA((2, 4)),
                    pltpu.SemaphoreType.DMA((2,)),
                ],
                compiler_params=pltpu.CompilerParams(vmem_limit_bytes=VMEM_BYTES),
                cost_estimate=pl.CostEstimate(
                    flops=6 * rows * d * ff, bytes_accessed=6 * e_loc * d * ff + 8 * rows * d, transcendentals=0
                ),
            )(off, cnt, pos, mine, other, w1, w3, w2)

        def merge(parts):
            return [parts[2 + q] + swap(parts[q]) for q in range(2)]

        out, back = (1, 2), (2, 1)
        x_n, x_f = shift(x, out), shift(x, back)
        diag = merge(stage((3, 3), x_d, swap(x_d)))
        via = [shift(a, out) for a in diag]
        x_n, x_f = after(x_n, *diag), after(x_f, *diag)
        near = merge(stage(out, x_n, swap(x_n)))
        near = [shift(a, out) for a in near]
        part = stage(back, x_f, swap(x_f))
        far = merge(part)
        far = [a + b for a, b in zip(far, via)]
        x_o = after(x, *far)
        far = [shift(a, back) for a in far]
        own = merge(stage((0, 0), x_o, swap(x_o), sizes[-1:]))
        sums = [a + b for a, b in zip(own, near)]
        width = d // 4
        return pl.pallas_call(
            _combine_kernel,
            out_shape=jax.ShapeDtypeStruct((t_loc, d), BF16),
            grid=(4,),
            in_specs=[pl.BlockSpec((t_loc, 8), lambda i: (0, 0))] + [pl.BlockSpec((half, width), lambda i: (0, i))] * 4,
            out_specs=pl.BlockSpec((t_loc, width), lambda i: (0, i)),
            scratch_shapes=[pltpu.VMEM((top, t_loc, rows), BF16)],
            name="combine",
        )(mine, *sums, *far)

    rows = P(("ep", "tp"), None)
    return jax.shard_map(
        layer,
        mesh=mesh,
        in_specs=(rows, rows, rows, P(None), P("ep", None, "tp"), P("ep", None, "tp"), P("ep", "tp", None)),
        out_specs=rows,
        check_vma=False,
    )
```

```python
import functools

import jax
import jax.numpy as jnp
from jax import lax
from jax.experimental import pallas as pl
from jax.experimental.pallas import tpu as pltpu
from jax.sharding import PartitionSpec as P


F32 = jnp.float32
BF16 = jnp.bfloat16
VMEM_BYTES = 67_043_328


def _route_kernel(chips, turns, idx_ref, g_ref, cap_ref, x_ref, *refs):
    pos_ref, off_ref, cnt_ref, mine_ref, xm_ref, xo_ref, ids_all, send_sem, recv_sem, xsend, xrecv = refs
    core, me = lax.axis_index("ep"), lax.axis_index("tp")
    blocks, top, t = ids_all.shape
    e_all = cap_ref.shape[0]
    here = core * chips + me
    mesh_id = pl.DeviceIdType.MESH
    peers = [
        (k, {"ep": jnp.bitwise_xor(core, k // chips), "tp": jnp.bitwise_xor(me, k % chips)}) for k in range(1, blocks)
    ]
    barrier = pltpu.get_barrier_semaphore()
    for _, peer in peers:
        pl.semaphore_signal(barrier, inc=1, device_id=peer, device_id_type=mesh_id)
    pl.semaphore_wait(barrier, blocks - 1)
    copies = [
        pltpu.make_async_remote_copy(
            src_ref=idx_ref,
            dst_ref=ids_all.at[here],
            send_sem=send_sem.at[k],
            recv_sem=recv_sem.at[k],
            device_id=peer,
            device_id_type=mesh_id,
        )
        for k, peer in peers
    ]
    for c in copies:
        c.start()
    pieces = xsend.shape[1]
    turn = turns[0] + (turns[1] - turns[0]) * core
    piece = x_ref.shape[0] // pieces

    def tokens(hop, i, src, dst, peer):
        part = pl.ds(i * piece, piece)
        return pltpu.make_async_remote_copy(
            src_ref=src.at[part],
            dst_ref=dst.at[part],
            send_sem=xsend.at[hop, i],
            recv_sem=xrecv.at[hop, i],
            device_id=peer,
            device_id_type=mesh_id,
        )

    arrive = [tokens(0, i, x_ref, xm_ref, {"ep": core, "tp": jnp.bitwise_xor(me, turn)}) for i in range(pieces)]
    forward = [tokens(1, i, xm_ref, xo_ref, {"ep": 1 - core, "tp": me}) for i in range(pieces)]
    for c in arrive:
        c.start()
    ids_all[pl.ds(here, 1)] = idx_ref[...][None]
    before = (
        lax.broadcasted_iota(jnp.int32, (t, t), 0) < lax.broadcasted_iota(jnp.int32, (t, t), 1)
    ).astype(F32).astype(BF16)
    ids = lax.broadcasted_iota(jnp.int32, (e_all, t), 0)
    cap = jnp.broadcast_to(cap_ref[...], (e_all, t))
    for c in copies:
        c.wait()

    for b in range(blocks):
        hit = (ids_all[b, 0:1, :] == ids) | (ids_all[b, 1:2, :] == ids)
        one = hit.astype(F32)
        rank = jnp.dot(one.astype(BF16), before, preferred_element_type=F32).astype(jnp.int32)
        total = jnp.sum(one, axis=1, keepdims=True).astype(jnp.int32)
        count = jnp.minimum(jnp.broadcast_to(total, (e_all, t)), cap)
        first = jnp.zeros_like(count)
        for e in range(e_all - 1):
            first = first + jnp.where(ids > e, jnp.broadcast_to(count[e : e + 1, :], count.shape), 0)
        off_ref[b] = first[:, :128]
        cnt_ref[b] = count[:, :128]
        pos_ref[b] = jnp.where(hit & (rank < cap), first + rank, -1)
    pos = pos_ref[here]
    lines = [
        jnp.max(jnp.where(idx_ref[j : j + 1, :] == ids, pos, -1), axis=0, keepdims=True).astype(F32) for j in range(top)
    ]
    lines += [g_ref[j : j + 1, :] for j in range(top)]
    table = jnp.concatenate(lines + [jnp.zeros((8 - 2 * top, t), F32)], axis=0)
    mine_ref[...] = jnp.transpose(table)
    for c, f in zip(arrive, forward):
        c.wait_recv()
        f.start()
    for c, f in zip(arrive, forward):
        c.wait_send()
        f.wait()


def _expert_kernel(
    turns, sizes, cut, off_ref, cnt_ref, pos_ref, xm_hbm, xo_hbm, w1_hbm, w3_hbm, w2_hbm, *refs
):
    outs = refs[:4]
    acc, xbuf, w1a, w3a, w1b, w3b, w2s, wsem, osem, xsem = refs[4:]
    e_loc, d, ff = w1_hbm.shape
    _, rows, _ = acc.shape
    t = xbuf.shape[1]
    half_d, half = d // 2, rows // 2
    core, me = lax.axis_index("ep"), lax.axis_index("tp")
    chips = pos_ref.shape[0] // 2
    blocks = []
    for c in (core, 1 - core):
        turn = jnp.where(c == 0, turns[0], turns[1])
        blocks.append(c * chips + jnp.bitwise_xor(me, turn))

    def chunk(k, e):
        if isinstance(k, int) and k == 0:
            return [
                pltpu.make_async_copy(w1_hbm.at[e, :, pl.ds(0, cut)], w1a, wsem.at[0]),
                pltpu.make_async_copy(w3_hbm.at[e, :, pl.ds(0, cut)], w3a, wsem.at[1]),
            ]
        if isinstance(k, int) and k == 1:
            return [
                pltpu.make_async_copy(w1_hbm.at[e, :, pl.ds(cut, ff - cut)], w1b, wsem.at[2]),
                pltpu.make_async_copy(w3_hbm.at[e, :, pl.ds(cut, ff - cut)], w3b, wsem.at[3]),
            ]
        h = k - 2
        cols = pl.ds(pl.multiple_of(h * half_d, half_d), half_d)
        return [pltpu.make_async_copy(w2_hbm.at[e, :, cols], w2s.at[h], wsem.at[2 + k])]

    def start(k, e):
        for c in chunk(k, e):
            c.start()

    def finish(k, e):
        for c in chunk(k, e):
            c.wait()

    def following(k, e):
        @pl.when(e + 1 < e_loc)
        def _():
            start(k, e + 1)

    def out_copies(h):
        cols = pl.ds(h * half_d, half_d)
        return [
            pltpu.make_async_copy(
                acc.at[1 - i // 2, pl.ds((i % 2) * half, half), cols], outs[i].at[:, cols], osem.at[h, i]
            )
            for i in range(4)
        ]

    tokens = [
        pltpu.make_async_copy(xm_hbm, xbuf.at[0], xsem.at[0]),
        pltpu.make_async_copy(xo_hbm, xbuf.at[1], xsem.at[1]),
    ]
    for c in tokens:
        c.start()
    for k in range(4):
        start(k, 0)
    acc[...] = jnp.zeros_like(acc)
    for c in tokens:
        c.wait()

    def step(e, carry):
        expert = core * e_loc + e
        offs = [off_ref[b, expert, 0] for b in blocks]
        cnts = [cnt_ref[b, expert, 0] for b in blocks]
        need = functools.reduce(jnp.maximum, [jnp.where(k > 0, o - o // 8 * 8 + k, 0) for o, k in zip(offs, cnts)])

        def last(k):
            @pl.when((e == e_loc - 1) & (k == 0))
            def _():
                for c in out_copies(0):
                    c.start()

        def run(m):
            bases = [pl.multiple_of(jnp.minimum(o // 8 * 8, rows - m), 8) for o in offs]
            parts = []
            for s in range(2):
                row = lax.broadcasted_iota(jnp.int32, (m, t), 0) + bases[s]
                hit = (row == pos_ref[blocks[s], pl.ds(expert, 1), :]).astype(F32).astype(BF16)
                parts.append(jnp.dot(hit, xbuf[s], preferred_element_type=F32))
            xs = jnp.concatenate(parts, axis=0).astype(BF16)
            hs = []
            for k, (wa, wb) in enumerate(((w1a, w3a), (w1b, w3b))):
                finish(k, e)
                h1 = jnp.dot(xs, wa[...], preferred_element_type=F32)
                h3 = jnp.dot(xs, wb[...], preferred_element_type=F32)
                hs.append((jax.nn.silu(h1) * h3).astype(BF16))
                following(k, e)
            h = jnp.concatenate(hs, axis=1)

            def project(k, carry):
                finish(2 + k, e)
                p = jnp.dot(h, w2s[k], preferred_element_type=F32)
                cols = pl.ds(pl.multiple_of(k * half_d, half_d), half_d)
                for s in range(2):
                    acc[s, pl.ds(bases[s], m), cols] += p[s * m : (s + 1) * m]
                following(2 + k, e)
                last(k)
                return carry

            lax.fori_loop(0, 2, project, 0)

        @pl.when(need == 0)
        def _():
            for k in range(4):
                finish(k, e)
                following(k, e)
                last(k - 2)

        lo = 0
        for m in sizes:
            pl.when((need > lo) & (need <= m))(functools.partial(run, m))
            lo = m
        return carry

    lax.fori_loop(0, e_loc, step, 0)
    for c in out_copies(1):
        c.start()
    for c in out_copies(0) + out_copies(1):
        c.wait()


def _combine_kernel(mine_ref, s0_ref, s1_ref, f0_ref, f1_ref, out_ref, hit):
    top, t, rows = hit.shape

    @pl.when(pl.program_id(0) == 0)
    def _():
        row = lax.broadcasted_iota(jnp.int32, (t, rows), 1)
        for j in range(top):
            hit[j] = (row == mine_ref[:, j : j + 1].astype(jnp.int32)).astype(F32).astype(BF16)

    y = jnp.concatenate([s0_ref[...] + f0_ref[...], s1_ref[...] + f1_ref[...]], axis=0).astype(BF16)
    total = None
    for j in range(top):
        part = jnp.dot(hit[j], y, preferred_element_type=F32) * mine_ref[:, top + j : top + j + 1]
        total = part if total is None else total + part
    out_ref[...] = total.astype(out_ref.dtype)


def solution(mesh):
    chips = mesh.shape["tp"]
    vmem = pl.BlockSpec(memory_space=pltpu.VMEM)
    anym = pl.BlockSpec(memory_space=pl.ANY)
    smem = pl.BlockSpec(memory_space=pltpu.SMEM)

    def layer(x, idx, g, cap, w1, w3, w2):
        t_loc, d = x.shape
        top = idx.shape[1]
        e_all = cap.shape[0]
        e_loc, _, ff = w1.shape
        c = (5 * top * t_loc // (2 * e_all) + 7) // 8 * 8
        rows = top * t_loc
        half = rows // 2
        cut = 512
        blocks = 2 * chips

        def swap(a):
            return lax.ppermute(a, "ep", [(0, 1), (1, 0)])

        def shift(a, turns):
            pairs = [(2 * k + i, 2 * (k ^ turns[i]) + i) for k in range(chips) for i in range(2)]
            return lax.ppermute(a, ("tp", "ep"), pairs)

        def after(a, *first):
            return lax.optimization_barrier((a, *first))[0]

        out, back = (1, 2), (2, 1)
        pieces = 4
        pos, off, cnt, mine, xn_mine, xn_other = pl.pallas_call(
            functools.partial(_route_kernel, chips, out),
            out_shape=[
                jax.ShapeDtypeStruct((blocks, e_all, t_loc), jnp.int32),
                jax.ShapeDtypeStruct((blocks, e_all, 128), jnp.int32),
                jax.ShapeDtypeStruct((blocks, e_all, 128), jnp.int32),
                jax.ShapeDtypeStruct((t_loc, 8), F32),
                jax.ShapeDtypeStruct((t_loc, d), BF16),
                jax.ShapeDtypeStruct((t_loc, d), BF16),
            ],
            in_specs=[vmem] * 3 + [anym],
            out_specs=[vmem] * 4 + [anym] * 2,
            scratch_shapes=[
                pltpu.VMEM((blocks, top, t_loc), jnp.int32),
                pltpu.SemaphoreType.DMA((blocks,)),
                pltpu.SemaphoreType.DMA((blocks,)),
                pltpu.SemaphoreType.DMA((2, pieces)),
                pltpu.SemaphoreType.DMA((2, pieces)),
            ],
            compiler_params=pltpu.CompilerParams(collective_id=0, has_side_effects=True, vmem_limit_bytes=VMEM_BYTES),
            name="route",
        )(idx.T, g.T, cap[:, None], x)

        sizes = (64, (c + 7 + 7) // 8 * 8)

        def stage(turns, mine, other, sizes=sizes):
            return pl.pallas_call(
                functools.partial(_expert_kernel, turns, sizes, cut),
                out_shape=[jax.ShapeDtypeStruct((half, d), F32)] * 4,
                in_specs=[smem, smem, vmem] + [anym] * 5,
                out_specs=[anym] * 4,
                scratch_shapes=[
                    pltpu.VMEM((2, rows, d), F32),
                    pltpu.VMEM((2, t_loc, d), BF16),
                    pltpu.VMEM((d, cut), BF16),
                    pltpu.VMEM((d, cut), BF16),
                    pltpu.VMEM((d, ff - cut), BF16),
                    pltpu.VMEM((d, ff - cut), BF16),
                    pltpu.VMEM((2, ff, d // 2), BF16),
                    pltpu.SemaphoreType.DMA((6,)),
                    pltpu.SemaphoreType.DMA((2, 4)),
                    pltpu.SemaphoreType.DMA((2,)),
                ],
                compiler_params=pltpu.CompilerParams(vmem_limit_bytes=VMEM_BYTES),
                cost_estimate=pl.CostEstimate(
                    flops=6 * rows * d * ff, bytes_accessed=6 * e_loc * d * ff + 8 * rows * d, transcendentals=0
                ),
            )(off, cnt, pos, mine, other, w1, w3, w2)

        def merge(parts, *more):
            sums = []
            for q in range(2):
                other = swap(parts[q])
                sums.append(functools.reduce(jnp.add, [m[q] for m in more], parts[2 + q] + other))
            return sums

        x_next = after(x, pos)
        x_d, x_f = shift(x_next, (3, 3)), shift(x_next, back)
        near = merge(stage(out, xn_mine, xn_other))
        x_d = after(x_d, *near)
        near = [shift(a, out) for a in near]
        diag = merge(stage((3, 3), x_d, swap(x_d)))
        x_f = after(x_f, *diag)
        via = [shift(a, out) for a in diag]
        far = merge(stage(back, x_f, swap(x_f)), via)
        x_o = after(x, *far)
        far = [shift(a, back) for a in far]
        sums = merge(stage((0, 0), x_o, swap(x_o)), near)
        width = d // 4
        return pl.pallas_call(
            _combine_kernel,
            out_shape=jax.ShapeDtypeStruct((t_loc, d), BF16),
            grid=(4,),
            in_specs=[pl.BlockSpec((t_loc, 8), lambda i: (0, 0))] + [pl.BlockSpec((half, width), lambda i: (0, i))] * 4,
            out_specs=pl.BlockSpec((t_loc, width), lambda i: (0, i)),
            scratch_shapes=[pltpu.VMEM((top, t_loc, rows), BF16)],
            name="combine",
        )(mine, *sums, *far)

    rows = P(("ep", "tp"), None)
    return jax.shard_map(
        layer,
        mesh=mesh,
        in_specs=(rows, rows, rows, P(None), P("ep", None, "tp"), P("ep", None, "tp"), P("ep", "tp", None)),
        out_specs=rows,
        check_vma=False,
    )
```

```python
import functools

import jax
import jax.numpy as jnp
from jax import lax
from jax.experimental import pallas as pl
from jax.experimental.pallas import tpu as pltpu
from jax.sharding import PartitionSpec as P


F32 = jnp.float32
BF16 = jnp.bfloat16
VMEM_BYTES = 67_043_328


def _route_kernel(chips, turns, idx_ref, g_ref, cap_ref, x_ref, *refs):
    pos_ref, off_ref, cnt_ref, mine_ref, xm_ref, xo_ref, ids_all, send_sem, recv_sem, xsend, xrecv = refs
    core, me = lax.axis_index("ep"), lax.axis_index("tp")
    blocks, top, t = ids_all.shape
    e_all = pos_ref.shape[1]
    here = core * chips + me
    mesh_id = pl.DeviceIdType.MESH
    peers = [
        (k, {"ep": jnp.bitwise_xor(core, k // chips), "tp": jnp.bitwise_xor(me, k % chips)}) for k in range(1, blocks)
    ]
    barrier = pltpu.get_barrier_semaphore()
    for _, peer in peers:
        pl.semaphore_signal(barrier, inc=1, device_id=peer, device_id_type=mesh_id)
    pl.semaphore_wait(barrier, blocks - 1)
    copies = [
        pltpu.make_async_remote_copy(
            src_ref=idx_ref,
            dst_ref=ids_all.at[here],
            send_sem=send_sem.at[k],
            recv_sem=recv_sem.at[k],
            device_id=peer,
            device_id_type=mesh_id,
        )
        for k, peer in peers
    ]
    for c in copies:
        c.start()
    pieces = xsend.shape[1]
    turn = turns[0] + (turns[1] - turns[0]) * core
    piece = x_ref.shape[0] // pieces

    def tokens(hop, i, src, dst, peer):
        part = pl.ds(i * piece, piece)
        return pltpu.make_async_remote_copy(
            src_ref=src.at[part],
            dst_ref=dst.at[part],
            send_sem=xsend.at[hop, i],
            recv_sem=xrecv.at[hop, i],
            device_id=peer,
            device_id_type=mesh_id,
        )

    arrive = [tokens(0, i, x_ref, xm_ref, {"ep": core, "tp": jnp.bitwise_xor(me, turn)}) for i in range(pieces)]
    forward = [tokens(1, i, xm_ref, xo_ref, {"ep": 1 - core, "tp": me}) for i in range(pieces)]
    for c in arrive:
        c.start()
    ids_all[pl.ds(here, 1)] = idx_ref[...][None]
    before = (
        lax.broadcasted_iota(jnp.int32, (t, t), 0) < lax.broadcasted_iota(jnp.int32, (t, t), 1)
    ).astype(F32).astype(BF16)
    ids = lax.broadcasted_iota(jnp.int32, (e_all, t), 0)
    cap = jnp.zeros((e_all, t), jnp.int32)
    for e in range(e_all):
        cap = jnp.where(ids == e, cap_ref[e], cap)
    for c in copies:
        c.wait()

    for b in range(blocks):
        hit = (ids_all[b, 0:1, :] == ids) | (ids_all[b, 1:2, :] == ids)
        one = hit.astype(F32)
        rank = jnp.dot(one.astype(BF16), before, preferred_element_type=F32).astype(jnp.int32)
        total = jnp.sum(one, axis=1, keepdims=True).astype(jnp.int32)
        count = jnp.minimum(jnp.broadcast_to(total, (e_all, t)), cap)
        first = jnp.zeros_like(count)
        for e in range(e_all - 1):
            first = first + jnp.where(ids > e, jnp.broadcast_to(count[e : e + 1, :], count.shape), 0)
        off_ref[b] = first[:, :128]
        cnt_ref[b] = count[:, :128]
        pos_ref[b] = jnp.where(hit & (rank < cap), first + rank, -1)
    pos = pos_ref[here]
    lines = [
        jnp.max(jnp.where(idx_ref[j : j + 1, :] == ids, pos, -1), axis=0, keepdims=True).astype(F32) for j in range(top)
    ]
    lines += [g_ref[j : j + 1, :] for j in range(top)]
    table = jnp.concatenate(lines + [jnp.zeros((8 - 2 * top, t), F32)], axis=0)
    mine_ref[...] = jnp.transpose(table)
    for c, f in zip(arrive, forward):
        c.wait_recv()
        f.start()
    for c, f in zip(arrive, forward):
        c.wait_send()
        f.wait()


def _expert_kernel(
    turns, sizes, cut, off_ref, cnt_ref, pos_ref, xm_hbm, xo_hbm, w1_hbm, w3_hbm, w2_hbm, *refs
):
    outs = refs[:4]
    acc, xbuf, w1a, w3a, w1b, w3b, w2s, wsem, osem, xsem = refs[4:]
    e_loc, d, ff = w1_hbm.shape
    _, rows, _ = acc.shape
    t = xbuf.shape[1]
    half_d = d // 2
    core, me = lax.axis_index("ep"), lax.axis_index("tp")
    chips = pos_ref.shape[0] // 2
    blocks = []
    for c in (core, 1 - core):
        turn = jnp.where(c == 0, turns[0], turns[1])
        blocks.append(c * chips + jnp.bitwise_xor(me, turn))

    def first(e):
        cols, b = pl.ds(0, cut), e % 2
        return [
            pltpu.make_async_copy(w1_hbm.at[e, :, cols], w1a.at[b], wsem.at[b, 0]),
            pltpu.make_async_copy(w3_hbm.at[e, :, cols], w3a.at[b], wsem.at[b, 1]),
        ]

    def second(e):
        cols, b = pl.ds(cut, ff - cut), e % 2
        return [
            pltpu.make_async_copy(w1_hbm.at[e, :, cols], w1b.at[b], wsem.at[b, 2]),
            pltpu.make_async_copy(w3_hbm.at[e, :, cols], w3b.at[b], wsem.at[b, 3]),
        ]

    def third(k):
        def copies(e):
            cols, b = pl.ds(pl.multiple_of(k * half_d, half_d), half_d), e % 2
            return [pltpu.make_async_copy(w2_hbm.at[e, :, cols], w2s.at[b, k], wsem.at[b, 4 + k])]

        return copies

    def arrive(chunk, e):
        for c in chunk(e):
            c.wait()

        @pl.when(e + 1 < e_loc)
        def _():
            for c in chunk(e + 1):
                c.start()

    def out_copies(h):
        cols = pl.ds(h * half_d, half_d)
        copies = []
        for i in range(4):
            size = outs[i].shape[0]
            part = pl.ds(0 if i % 2 == 0 else rows - size, size)
            copies.append(pltpu.make_async_copy(acc.at[1 - i // 2, part, cols], outs[i].at[:, cols], osem.at[h, i]))
        return copies

    tokens = [
        pltpu.make_async_copy(xm_hbm, xbuf.at[0], xsem.at[0]),
        pltpu.make_async_copy(xo_hbm, xbuf.at[1], xsem.at[1]),
    ]
    for c in tokens:
        c.start()
    for chunk in (first, second, third(0), third(1)):
        for c in chunk(0):
            c.start()
    acc[...] = jnp.zeros_like(acc)
    for c in tokens:
        c.wait()

    def step(e, carry):
        expert = core * e_loc + e
        offs = [off_ref[b, expert, 0] for b in blocks]
        cnts = [cnt_ref[b, expert, 0] for b in blocks]
        need = functools.reduce(jnp.maximum, [jnp.where(k > 0, o - o // 8 * 8 + k, 0) for o, k in zip(offs, cnts)])

        def last(k):
            @pl.when((e == e_loc - 1) & (k == 0))
            def _():
                for c in out_copies(0):
                    c.start()

        def run(m):
            bases = [pl.multiple_of(jnp.minimum(o // 8 * 8, rows - m), 8) for o in offs]
            parts = []
            for s in range(2):
                row = lax.broadcasted_iota(jnp.int32, (m, t), 0) + bases[s]
                hit = (row == pos_ref[blocks[s], pl.ds(expert, 1), :]).astype(F32).astype(BF16)
                parts.append(jnp.dot(hit, xbuf[s], preferred_element_type=F32))
            xs = jnp.concatenate(parts, axis=0).astype(BF16)
            hs = []
            for chunk, wa, wb in ((first, w1a, w3a), (second, w1b, w3b)):
                arrive(chunk, e)
                h1 = jnp.dot(xs, wa[e % 2], preferred_element_type=F32)
                h3 = jnp.dot(xs, wb[e % 2], preferred_element_type=F32)
                hs.append((jax.nn.silu(h1) * h3).astype(BF16))
            h = jnp.concatenate(hs, axis=1)

            def project(k, carry):
                arrive(third(k), e)
                p = jnp.dot(h, w2s[e % 2, k], preferred_element_type=F32)
                cols = pl.ds(pl.multiple_of(k * half_d, half_d), half_d)
                for s in range(2):
                    acc[s, pl.ds(bases[s], m), cols] += p[s * m : (s + 1) * m]
                last(k)
                return carry

            lax.fori_loop(0, 2, project, 0)

        @pl.when(need == 0)
        def _():
            for chunk in (first, second, third(0), third(1)):
                arrive(chunk, e)
            last(0)

        lo = 0
        for m in sizes:
            pl.when((need > lo) & (need <= m))(functools.partial(run, m))
            lo = m
        return carry

    lax.fori_loop(0, e_loc, step, 0)
    for c in out_copies(1):
        c.start()
    for c in out_copies(0) + out_copies(1):
        c.wait()


def _combine_kernel(first, mine_ref, sum_ref, last_ref, *refs):
    out_ref, hit = refs[-2:]
    top, t, rows = hit.shape

    @pl.when(pl.program_id(0) == 0)
    def _():
        row = lax.broadcasted_iota(jnp.int32, (t, rows), 1) + first
        for j in range(top):
            hit[j] = (row == mine_ref[:, j : j + 1].astype(jnp.int32)).astype(F32).astype(BF16)

    y = (sum_ref[...] + last_ref[...]).astype(BF16)
    total = refs[0][...] if len(refs) == 3 else None
    for j in range(top):
        part = jnp.dot(hit[j], y, preferred_element_type=F32) * mine_ref[:, top + j : top + j + 1]
        total = part if total is None else total + part
    out_ref[...] = total.astype(out_ref.dtype)


def solution(mesh):
    chips = mesh.shape["tp"]
    vmem = pl.BlockSpec(memory_space=pltpu.VMEM)
    anym = pl.BlockSpec(memory_space=pl.ANY)
    smem = pl.BlockSpec(memory_space=pltpu.SMEM)

    def layer(x, idx, g, cap, w1, w3, w2):
        t_loc, d = x.shape
        top = idx.shape[1]
        e_all = cap.shape[0]
        e_loc, _, ff = w1.shape
        c = (5 * top * t_loc // (2 * e_all) + 7) // 8 * 8
        rows = top * t_loc
        cut = 512
        blocks = 2 * chips

        def swap(a):
            return lax.ppermute(a, "ep", [(0, 1), (1, 0)])

        def shift(a, turns):
            pairs = [(2 * k + i, 2 * (k ^ turns[i]) + i) for k in range(chips) for i in range(2)]
            return lax.ppermute(a, ("tp", "ep"), pairs)

        def after(a, *first):
            return lax.optimization_barrier((a, *first))[0]

        out, back = (1, 2), (2, 1)
        pieces = 4
        pos, off, cnt, mine, xn_mine, xn_other = pl.pallas_call(
            functools.partial(_route_kernel, chips, out),
            out_shape=[
                jax.ShapeDtypeStruct((blocks, e_all, t_loc), jnp.int32),
                jax.ShapeDtypeStruct((blocks, e_all, 128), jnp.int32),
                jax.ShapeDtypeStruct((blocks, e_all, 128), jnp.int32),
                jax.ShapeDtypeStruct((t_loc, 8), F32),
                jax.ShapeDtypeStruct((t_loc, d), BF16),
                jax.ShapeDtypeStruct((t_loc, d), BF16),
            ],
            in_specs=[vmem, vmem, smem, anym],
            out_specs=[vmem] * 4 + [anym] * 2,
            scratch_shapes=[
                pltpu.VMEM((blocks, top, t_loc), jnp.int32),
                pltpu.SemaphoreType.DMA((blocks,)),
                pltpu.SemaphoreType.DMA((blocks,)),
                pltpu.SemaphoreType.DMA((2, pieces)),
                pltpu.SemaphoreType.DMA((2, pieces)),
            ],
            compiler_params=pltpu.CompilerParams(collective_id=0, has_side_effects=True, vmem_limit_bytes=VMEM_BYTES),
            name="route",
        )(idx.T, g.T, cap, x)

        sizes = (64, (c + 7 + 7) // 8 * 8)

        def stage(turns, mine, other, split):
            return pl.pallas_call(
                functools.partial(_expert_kernel, turns, sizes, cut),
                out_shape=[jax.ShapeDtypeStruct((n, d), F32) for n in split * 2],
                in_specs=[smem, smem, vmem] + [anym] * 5,
                out_specs=[anym] * 4,
                scratch_shapes=[
                    pltpu.VMEM((2, rows, d), F32),
                    pltpu.VMEM((2, t_loc, d), BF16),
                    pltpu.VMEM((2, d, cut), BF16),
                    pltpu.VMEM((2, d, cut), BF16),
                    pltpu.VMEM((2, d, ff - cut), BF16),
                    pltpu.VMEM((2, d, ff - cut), BF16),
                    pltpu.VMEM((2, 2, ff, d // 2), BF16),
                    pltpu.SemaphoreType.DMA((2, 6)),
                    pltpu.SemaphoreType.DMA((2, 4)),
                    pltpu.SemaphoreType.DMA((2,)),
                ],
                compiler_params=pltpu.CompilerParams(vmem_limit_bytes=VMEM_BYTES),
                cost_estimate=pl.CostEstimate(
                    flops=6 * rows * d * ff, bytes_accessed=6 * e_loc * d * ff + 8 * rows * d, transcendentals=0
                ),
            )(off, cnt, pos, mine, other, w1, w3, w2)

        def merge(parts, *more):
            sums = []
            for q in range(2):
                other = swap(parts[q])
                sums.append(functools.reduce(jnp.add, [m[q] for m in more], parts[2 + q] + other))
            return sums

        x_next = after(x, pos)
        x_d, x_f = shift(x_next, (3, 3)), shift(x_next, back)
        early, late = (rows // 4, rows - rows // 4), (rows - rows // 4, rows // 4)
        near = merge(stage(out, xn_mine, xn_other, early))
        x_d = after(x_d, *near)
        near = [shift(a, out) for a in near]
        diag = merge(stage((3, 3), x_d, swap(x_d), late))
        x_f = after(x_f, *diag)
        via = [shift(a, out) for a in diag]
        far = merge(stage(back, x_f, swap(x_f), late), via)
        x_o = after(x, *far)
        far = [shift(a, back) for a in far]
        near = jnp.concatenate(near, axis=0)
        near = [near[: late[0]], near[late[0] :]]
        sums = merge(stage((0, 0), x_o, swap(x_o), late), near)
        width = d // 4
        total = None
        for q in range(2):
            table = pl.BlockSpec((t_loc, 8), lambda i: (0, 0))
            part = pl.BlockSpec((late[q], width), lambda i: (0, i))
            wide = pl.BlockSpec((t_loc, width), lambda i: (0, i))
            total = pl.pallas_call(
                functools.partial(_combine_kernel, q * late[0]),
                out_shape=jax.ShapeDtypeStruct((t_loc, d), (F32, BF16)[q]),
                grid=(4,),
                in_specs=[table, part, part] + [wide] * q,
                out_specs=wide,
                scratch_shapes=[pltpu.VMEM((top, t_loc, late[q]), BF16)],
                cost_estimate=pl.CostEstimate(flops=8 * t_loc * late[q] * d, bytes_accessed=16 * late[q] * d, transcendentals=0),
            )(mine, sums[q], far[q], *([total] * q))
        return total

    rows = P(("ep", "tp"), None)
    return jax.shard_map(
        layer,
        mesh=mesh,
        in_specs=(rows, rows, rows, P(None), P("ep", None, "tp"), P("ep", None, "tp"), P("ep", "tp", None)),
        out_specs=rows,
        check_vma=False,
    )
```

```python
import functools

import jax
import jax.numpy as jnp
from jax import lax
from jax.experimental import pallas as pl
from jax.experimental.pallas import tpu as pltpu
from jax.sharding import PartitionSpec as P


F32 = jnp.float32
BF16 = jnp.bfloat16
VMEM_BYTES = 67_043_328


def _route_kernel(chips, turns, idx_ref, g_ref, cap_ref, x_ref, *refs):
    pos_ref, table_ref, mine_ref, xm_ref, xo_ref, ids_all, send_sem, recv_sem, xsend, xrecv = refs
    core, me = lax.axis_index("ep"), lax.axis_index("tp")
    blocks, top, t = ids_all.shape
    e_all = pos_ref.shape[1]
    here = core * chips + me
    mesh_id = pl.DeviceIdType.MESH
    peers = [
        (k, {"ep": jnp.bitwise_xor(core, k // chips), "tp": jnp.bitwise_xor(me, k % chips)}) for k in range(1, blocks)
    ]
    barrier = pltpu.get_barrier_semaphore()
    for _, peer in peers:
        pl.semaphore_signal(barrier, inc=1, device_id=peer, device_id_type=mesh_id)
    pl.semaphore_wait(barrier, blocks - 1)
    copies = [
        pltpu.make_async_remote_copy(
            src_ref=idx_ref,
            dst_ref=ids_all.at[here],
            send_sem=send_sem.at[k],
            recv_sem=recv_sem.at[k],
            device_id=peer,
            device_id_type=mesh_id,
        )
        for k, peer in peers
    ]
    for c in copies:
        c.start()
    pieces = xsend.shape[1]
    turn = turns[0] + (turns[1] - turns[0]) * core
    piece = x_ref.shape[0] // pieces

    def tokens(hop, i, src, dst, peer):
        part = pl.ds(i * piece, piece)
        return pltpu.make_async_remote_copy(
            src_ref=src.at[part],
            dst_ref=dst.at[part],
            send_sem=xsend.at[hop, i],
            recv_sem=xrecv.at[hop, i],
            device_id=peer,
            device_id_type=mesh_id,
        )

    arrive = [tokens(0, i, x_ref, xm_ref, {"ep": core, "tp": jnp.bitwise_xor(me, turn)}) for i in range(pieces)]
    forward = [tokens(1, i, xm_ref, xo_ref, {"ep": 1 - core, "tp": me}) for i in range(pieces)]
    for c in arrive:
        c.start()
    ids_all[pl.ds(here, 1)] = idx_ref[...][None]
    before = (
        lax.broadcasted_iota(jnp.int32, (t, t), 0) < lax.broadcasted_iota(jnp.int32, (t, t), 1)
    ).astype(F32).astype(BF16)
    ids = lax.broadcasted_iota(jnp.int32, (e_all, t), 0)
    cap = jnp.zeros((e_all, t), jnp.int32)
    for e in range(e_all):
        cap = jnp.where(ids == e, cap_ref[e], cap)
    sub, lane = (lax.broadcasted_iota(jnp.int32, (e_all, 128), i) for i in range(2))
    for c in copies:
        c.wait()

    for b in range(blocks):
        hit = (ids_all[b, 0:1, :] == ids) | (ids_all[b, 1:2, :] == ids)
        one = hit.astype(F32)
        rank = jnp.dot(one.astype(BF16), before, preferred_element_type=F32).astype(jnp.int32)
        total = jnp.sum(one, axis=1, keepdims=True).astype(jnp.int32)
        count = jnp.minimum(jnp.broadcast_to(total, (e_all, t)), cap)
        first = jnp.zeros_like(count)
        for e in range(e_all - 1):
            first = first + jnp.where(ids > e, jnp.broadcast_to(count[e : e + 1, :], count.shape), 0)
        pair = jnp.where(lane == sub, first[:, :128], 0) + jnp.where(lane == sub + e_all, count[:, :128], 0)
        table_ref[pl.ds(b, 1)] = jnp.sum(pair, axis=0, keepdims=True)
        pos_ref[b] = jnp.where(hit & (rank < cap), first + rank, -1)
    pos = pos_ref[here]
    lines = [
        jnp.max(jnp.where(idx_ref[j : j + 1, :] == ids, pos, -1), axis=0, keepdims=True).astype(F32) for j in range(top)
    ]
    lines += [g_ref[j : j + 1, :] for j in range(top)]
    table = jnp.concatenate(lines + [jnp.zeros((8 - 2 * top, t), F32)], axis=0)
    mine_ref[...] = jnp.transpose(table)
    for c, f in zip(arrive, forward):
        c.wait_recv()
        f.start()
    for c, f in zip(arrive, forward):
        c.wait_send()
        f.wait()


def _expert_kernel(
    turns, sizes, cut, table_ref, pos_ref, xm_hbm, xo_hbm, w1_hbm, w3_hbm, w2_hbm, *refs
):
    outs = refs[:4]
    acc, xbuf, w1a, w3a, w1b, w3b, w2s, wsem, osem, xsem = refs[4:]
    e_loc, d, ff = w1_hbm.shape
    _, rows, _ = acc.shape
    t = xbuf.shape[1]
    half_d = d // 2
    core, me = lax.axis_index("ep"), lax.axis_index("tp")
    chips = pos_ref.shape[0] // 2
    blocks = []
    for c in (core, 1 - core):
        turn = jnp.where(c == 0, turns[0], turns[1])
        blocks.append(c * chips + jnp.bitwise_xor(me, turn))

    def first(e):
        cols, b = pl.ds(0, cut), e % 2
        return [
            pltpu.make_async_copy(w1_hbm.at[e, :, cols], w1a.at[b], wsem.at[b, 0]),
            pltpu.make_async_copy(w3_hbm.at[e, :, cols], w3a.at[b], wsem.at[b, 1]),
        ]

    def second(e):
        cols, b = pl.ds(cut, ff - cut), e % 2
        return [
            pltpu.make_async_copy(w1_hbm.at[e, :, cols], w1b.at[b], wsem.at[b, 2]),
            pltpu.make_async_copy(w3_hbm.at[e, :, cols], w3b.at[b], wsem.at[b, 3]),
        ]

    def third(k):
        def copies(e):
            cols, b = pl.ds(pl.multiple_of(k * half_d, half_d), half_d), e % 2
            return [pltpu.make_async_copy(w2_hbm.at[e, :, cols], w2s.at[b, k], wsem.at[b, 4 + k])]

        return copies

    def arrive(chunk, e):
        for c in chunk(e):
            c.wait()

        @pl.when(e + 1 < e_loc)
        def _():
            for c in chunk(e + 1):
                c.start()

    def out_copies(h):
        cols = pl.ds(h * half_d, half_d)
        copies = []
        for i in range(4):
            size = outs[i].shape[0]
            part = pl.ds(0 if i % 2 == 0 else rows - size, size)
            copies.append(pltpu.make_async_copy(acc.at[1 - i // 2, part, cols], outs[i].at[:, cols], osem.at[h, i]))
        return copies

    tokens = [
        pltpu.make_async_copy(xm_hbm, xbuf.at[0], xsem.at[0]),
        pltpu.make_async_copy(xo_hbm, xbuf.at[1], xsem.at[1]),
    ]
    for c in tokens:
        c.start()
    for chunk in (first, second, third(0), third(1)):
        for c in chunk(0):
            c.start()
    acc[...] = jnp.zeros_like(acc)
    for c in tokens:
        c.wait()

    def step(e, carry):
        expert = core * e_loc + e
        offs = [table_ref[b, expert] for b in blocks]
        cnts = [table_ref[b, 2 * e_loc + expert] for b in blocks]
        need = functools.reduce(jnp.maximum, [jnp.where(k > 0, o - o // 8 * 8 + k, 0) for o, k in zip(offs, cnts)])

        def last(k):
            @pl.when((e == e_loc - 1) & (k == 0))
            def _():
                for c in out_copies(0):
                    c.start()

        def run(m):
            bases = [pl.multiple_of(jnp.minimum(o // 8 * 8, rows - m), 8) for o in offs]
            parts = []
            for s in range(2):
                row = lax.broadcasted_iota(jnp.int32, (m, t), 0) + bases[s]
                hit = (row == pos_ref[blocks[s], pl.ds(expert, 1), :]).astype(F32).astype(BF16)
                parts.append(jnp.dot(hit, xbuf[s], preferred_element_type=F32))
            xs = jnp.concatenate(parts, axis=0).astype(BF16)
            hs = []
            for chunk, wa, wb in ((first, w1a, w3a), (second, w1b, w3b)):
                arrive(chunk, e)
                h1 = jnp.dot(xs, wa[e % 2], preferred_element_type=F32)
                h3 = jnp.dot(xs, wb[e % 2], preferred_element_type=F32)
                hs.append((jax.nn.silu(h1) * h3).astype(BF16))
            h = jnp.concatenate(hs, axis=1)

            def project(k, carry):
                arrive(third(k), e)
                p = jnp.dot(h, w2s[e % 2, k], preferred_element_type=F32)
                cols = pl.ds(pl.multiple_of(k * half_d, half_d), half_d)
                for s in range(2):
                    acc[s, pl.ds(bases[s], m), cols] += p[s * m : (s + 1) * m]
                last(k)
                return carry

            lax.fori_loop(0, 2, project, 0)

        @pl.when(need == 0)
        def _():
            for chunk in (first, second, third(0), third(1)):
                arrive(chunk, e)
            last(0)

        lo = 0
        for m in sizes:
            pl.when((need > lo) & (need <= m))(functools.partial(run, m))
            lo = m
        return carry

    lax.fori_loop(0, e_loc, step, 0)
    for c in out_copies(1):
        c.start()
    for c in out_copies(0) + out_copies(1):
        c.wait()


def _combine_kernel(mine_ref, s0_ref, s1_ref, f0_ref, f1_ref, out_ref, hit):
    top, t, rows = hit.shape

    @pl.when(pl.program_id(0) == 0)
    def _():
        row = lax.broadcasted_iota(jnp.int32, (t, rows), 1)
        for j in range(top):
            hit[j] = (row == mine_ref[:, j : j + 1].astype(jnp.int32)).astype(F32).astype(BF16)

    y = jnp.concatenate([s0_ref[...] + f0_ref[...], s1_ref[...] + f1_ref[...]], axis=0).astype(BF16)
    total = None
    for j in range(top):
        part = jnp.dot(hit[j], y, preferred_element_type=F32) * mine_ref[:, top + j : top + j + 1]
        total = part if total is None else total + part
    out_ref[...] = total.astype(out_ref.dtype)


def solution(mesh):
    chips = mesh.shape["tp"]
    vmem = pl.BlockSpec(memory_space=pltpu.VMEM)
    anym = pl.BlockSpec(memory_space=pl.ANY)
    smem = pl.BlockSpec(memory_space=pltpu.SMEM)

    def layer(x, idx, g, cap, w1, w3, w2):
        t_loc, d = x.shape
        top = idx.shape[1]
        e_all = cap.shape[0]
        e_loc, _, ff = w1.shape
        c = (5 * top * t_loc // (2 * e_all) + 7) // 8 * 8
        rows = top * t_loc
        cut = 512
        blocks = 2 * chips

        def swap(a):
            return lax.ppermute(a, "ep", [(0, 1), (1, 0)])

        def shift(a, turns):
            pairs = [(2 * k + i, 2 * (k ^ turns[i]) + i) for k in range(chips) for i in range(2)]
            return lax.ppermute(a, ("tp", "ep"), pairs)

        def after(a, *first):
            return lax.optimization_barrier((a, *first))[0]

        out, back = (1, 2), (2, 1)
        pieces = 4
        pos, groups, mine, xn_mine, xn_other = pl.pallas_call(
            functools.partial(_route_kernel, chips, out),
            out_shape=[
                jax.ShapeDtypeStruct((blocks, e_all, t_loc), jnp.int32),
                jax.ShapeDtypeStruct((blocks, 128), jnp.int32),
                jax.ShapeDtypeStruct((t_loc, 8), F32),
                jax.ShapeDtypeStruct((t_loc, d), BF16),
                jax.ShapeDtypeStruct((t_loc, d), BF16),
            ],
            in_specs=[vmem, vmem, smem, anym],
            out_specs=[vmem] * 3 + [anym] * 2,
            scratch_shapes=[
                pltpu.VMEM((blocks, top, t_loc), jnp.int32),
                pltpu.SemaphoreType.DMA((blocks,)),
                pltpu.SemaphoreType.DMA((blocks,)),
                pltpu.SemaphoreType.DMA((2, pieces)),
                pltpu.SemaphoreType.DMA((2, pieces)),
            ],
            compiler_params=pltpu.CompilerParams(collective_id=0, has_side_effects=True, vmem_limit_bytes=VMEM_BYTES),
            name="route",
        )(idx.T, g.T, cap, x)

        sizes = (64, (c + 7 + 7) // 8 * 8)

        def stage(turns, mine, other, split):
            return pl.pallas_call(
                functools.partial(_expert_kernel, turns, sizes, cut),
                out_shape=[jax.ShapeDtypeStruct((n, d), F32) for n in split * 2],
                in_specs=[smem, vmem] + [anym] * 5,
                out_specs=[anym] * 4,
                scratch_shapes=[
                    pltpu.VMEM((2, rows, d), F32),
                    pltpu.VMEM((2, t_loc, d), BF16),
                    pltpu.VMEM((2, d, cut), BF16),
                    pltpu.VMEM((2, d, cut), BF16),
                    pltpu.VMEM((2, d, ff - cut), BF16),
                    pltpu.VMEM((2, d, ff - cut), BF16),
                    pltpu.VMEM((2, 2, ff, d // 2), BF16),
                    pltpu.SemaphoreType.DMA((2, 6)),
                    pltpu.SemaphoreType.DMA((2, 4)),
                    pltpu.SemaphoreType.DMA((2,)),
                ],
                compiler_params=pltpu.CompilerParams(vmem_limit_bytes=VMEM_BYTES),
                cost_estimate=pl.CostEstimate(
                    flops=6 * rows * d * ff, bytes_accessed=6 * e_loc * d * ff + 8 * rows * d, transcendentals=0
                ),
            )(groups, pos, mine, other, w1, w3, w2)

        def merge(parts, *more):
            sums = []
            for q in range(2):
                other = swap(parts[q])
                sums.append(functools.reduce(jnp.add, [m[q] for m in more], parts[2 + q] + other))
            return sums

        x_next = after(x, pos)
        x_d, x_f = shift(x_next, (3, 3)), shift(x_next, back)
        halves = (rows // 2, rows // 2)
        near = merge(stage(out, xn_mine, xn_other, halves))
        x_d = after(x_d, *near)
        near = [shift(a, out) for a in near]
        diag = merge(stage((3, 3), x_d, swap(x_d), halves))
        x_f = after(x_f, *diag)
        via = [shift(a, out) for a in diag]
        far = merge(stage(back, x_f, swap(x_f), halves), via)
        x_o = after(x, *far)
        far = [shift(a, back) for a in far]
        sums = merge(stage((0, 0), x_o, swap(x_o), halves), near)
        width = d // 4
        part = pl.BlockSpec((rows // 2, width), lambda i: (0, i))
        return pl.pallas_call(
            _combine_kernel,
            out_shape=jax.ShapeDtypeStruct((t_loc, d), BF16),
            grid=(4,),
            in_specs=[pl.BlockSpec((t_loc, 8), lambda i: (0, 0))] + [part] * 4,
            out_specs=pl.BlockSpec((t_loc, width), lambda i: (0, i)),
            scratch_shapes=[pltpu.VMEM((top, t_loc, rows), BF16)],
            name="combine",
        )(mine, *sums, *far)

    rows = P(("ep", "tp"), None)
    return jax.shard_map(
        layer,
        mesh=mesh,
        in_specs=(rows, rows, rows, P(None), P("ep", None, "tp"), P("ep", None, "tp"), P("ep", "tp", None)),
        out_specs=rows,
        check_vma=False,
    )
```

```python
import functools

import jax
import jax.numpy as jnp
from jax import lax
from jax.experimental import pallas as pl
from jax.experimental.pallas import tpu as pltpu
from jax.sharding import PartitionSpec as P


F32 = jnp.float32
BF16 = jnp.bfloat16
VMEM_BYTES = 67_043_328


def _route_kernel(chips, turns, idx_ref, g_ref, cap_ref, x_ref, *refs):
    pos_ref, table_ref, hit_ref, gate_ref, xm_ref, xo_ref, ids_all, send_sem, recv_sem, xsend, xrecv = refs
    core, me = lax.axis_index("ep"), lax.axis_index("tp")
    blocks, top, t = ids_all.shape
    e_all = pos_ref.shape[1]
    here = core * chips + me
    mesh_id = pl.DeviceIdType.MESH
    peers = [
        (k, {"ep": jnp.bitwise_xor(core, k // chips), "tp": jnp.bitwise_xor(me, k % chips)}) for k in range(1, blocks)
    ]
    barrier = pltpu.get_barrier_semaphore()
    for _, peer in peers:
        pl.semaphore_signal(barrier, inc=1, device_id=peer, device_id_type=mesh_id)
    pl.semaphore_wait(barrier, blocks - 1)
    copies = [
        pltpu.make_async_remote_copy(
            src_ref=idx_ref,
            dst_ref=ids_all.at[here],
            send_sem=send_sem.at[k],
            recv_sem=recv_sem.at[k],
            device_id=peer,
            device_id_type=mesh_id,
        )
        for k, peer in peers
    ]
    for c in copies:
        c.start()
    pieces = xsend.shape[1]
    turn = turns[0] + (turns[1] - turns[0]) * core
    piece = x_ref.shape[0] // pieces

    def tokens(hop, i, src, dst, peer):
        part = pl.ds(i * piece, piece)
        return pltpu.make_async_remote_copy(
            src_ref=src.at[part],
            dst_ref=dst.at[part],
            send_sem=xsend.at[hop, i],
            recv_sem=xrecv.at[hop, i],
            device_id=peer,
            device_id_type=mesh_id,
        )

    arrive = [tokens(0, i, x_ref, xm_ref, {"ep": core, "tp": jnp.bitwise_xor(me, turn)}) for i in range(pieces)]
    forward = [tokens(1, i, xm_ref, xo_ref, {"ep": 1 - core, "tp": me}) for i in range(pieces)]
    for c in arrive:
        c.start()
    ids_all[pl.ds(here, 1)] = idx_ref[...][None]
    before = (
        lax.broadcasted_iota(jnp.int32, (t, t), 0) < lax.broadcasted_iota(jnp.int32, (t, t), 1)
    ).astype(F32).astype(BF16)
    ids = lax.broadcasted_iota(jnp.int32, (e_all, t), 0)
    cap = jnp.zeros((e_all, t), jnp.int32)
    for e in range(e_all):
        cap = jnp.where(ids == e, cap_ref[e], cap)
    sub, lane = (lax.broadcasted_iota(jnp.int32, (e_all, 128), i) for i in range(2))
    for c in copies:
        c.wait()

    for b in range(blocks):
        hit = (ids_all[b, 0:1, :] == ids) | (ids_all[b, 1:2, :] == ids)
        one = hit.astype(F32)
        rank = jnp.dot(one.astype(BF16), before, preferred_element_type=F32).astype(jnp.int32)
        total = jnp.sum(one, axis=1, keepdims=True).astype(jnp.int32)
        count = jnp.minimum(jnp.broadcast_to(total, (e_all, t)), cap)
        first = jnp.zeros_like(count)
        for e in range(e_all - 1):
            first = first + jnp.where(ids > e, jnp.broadcast_to(count[e : e + 1, :], count.shape), 0)
        pair = jnp.where(lane == sub, first[:, :128], 0) + jnp.where(lane == sub + e_all, count[:, :128], 0)
        table_ref[pl.ds(b, 1)] = jnp.sum(pair, axis=0, keepdims=True)
        pos_ref[b] = jnp.where(hit & (rank < cap), first + rank, -1)
    pos = pos_ref[here]
    lines = [
        jnp.max(jnp.where(idx_ref[j : j + 1, :] == ids, pos, -1), axis=0, keepdims=True).astype(F32) for j in range(top)
    ]
    lines += [g_ref[j : j + 1, :] for j in range(top)]
    table = jnp.concatenate(lines + [jnp.zeros((8 - 2 * top, t), F32)], axis=0)
    table = jnp.transpose(table)
    gate_ref[...] = table
    row = lax.broadcasted_iota(jnp.int32, hit_ref.shape[1:], 1)
    for j in range(top):
        hit_ref[j] = (row == table[:, j : j + 1].astype(jnp.int32)).astype(F32).astype(BF16)
    for c, f in zip(arrive, forward):
        c.wait_recv()
        f.start()
    for c, f in zip(arrive, forward):
        c.wait_send()
        f.wait()


def _expert_kernel(
    turns, sizes, cuts, table_ref, pos_ref, xm_hbm, xo_hbm, w1_hbm, w3_hbm, w2_hbm, *refs
):
    outs = refs[:4]
    acc, xbuf, *ws, w2s, wsem, osem, xsem = refs[4:]
    w1s, w3s = ws[: len(ws) // 2], ws[len(ws) // 2 :]
    ahead = 2
    e_loc, d, _ = w1_hbm.shape
    _, rows, _ = acc.shape
    t = xbuf.shape[1]
    half_d = d // 2
    core, me = lax.axis_index("ep"), lax.axis_index("tp")
    chips = pos_ref.shape[0] // 2
    blocks = []
    for c in (core, 1 - core):
        turn = jnp.where(c == 0, turns[0], turns[1])
        blocks.append(c * chips + jnp.bitwise_xor(me, turn))

    def columns(k):
        def copies(e):
            cols, b = pl.ds(cuts[k], cuts[k + 1] - cuts[k]), e % 2
            return [
                pltpu.make_async_copy(w1_hbm.at[e, :, cols], w1s[k].at[b], wsem.at[b, 2 * k]),
                pltpu.make_async_copy(w3_hbm.at[e, :, cols], w3s[k].at[b], wsem.at[b, 2 * k + 1]),
            ]

        return copies

    def output(k):
        def copies(e):
            cols, b = pl.ds(pl.multiple_of(k * half_d, half_d), half_d), e % 2
            return [pltpu.make_async_copy(w2_hbm.at[e, :, cols], w2s.at[b, k], wsem.at[b, 2 * len(w1s) + k])]

        return copies

    chunks = [columns(k) for k in range(len(w1s))] + [output(k) for k in range(2)]

    def arrive(i, e):
        for c in chunks[i](e):
            c.wait()
        i += ahead
        if i < len(chunks):
            for c in chunks[i](e):
                c.start()
        else:

            @pl.when(e + 1 < e_loc)
            def _():
                for c in chunks[i - len(chunks)](e + 1):
                    c.start()

    def out_copies(h):
        cols = pl.ds(h * half_d, half_d)
        copies = []
        for i in range(4):
            size = outs[i].shape[0]
            part = pl.ds(0 if i % 2 == 0 else rows - size, size)
            copies.append(pltpu.make_async_copy(acc.at[1 - i // 2, part, cols], outs[i].at[:, cols], osem.at[h, i]))
        return copies

    tokens = [
        pltpu.make_async_copy(xm_hbm, xbuf.at[0], xsem.at[0]),
        pltpu.make_async_copy(xo_hbm, xbuf.at[1], xsem.at[1]),
    ]
    for c in tokens:
        c.start()
    for i in range(ahead):
        for c in chunks[i](0):
            c.start()
    acc[...] = jnp.zeros_like(acc)
    for c in tokens:
        c.wait()

    def step(e, carry):
        expert = core * e_loc + e
        offs = [table_ref[b, expert] for b in blocks]
        cnts = [table_ref[b, 2 * e_loc + expert] for b in blocks]
        need = functools.reduce(jnp.maximum, [jnp.where(k > 0, o - o // 8 * 8 + k, 0) for o, k in zip(offs, cnts)])

        def last(k):
            @pl.when((e == e_loc - 1) & (k == 0))
            def _():
                for c in out_copies(0):
                    c.start()

        def run(m):
            bases = [pl.multiple_of(jnp.minimum(o // 8 * 8, rows - m), 8) for o in offs]
            parts = []
            for s in range(2):
                row = lax.broadcasted_iota(jnp.int32, (m, t), 0) + bases[s]
                hit = (row == pos_ref[blocks[s], pl.ds(expert, 1), :]).astype(F32).astype(BF16)
                parts.append(jnp.dot(hit, xbuf[s], preferred_element_type=F32))
            xs = jnp.concatenate(parts, axis=0).astype(BF16)
            hs = []
            for i, (wa, wb) in enumerate(zip(w1s, w3s)):
                arrive(i, e)
                h1 = jnp.dot(xs, wa[e % 2], preferred_element_type=F32)
                h3 = jnp.dot(xs, wb[e % 2], preferred_element_type=F32)
                hs.append((jax.nn.silu(h1) * h3).astype(BF16))
            h = jnp.concatenate(hs, axis=1)

            def project(k, carry):
                for i in range(2):
                    pl.when(k == i)(functools.partial(arrive, len(w1s) + i, e))
                p = jnp.dot(h, w2s[e % 2, k], preferred_element_type=F32)
                cols = pl.ds(pl.multiple_of(k * half_d, half_d), half_d)
                for s in range(2):
                    acc[s, pl.ds(bases[s], m), cols] += p[s * m : (s + 1) * m]
                last(k)
                return carry

            lax.fori_loop(0, 2, project, 0)

        @pl.when(need == 0)
        def _():
            for i in range(len(chunks)):
                arrive(i, e)
            last(0)

        lo = 0
        for m in sizes:
            pl.when((need > lo) & (need <= m))(functools.partial(run, m))
            lo = m
        return carry

    lax.fori_loop(0, e_loc, step, 0)
    for c in out_copies(1):
        c.start()
    for c in out_copies(0) + out_copies(1):
        c.wait()


def _combine_kernel(hit_ref, gate_ref, s0_ref, s1_ref, f0_ref, f1_ref, out_ref):
    top = hit_ref.shape[0]
    y = jnp.concatenate([s0_ref[...] + f0_ref[...], s1_ref[...] + f1_ref[...]], axis=0).astype(BF16)
    total = None
    for j in range(top):
        part = jnp.dot(hit_ref[j], y, preferred_element_type=F32) * gate_ref[:, top + j : top + j + 1]
        total = part if total is None else total + part
    out_ref[...] = total.astype(out_ref.dtype)


def solution(mesh):
    chips = mesh.shape["tp"]
    vmem = pl.BlockSpec(memory_space=pltpu.VMEM)
    anym = pl.BlockSpec(memory_space=pl.ANY)
    smem = pl.BlockSpec(memory_space=pltpu.SMEM)

    def layer(x, idx, g, cap, w1, w3, w2):
        t_loc, d = x.shape
        top = idx.shape[1]
        e_all = cap.shape[0]
        e_loc, _, ff = w1.shape
        c = (5 * top * t_loc // (2 * e_all) + 7) // 8 * 8
        rows = top * t_loc
        cuts = (0, 512, 1024, ff)
        widths = [b - a for a, b in zip(cuts, cuts[1:])]
        blocks = 2 * chips

        def swap(a):
            return lax.ppermute(a, "ep", [(0, 1), (1, 0)])

        def shift(a, turns):
            pairs = [(2 * k + i, 2 * (k ^ turns[i]) + i) for k in range(chips) for i in range(2)]
            return lax.ppermute(a, ("tp", "ep"), pairs)

        def after(a, *first):
            return lax.optimization_barrier((a, *first))[0]

        out, back = (1, 2), (2, 1)
        pieces = 4
        pos, groups, hit, gate, xn_mine, xn_other = pl.pallas_call(
            functools.partial(_route_kernel, chips, out),
            out_shape=[
                jax.ShapeDtypeStruct((blocks, e_all, t_loc), jnp.int32),
                jax.ShapeDtypeStruct((blocks, 128), jnp.int32),
                jax.ShapeDtypeStruct((top, t_loc, rows), BF16),
                jax.ShapeDtypeStruct((t_loc, 8), F32),
                jax.ShapeDtypeStruct((t_loc, d), BF16),
                jax.ShapeDtypeStruct((t_loc, d), BF16),
            ],
            in_specs=[vmem, vmem, smem, anym],
            out_specs=[vmem] * 4 + [anym] * 2,
            scratch_shapes=[
                pltpu.VMEM((blocks, top, t_loc), jnp.int32),
                pltpu.SemaphoreType.DMA((blocks,)),
                pltpu.SemaphoreType.DMA((blocks,)),
                pltpu.SemaphoreType.DMA((2, pieces)),
                pltpu.SemaphoreType.DMA((2, pieces)),
            ],
            compiler_params=pltpu.CompilerParams(collective_id=0, has_side_effects=True, vmem_limit_bytes=VMEM_BYTES),
            name="route",
        )(idx.T, g.T, cap, x)

        sizes = (64, (c + 7 + 7) // 8 * 8)

        def stage(turns, mine, other, split):
            return pl.pallas_call(
                functools.partial(_expert_kernel, turns, sizes, cuts),
                out_shape=[jax.ShapeDtypeStruct((n, d), F32) for n in split * 2],
                in_specs=[smem, vmem] + [anym] * 5,
                out_specs=[anym] * 4,
                scratch_shapes=[
                    pltpu.VMEM((2, rows, d), F32),
                    pltpu.VMEM((2, t_loc, d), BF16),
                    *[pltpu.VMEM((2, d, w), BF16) for w in widths * 2],
                    pltpu.VMEM((2, 2, ff, d // 2), BF16),
                    pltpu.SemaphoreType.DMA((2, 2 * len(widths) + 2)),
                    pltpu.SemaphoreType.DMA((2, 4)),
                    pltpu.SemaphoreType.DMA((2,)),
                ],
                compiler_params=pltpu.CompilerParams(vmem_limit_bytes=VMEM_BYTES),
                cost_estimate=pl.CostEstimate(
                    flops=6 * rows * d * ff, bytes_accessed=6 * e_loc * d * ff + 8 * rows * d, transcendentals=0
                ),
            )(groups, pos, mine, other, w1, w3, w2)

        def merge(parts, *more):
            sums = []
            for q in range(2):
                other = swap(parts[q])
                sums.append(functools.reduce(jnp.add, [m[q] for m in more], parts[2 + q] + other))
            return sums

        x_next = after(x, pos)
        x_d, x_f = shift(x_next, (3, 3)), shift(x_next, back)
        halves = (rows // 2, rows // 2)
        near = merge(stage(out, xn_mine, xn_other, halves))
        x_d = after(x_d, *near)
        near = [shift(a, out) for a in near]
        diag = merge(stage((3, 3), x_d, swap(x_d), halves))
        x_f = after(x_f, *diag)
        via = [shift(a, out) for a in diag]
        far = merge(stage(back, x_f, swap(x_f), halves), via)
        x_o = after(x, *far)
        far = [shift(a, back) for a in far]
        sums = merge(stage((0, 0), x_o, swap(x_o), halves), near)
        steps = 8
        part = pl.BlockSpec((rows // 2, d // steps), lambda i: (0, i))
        return pl.pallas_call(
            _combine_kernel,
            out_shape=jax.ShapeDtypeStruct((t_loc, d), BF16),
            grid=(steps,),
            in_specs=[vmem, vmem] + [part] * 4,
            out_specs=pl.BlockSpec((t_loc, d // steps), lambda i: (0, i)),
            name="combine",
        )(hit, gate, *sums, *far)

    rows = P(("ep", "tp"), None)
    return jax.shard_map(
        layer,
        mesh=mesh,
        in_specs=(rows, rows, rows, P(None), P("ep", None, "tp"), P("ep", None, "tp"), P("ep", "tp", None)),
        out_specs=rows,
        check_vma=False,
    )
```

```python
import functools

import jax
import jax.numpy as jnp
from jax import lax
from jax.experimental import pallas as pl
from jax.experimental.pallas import tpu as pltpu
from jax.sharding import PartitionSpec as P


F32 = jnp.float32
BF16 = jnp.bfloat16
VMEM_BYTES = 67_043_328


def _route_kernel(chips, turns, idx_ref, g_ref, cap_ref, x_ref, *refs):
    pos_ref, table_ref, hit_ref, gate_ref, pair_ref, xo_ref, ids_all, held, landed, send_sem, recv_sem, xsend, xrecv, lsem = refs
    core, me = lax.axis_index("ep"), lax.axis_index("tp")
    blocks, top, t = ids_all.shape
    e_all = pos_ref.shape[1]
    here = core * chips + me
    mesh_id = pl.DeviceIdType.MESH
    peers = [
        (k, {"ep": jnp.bitwise_xor(core, k // chips), "tp": jnp.bitwise_xor(me, k % chips)}) for k in range(1, blocks)
    ]
    load = pltpu.make_async_copy(x_ref, held, lsem.at[0])
    load.start()
    barrier = pltpu.get_barrier_semaphore()
    for _, peer in peers:
        pl.semaphore_signal(barrier, inc=1, device_id=peer, device_id_type=mesh_id)
    pl.semaphore_wait(barrier, blocks - 1)
    copies = [
        pltpu.make_async_remote_copy(
            src_ref=idx_ref,
            dst_ref=ids_all.at[here],
            send_sem=send_sem.at[k],
            recv_sem=recv_sem.at[k],
            device_id=peer,
            device_id_type=mesh_id,
        )
        for k, peer in peers
    ]
    for c in copies:
        c.start()
    pieces = xsend.shape[1]
    turn = turns[0] + (turns[1] - turns[0]) * core
    piece = x_ref.shape[0] // pieces

    def tokens(hop, i, src, dst, peer):
        part = pl.ds(i * piece, piece)
        return pltpu.make_async_remote_copy(
            src_ref=src.at[part],
            dst_ref=dst.at[part],
            send_sem=xsend.at[hop, i],
            recv_sem=xrecv.at[hop, i],
            device_id=peer,
            device_id_type=mesh_id,
        )

    arrive = [tokens(0, i, held, landed, {"ep": core, "tp": jnp.bitwise_xor(me, turn)}) for i in range(pieces)]
    forward = [tokens(1, i, landed, xo_ref, {"ep": 1 - core, "tp": me}) for i in range(pieces)]
    keep = [
        pltpu.make_async_copy(
            landed.at[pl.ds(i * piece, piece)], pair_ref.at[pl.ds(i * piece, piece)], lsem.at[2 + i]
        )
        for i in range(pieces)
    ]
    own = pltpu.make_async_copy(held, pair_ref.at[pl.ds(t, t)], lsem.at[1])
    load.wait()
    for c in arrive:
        c.start()
    own.start()
    ids_all[pl.ds(here, 1)] = idx_ref[...][None]
    before = (
        lax.broadcasted_iota(jnp.int32, (t, t), 0) < lax.broadcasted_iota(jnp.int32, (t, t), 1)
    ).astype(F32).astype(BF16)
    ids = lax.broadcasted_iota(jnp.int32, (e_all, t), 0)
    cap = jnp.zeros((e_all, t), jnp.int32)
    for e in range(e_all):
        cap = jnp.where(ids == e, cap_ref[e], cap)
    sub, lane = (lax.broadcasted_iota(jnp.int32, (e_all, 128), i) for i in range(2))
    for c in copies:
        c.wait()

    for b in range(blocks):
        hit = (ids_all[b, 0:1, :] == ids) | (ids_all[b, 1:2, :] == ids)
        one = hit.astype(F32)
        rank = jnp.dot(one.astype(BF16), before, preferred_element_type=F32).astype(jnp.int32)
        total = jnp.sum(one, axis=1, keepdims=True).astype(jnp.int32)
        count = jnp.minimum(jnp.broadcast_to(total, (e_all, t)), cap)
        first = jnp.zeros_like(count)
        for e in range(e_all - 1):
            first = first + jnp.where(ids > e, jnp.broadcast_to(count[e : e + 1, :], count.shape), 0)
        pair = jnp.where(lane == sub, first[:, :128], 0) + jnp.where(lane == sub + e_all, count[:, :128], 0)
        table_ref[pl.ds(b, 1)] = jnp.sum(pair, axis=0, keepdims=True)
        pos_ref[b] = jnp.where(hit & (rank < cap), first + rank, -1)
    pos = pos_ref[here]
    lines = [
        jnp.max(jnp.where(idx_ref[j : j + 1, :] == ids, pos, -1), axis=0, keepdims=True).astype(F32) for j in range(top)
    ]
    lines += [g_ref[j : j + 1, :] for j in range(top)]
    table = jnp.concatenate(lines + [jnp.zeros((8 - 2 * top, t), F32)], axis=0)
    table = jnp.transpose(table)
    gate_ref[...] = table
    row = lax.broadcasted_iota(jnp.int32, hit_ref.shape[1:], 1)
    for j in range(top):
        hit_ref[j] = (row == table[:, j : j + 1].astype(jnp.int32)).astype(F32).astype(BF16)
    for c, f, k in zip(arrive, forward, keep):
        c.wait_recv()
        f.start()
        k.start()
    for c, f, k in zip(arrive, forward, keep):
        c.wait_send()
        k.wait()
        f.wait()
    own.wait()


def _expert_kernel(
    turns, rows0, sizes, cuts, table_ref, pos_ref, xm_hbm, xo_hbm, w1_hbm, w3_hbm, w2_hbm, *refs
):
    outs = refs[:4]
    acc, xbuf, *ws, w2s, wsem, osem, xsem = refs[4:]
    w1s, w3s = ws[: len(ws) // 2], ws[len(ws) // 2 :]
    ahead = len(w1s) + 2
    e_loc, d, _ = w1_hbm.shape
    _, rows, _ = acc.shape
    t = xbuf.shape[1]
    half_d = d // 2
    core, me = lax.axis_index("ep"), lax.axis_index("tp")
    chips = pos_ref.shape[0] // 2
    blocks = []
    for c in (core, 1 - core):
        turn = jnp.where(c == 0, turns[0], turns[1])
        blocks.append(c * chips + jnp.bitwise_xor(me, turn))

    def columns(k):
        def copies(e):
            cols, b = pl.ds(cuts[k], cuts[k + 1] - cuts[k]), e % 2
            return [
                pltpu.make_async_copy(w1_hbm.at[e, :, cols], w1s[k].at[b], wsem.at[b, 2 * k]),
                pltpu.make_async_copy(w3_hbm.at[e, :, cols], w3s[k].at[b], wsem.at[b, 2 * k + 1]),
            ]

        return copies

    def output(k):
        def copies(e):
            cols, b = pl.ds(pl.multiple_of(k * half_d, half_d), half_d), e % 2
            return [pltpu.make_async_copy(w2_hbm.at[e, :, cols], w2s.at[b, k], wsem.at[b, 2 * len(w1s) + k])]

        return copies

    chunks = [columns(k) for k in range(len(w1s))] + [output(k) for k in range(2)]

    def arrive(i, e):
        for c in chunks[i](e):
            c.wait()
        i += ahead
        if i < len(chunks):
            for c in chunks[i](e):
                c.start()
        else:

            @pl.when(e + 1 < e_loc)
            def _():
                for c in chunks[i - len(chunks)](e + 1):
                    c.start()

    def out_copies(h):
        cols = pl.ds(h * half_d, half_d)
        copies = []
        for i in range(4):
            size = outs[i].shape[0]
            part = pl.ds(0 if i % 2 == 0 else rows - size, size)
            copies.append(pltpu.make_async_copy(acc.at[1 - i // 2, part, cols], outs[i].at[:, cols], osem.at[h, i]))
        return copies

    tokens = [
        pltpu.make_async_copy(ref.at[pl.ds(rows0[i], t)], xbuf.at[i], xsem.at[i]) for i, ref in enumerate((xm_hbm, xo_hbm))
    ]
    for c in tokens:
        c.start()
    for i in range(ahead):
        for c in chunks[i](0):
            c.start()
    acc[...] = jnp.zeros_like(acc)
    for c in tokens:
        c.wait()

    def step(e, carry):
        expert = core * e_loc + e
        offs = [table_ref[b, expert] for b in blocks]
        cnts = [table_ref[b, 2 * e_loc + expert] for b in blocks]
        need = functools.reduce(jnp.maximum, [jnp.where(k > 0, o - o // 8 * 8 + k, 0) for o, k in zip(offs, cnts)])

        def last(k):
            @pl.when((e == e_loc - 1) & (k == 0))
            def _():
                for c in out_copies(0):
                    c.start()

        def run(m):
            bases = [pl.multiple_of(jnp.minimum(o // 8 * 8, rows - m), 8) for o in offs]
            parts = []
            for s in range(2):
                row = lax.broadcasted_iota(jnp.int32, (m, t), 0) + bases[s]
                hit = (row == pos_ref[blocks[s], pl.ds(expert, 1), :]).astype(F32).astype(BF16)
                parts.append(jnp.dot(hit, xbuf[s], preferred_element_type=F32))
            xs = jnp.concatenate(parts, axis=0).astype(BF16)
            hs = []
            for i, (wa, wb) in enumerate(zip(w1s, w3s)):
                arrive(i, e)
                h1 = jnp.dot(xs, wa[e % 2], preferred_element_type=F32)
                h3 = jnp.dot(xs, wb[e % 2], preferred_element_type=F32)
                hs.append((jax.nn.silu(h1) * h3).astype(BF16))
            h = jnp.concatenate(hs, axis=1)

            def project(k, carry):
                for i in range(2):
                    pl.when(k == i)(functools.partial(arrive, len(w1s) + i, e))
                p = jnp.dot(h, w2s[e % 2, k], preferred_element_type=F32)
                cols = pl.ds(pl.multiple_of(k * half_d, half_d), half_d)
                for s in range(2):
                    acc[s, pl.ds(bases[s], m), cols] += p[s * m : (s + 1) * m]
                last(k)
                return carry

            lax.fori_loop(0, 2, project, 0)

        @pl.when(need == 0)
        def _():
            for i in range(len(chunks)):
                arrive(i, e)
            last(0)

        lo = 0
        for m in sizes:
            pl.when((need > lo) & (need <= m))(functools.partial(run, m))
            lo = m
        return carry

    lax.fori_loop(0, e_loc, step, 0)
    for c in out_copies(1):
        c.start()
    for c in out_copies(0) + out_copies(1):
        c.wait()


def _combine_kernel(hit_ref, gate_ref, s0_ref, s1_ref, f0_ref, f1_ref, out_ref):
    top = hit_ref.shape[0]
    y = jnp.concatenate([s0_ref[...] + f0_ref[...], s1_ref[...] + f1_ref[...]], axis=0).astype(BF16)
    total = None
    for j in range(top):
        part = jnp.dot(hit_ref[j], y, preferred_element_type=F32) * gate_ref[:, top + j : top + j + 1]
        total = part if total is None else total + part
    out_ref[...] = total.astype(out_ref.dtype)


def solution(mesh):
    chips = mesh.shape["tp"]
    vmem = pl.BlockSpec(memory_space=pltpu.VMEM)
    anym = pl.BlockSpec(memory_space=pl.ANY)
    smem = pl.BlockSpec(memory_space=pltpu.SMEM)

    def layer(x, idx, g, cap, w1, w3, w2):
        t_loc, d = x.shape
        top = idx.shape[1]
        e_all = cap.shape[0]
        e_loc, _, ff = w1.shape
        c = (5 * top * t_loc // (2 * e_all) + 7) // 8 * 8
        rows = top * t_loc
        cuts = (0, 512, ff)
        widths = [b - a for a, b in zip(cuts, cuts[1:])]
        blocks = 2 * chips

        def swap(a):
            return lax.ppermute(a, "ep", [(0, 1), (1, 0)])

        def shift(a, turns):
            pairs = [(2 * k + i, 2 * (k ^ turns[i]) + i) for k in range(chips) for i in range(2)]
            return lax.ppermute(a, ("tp", "ep"), pairs)

        out, back = (1, 2), (2, 1)
        pieces = 4
        pos, groups, hit, gate, pair, x_near = pl.pallas_call(
            functools.partial(_route_kernel, chips, out),
            out_shape=[
                jax.ShapeDtypeStruct((blocks, e_all, t_loc), jnp.int32),
                jax.ShapeDtypeStruct((blocks, 128), jnp.int32),
                jax.ShapeDtypeStruct((top, t_loc, rows), BF16),
                jax.ShapeDtypeStruct((t_loc, 8), F32),
                jax.ShapeDtypeStruct((2 * t_loc, d), BF16),
                jax.ShapeDtypeStruct((t_loc, d), BF16),
            ],
            in_specs=[vmem, vmem, smem, anym],
            out_specs=[vmem] * 4 + [anym] * 2,
            scratch_shapes=[
                pltpu.VMEM((blocks, top, t_loc), jnp.int32),
                pltpu.VMEM((t_loc, d), BF16),
                pltpu.VMEM((t_loc, d), BF16),
                pltpu.SemaphoreType.DMA((blocks,)),
                pltpu.SemaphoreType.DMA((blocks,)),
                pltpu.SemaphoreType.DMA((2, pieces)),
                pltpu.SemaphoreType.DMA((2, pieces)),
                pltpu.SemaphoreType.DMA((2 + pieces,)),
            ],
            compiler_params=pltpu.CompilerParams(collective_id=0, has_side_effects=True, vmem_limit_bytes=VMEM_BYTES),
            name="route",
        )(idx.T, g.T, cap, x)

        sizes = (64, (c + 7 + 7) // 8 * 8)

        def stage(turns, mine, other, split, rows0=(0, 0)):
            return pl.pallas_call(
                functools.partial(_expert_kernel, turns, rows0, sizes, cuts),
                out_shape=[jax.ShapeDtypeStruct((n, d), F32) for n in split * 2],
                in_specs=[smem, vmem] + [anym] * 5,
                out_specs=[anym] * 4,
                scratch_shapes=[
                    pltpu.VMEM((2, rows, d), F32),
                    pltpu.VMEM((2, t_loc, d), BF16),
                    *[pltpu.VMEM((2, d, w), BF16) for w in widths * 2],
                    pltpu.VMEM((2, 2, ff, d // 2), BF16),
                    pltpu.SemaphoreType.DMA((2, 2 * len(widths) + 2)),
                    pltpu.SemaphoreType.DMA((2, 4)),
                    pltpu.SemaphoreType.DMA((2,)),
                ],
                compiler_params=pltpu.CompilerParams(vmem_limit_bytes=VMEM_BYTES),
                cost_estimate=pl.CostEstimate(
                    flops=6 * rows * d * ff, bytes_accessed=6 * e_loc * d * ff + 8 * rows * d, transcendentals=0
                ),
            )(groups, pos, mine, other, w1, w3, w2)

        def merge(parts, *more):
            sums = []
            for q in range(2):
                other = swap(parts[q])
                sums.append(functools.reduce(jnp.add, [m[q] for m in more], parts[2 + q] + other))
            return sums

        halves, early = (rows // 2, rows // 2), (rows // 4, rows - rows // 4)
        rest = shift(pair, back)
        rest_other = swap(rest)
        own_x = swap(x)
        near = merge(stage(out, pair, x_near, early))
        near = [shift(a, out) for a in near]
        diag = merge(stage((3, 3), rest, rest_other, halves))
        via = [shift(a, out) for a in diag]
        far = merge(stage(back, rest, rest_other, halves, (t_loc, t_loc)), via)
        far = [shift(a, back) for a in far]
        near = jnp.concatenate(near, axis=0)
        near = [near[: halves[0]], near[halves[0] :]]
        sums = merge(stage((0, 0), x, own_x, halves), near)
        steps = 4
        part = pl.BlockSpec((rows // 2, d // steps), lambda i: (0, i))
        return pl.pallas_call(
            _combine_kernel,
            out_shape=jax.ShapeDtypeStruct((t_loc, d), BF16),
            grid=(steps,),
            in_specs=[vmem, vmem] + [part] * 4,
            out_specs=pl.BlockSpec((t_loc, d // steps), lambda i: (0, i)),
            name="combine",
        )(hit, gate, *sums, *far)

    rows = P(("ep", "tp"), None)
    return jax.shard_map(
        layer,
        mesh=mesh,
        in_specs=(rows, rows, rows, P(None), P("ep", None, "tp"), P("ep", None, "tp"), P("ep", "tp", None)),
        out_specs=rows,
        check_vma=False,
    )
```

```python
import functools

import jax
import jax.numpy as jnp
from jax import lax
from jax.experimental import pallas as pl
from jax.experimental.pallas import tpu as pltpu
from jax.sharding import PartitionSpec as P


F32 = jnp.float32
BF16 = jnp.bfloat16
VMEM_BYTES = 67_043_328


def _route_kernel(chips, turns, idx_ref, g_ref, cap_ref, x_ref, *refs):
    pos_ref, table_ref, hit_ref, gate_ref, pair_ref, xo_ref, ids_all, held, landed, send_sem, recv_sem, xsend, xrecv, lsem = refs
    core, me = lax.axis_index("ep"), lax.axis_index("tp")
    blocks, top, t = ids_all.shape
    e_all = pos_ref.shape[1]
    here = core * chips + me
    mesh_id = pl.DeviceIdType.MESH
    peers = [
        (k, {"ep": jnp.bitwise_xor(core, k // chips), "tp": jnp.bitwise_xor(me, k % chips)}) for k in range(1, blocks)
    ]
    load = pltpu.make_async_copy(x_ref, held, lsem.at[0])
    load.start()
    barrier = pltpu.get_barrier_semaphore()
    for _, peer in peers:
        pl.semaphore_signal(barrier, inc=1, device_id=peer, device_id_type=mesh_id)
    pl.semaphore_wait(barrier, blocks - 1)
    copies = [
        pltpu.make_async_remote_copy(
            src_ref=idx_ref,
            dst_ref=ids_all.at[here],
            send_sem=send_sem.at[k],
            recv_sem=recv_sem.at[k],
            device_id=peer,
            device_id_type=mesh_id,
        )
        for k, peer in peers
    ]
    for c in copies:
        c.start()
    pieces = xsend.shape[1]
    turn = turns[0] + (turns[1] - turns[0]) * core
    piece = x_ref.shape[0] // pieces

    def tokens(hop, i, src, dst, peer):
        part = pl.ds(i * piece, piece)
        return pltpu.make_async_remote_copy(
            src_ref=src.at[part],
            dst_ref=dst.at[part],
            send_sem=xsend.at[hop, i],
            recv_sem=xrecv.at[hop, i],
            device_id=peer,
            device_id_type=mesh_id,
        )

    arrive = [tokens(0, i, held, landed, {"ep": core, "tp": jnp.bitwise_xor(me, turn)}) for i in range(pieces)]
    forward = [tokens(1, i, landed, xo_ref, {"ep": 1 - core, "tp": me}) for i in range(pieces)]
    keep = [
        pltpu.make_async_copy(
            landed.at[pl.ds(i * piece, piece)], pair_ref.at[pl.ds(i * piece, piece)], lsem.at[2 + i]
        )
        for i in range(pieces)
    ]
    own = pltpu.make_async_copy(held, pair_ref.at[pl.ds(t, t)], lsem.at[1])
    load.wait()
    for c in arrive:
        c.start()
    own.start()
    ids_all[pl.ds(here, 1)] = idx_ref[...][None]
    before = (
        lax.broadcasted_iota(jnp.int32, (t, t), 0) < lax.broadcasted_iota(jnp.int32, (t, t), 1)
    ).astype(F32).astype(BF16)
    ids = lax.broadcasted_iota(jnp.int32, (e_all, t), 0)
    cap = jnp.zeros((e_all, t), jnp.int32)
    for e in range(e_all):
        cap = jnp.where(ids == e, cap_ref[e], cap)
    sub, lane = (lax.broadcasted_iota(jnp.int32, (e_all, 128), i) for i in range(2))
    for c in copies:
        c.wait()

    for b in range(blocks):
        hit = (ids_all[b, 0:1, :] == ids) | (ids_all[b, 1:2, :] == ids)
        one = hit.astype(F32)
        rank = jnp.dot(one.astype(BF16), before, preferred_element_type=F32).astype(jnp.int32)
        total = jnp.sum(one, axis=1, keepdims=True).astype(jnp.int32)
        count = jnp.minimum(jnp.broadcast_to(total, (e_all, t)), cap)
        first = jnp.zeros_like(count)
        for e in range(e_all - 1):
            first = first + jnp.where(ids > e, jnp.broadcast_to(count[e : e + 1, :], count.shape), 0)
        pair = jnp.where(lane == sub, first[:, :128], 0) + jnp.where(lane == sub + e_all, count[:, :128], 0)
        table_ref[pl.ds(b, 1)] = jnp.sum(pair, axis=0, keepdims=True)
        pos_ref[b] = jnp.where(hit & (rank < cap), first + rank, -1)
    pos = pos_ref[here]
    lines = [
        jnp.max(jnp.where(idx_ref[j : j + 1, :] == ids, pos, -1), axis=0, keepdims=True).astype(F32) for j in range(top)
    ]
    lines += [g_ref[j : j + 1, :] for j in range(top)]
    table = jnp.concatenate(lines + [jnp.zeros((8 - 2 * top, t), F32)], axis=0)
    table = jnp.transpose(table)
    gate_ref[...] = table
    row = lax.broadcasted_iota(jnp.int32, hit_ref.shape[1:], 1)
    for j in range(top):
        hit_ref[j] = (row == table[:, j : j + 1].astype(jnp.int32)).astype(F32).astype(BF16)
    for c, f, k in zip(arrive, forward, keep):
        c.wait_recv()
        f.start()
        k.start()
    for c, f, k in zip(arrive, forward, keep):
        c.wait_send()
        k.wait()
        f.wait()
    own.wait()


def _expert_kernel(
    turns, rows0, sizes, cuts, table_ref, pos_ref, xm_hbm, xo_hbm, w1_hbm, w3_hbm, w2_hbm, *refs
):
    outs = refs[:4]
    acc, xbuf, *ws, w2s, wsem, osem, xsem = refs[4:]
    w1s, w3s = ws[: len(ws) // 2], ws[len(ws) // 2 :]
    ahead = len(w1s) + 2
    e_loc, d, _ = w1_hbm.shape
    _, rows, _ = acc.shape
    t = xbuf.shape[1]
    half_d = d // 2
    core, me = lax.axis_index("ep"), lax.axis_index("tp")
    chips = pos_ref.shape[0] // 2
    blocks = []
    for c in (core, 1 - core):
        turn = jnp.where(c == 0, turns[0], turns[1])
        blocks.append(c * chips + jnp.bitwise_xor(me, turn))

    def columns(k):
        def copies(e):
            cols, b = pl.ds(cuts[k], cuts[k + 1] - cuts[k]), e % 2
            return [
                pltpu.make_async_copy(w1_hbm.at[e, :, cols], w1s[k].at[b], wsem.at[b, 2 * k]),
                pltpu.make_async_copy(w3_hbm.at[e, :, cols], w3s[k].at[b], wsem.at[b, 2 * k + 1]),
            ]

        return copies

    def output(k):
        def copies(e):
            cols, b = pl.ds(pl.multiple_of(k * half_d, half_d), half_d), e % 2
            return [pltpu.make_async_copy(w2_hbm.at[e, :, cols], w2s.at[b, k], wsem.at[b, 2 * len(w1s) + k])]

        return copies

    chunks = [columns(k) for k in range(len(w1s))] + [output(k) for k in range(2)]

    def arrive(i, e):
        for c in chunks[i](e):
            c.wait()
        i += ahead
        if i < len(chunks):
            for c in chunks[i](e):
                c.start()
        else:

            @pl.when(e + 1 < e_loc)
            def _():
                for c in chunks[i - len(chunks)](e + 1):
                    c.start()

    def out_copies(h):
        cols = pl.ds(h * half_d, half_d)
        copies = []
        for i in range(4):
            size = outs[i].shape[0]
            part = pl.ds(0 if i % 2 == 0 else rows - size, size)
            copies.append(pltpu.make_async_copy(acc.at[1 - i // 2, part, cols], outs[i].at[:, cols], osem.at[h, i]))
        return copies

    tokens = [
        pltpu.make_async_copy(ref.at[pl.ds(rows0[i], t)], xbuf.at[i], xsem.at[i]) for i, ref in enumerate((xm_hbm, xo_hbm))
    ]
    for c in tokens:
        c.start()
    for i in range(ahead):
        for c in chunks[i](0):
            c.start()
    acc[...] = jnp.zeros_like(acc)
    for c in tokens:
        c.wait()

    def step(e, carry):
        expert = core * e_loc + e
        offs = [table_ref[b, expert] for b in blocks]
        cnts = [table_ref[b, 2 * e_loc + expert] for b in blocks]
        need = functools.reduce(jnp.maximum, [jnp.where(k > 0, o - o // 8 * 8 + k, 0) for o, k in zip(offs, cnts)])

        def last(k):
            @pl.when((e == e_loc - 1) & (k == 0))
            def _():
                for c in out_copies(0):
                    c.start()

        def run(m):
            bases = [pl.multiple_of(jnp.minimum(o // 8 * 8, rows - m), 8) for o in offs]
            parts = []
            for s in range(2):
                row = lax.broadcasted_iota(jnp.int32, (m, t), 0) + bases[s]
                hit = (row == pos_ref[blocks[s], pl.ds(expert, 1), :]).astype(F32).astype(BF16)
                parts.append(jnp.dot(hit, xbuf[s], preferred_element_type=F32))
            xs = jnp.concatenate(parts, axis=0).astype(BF16)
            hs = []
            for i, (wa, wb) in enumerate(zip(w1s, w3s)):
                arrive(i, e)
                h1 = jnp.dot(xs, wa[e % 2], preferred_element_type=F32)
                h3 = jnp.dot(xs, wb[e % 2], preferred_element_type=F32)
                hs.append((jax.nn.silu(h1) * h3).astype(BF16))
            h = jnp.concatenate(hs, axis=1)

            def project(k, carry):
                for i in range(2):
                    pl.when(k == i)(functools.partial(arrive, len(w1s) + i, e))
                p = jnp.dot(h, w2s[e % 2, k], preferred_element_type=F32)
                cols = pl.ds(pl.multiple_of(k * half_d, half_d), half_d)
                for s in range(2):
                    acc[s, pl.ds(bases[s], m), cols] += p[s * m : (s + 1) * m]
                last(k)
                return carry

            lax.fori_loop(0, 2, project, 0)

        @pl.when(need == 0)
        def _():
            for i in range(len(chunks)):
                arrive(i, e)
            last(0)

        lo = 0
        for m in sizes:
            pl.when((need > lo) & (need <= m))(functools.partial(run, m))
            lo = m
        return carry

    lax.fori_loop(0, e_loc, step, 0)
    for c in out_copies(1):
        c.start()
    for c in out_copies(0) + out_copies(1):
        c.wait()


def _combine_kernel(hit_ref, gate_ref, s0_ref, s1_ref, f0_ref, f1_ref, out_ref):
    top = hit_ref.shape[0]
    y = jnp.concatenate([s0_ref[...] + f0_ref[...], s1_ref[...] + f1_ref[...]], axis=0).astype(BF16)
    total = None
    for j in range(top):
        part = jnp.dot(hit_ref[j], y, preferred_element_type=F32) * gate_ref[:, top + j : top + j + 1]
        total = part if total is None else total + part
    out_ref[...] = total.astype(out_ref.dtype)


def solution(mesh):
    chips = mesh.shape["tp"]
    vmem = pl.BlockSpec(memory_space=pltpu.VMEM)
    anym = pl.BlockSpec(memory_space=pl.ANY)
    smem = pl.BlockSpec(memory_space=pltpu.SMEM)

    def layer(x, idx, g, cap, w1, w3, w2):
        t_loc, d = x.shape
        top = idx.shape[1]
        e_all = cap.shape[0]
        e_loc, _, ff = w1.shape
        c = (5 * top * t_loc // (2 * e_all) + 7) // 8 * 8
        rows = top * t_loc
        cuts = (0, 512, ff)
        widths = [b - a for a, b in zip(cuts, cuts[1:])]
        blocks = 2 * chips

        def swap(a):
            return lax.ppermute(a, "ep", [(0, 1), (1, 0)])

        def shift(a, turns):
            pairs = [(2 * k + i, 2 * (k ^ turns[i]) + i) for k in range(chips) for i in range(2)]
            return lax.ppermute(a, ("tp", "ep"), pairs)

        out, back = (1, 2), (2, 1)
        pieces = 4
        pos, groups, hit, gate, pair, x_near = pl.pallas_call(
            functools.partial(_route_kernel, chips, out),
            out_shape=[
                jax.ShapeDtypeStruct((blocks, e_all, t_loc), jnp.int32),
                jax.ShapeDtypeStruct((blocks, 128), jnp.int32),
                jax.ShapeDtypeStruct((top, t_loc, rows), BF16),
                jax.ShapeDtypeStruct((t_loc, 8), F32),
                jax.ShapeDtypeStruct((2 * t_loc, d), BF16),
                jax.ShapeDtypeStruct((t_loc, d), BF16),
            ],
            in_specs=[vmem, vmem, smem, anym],
            out_specs=[vmem] * 4 + [anym] * 2,
            scratch_shapes=[
                pltpu.VMEM((blocks, top, t_loc), jnp.int32),
                pltpu.VMEM((t_loc, d), BF16),
                pltpu.VMEM((t_loc, d), BF16),
                pltpu.SemaphoreType.DMA((blocks,)),
                pltpu.SemaphoreType.DMA((blocks,)),
                pltpu.SemaphoreType.DMA((2, pieces)),
                pltpu.SemaphoreType.DMA((2, pieces)),
                pltpu.SemaphoreType.DMA((2 + pieces,)),
            ],
            compiler_params=pltpu.CompilerParams(collective_id=0, has_side_effects=True, vmem_limit_bytes=VMEM_BYTES),
            name="route",
        )(idx.T, g.T, cap, x)

        sizes = (64, (c + 7 + 7) // 8 * 8)

        def stage(turns, mine, other, split, rows0=(0, 0)):
            return pl.pallas_call(
                functools.partial(_expert_kernel, turns, rows0, sizes, cuts),
                out_shape=[jax.ShapeDtypeStruct((n, d), F32) for n in split * 2],
                in_specs=[smem, vmem] + [anym] * 5,
                out_specs=[anym] * 4,
                scratch_shapes=[
                    pltpu.VMEM((2, rows, d), F32),
                    pltpu.VMEM((2, t_loc, d), BF16),
                    *[pltpu.VMEM((2, d, w), BF16) for w in widths * 2],
                    pltpu.VMEM((2, 2, ff, d // 2), BF16),
                    pltpu.SemaphoreType.DMA((2, 2 * len(widths) + 2)),
                    pltpu.SemaphoreType.DMA((2, 4)),
                    pltpu.SemaphoreType.DMA((2,)),
                ],
                compiler_params=pltpu.CompilerParams(vmem_limit_bytes=VMEM_BYTES),
                cost_estimate=pl.CostEstimate(
                    flops=6 * rows * d * ff, bytes_accessed=6 * e_loc * d * ff + 8 * rows * d, transcendentals=0
                ),
            )(groups, pos, mine, other, w1, w3, w2)

        def merge(parts, *more):
            sums = []
            for q in range(2):
                other = swap(parts[q])
                sums.append(functools.reduce(jnp.add, [m[q] for m in more], parts[2 + q] + other))
            return sums

        early, late = (rows // 4, rows - rows // 4), (rows - rows // 4, rows // 4)
        rest = shift(pair, back)
        rest_other = swap(rest)
        own_x = swap(x)
        near = merge(stage(out, pair, x_near, early))
        near = [shift(a, out) for a in near]
        diag = merge(stage((3, 3), rest, rest_other, late))
        via = [shift(a, out) for a in diag]
        far = merge(stage(back, rest, rest_other, late, (t_loc, t_loc)), via)
        far = [shift(a, back) for a in far]
        near = jnp.concatenate(near, axis=0)
        near = [near[: late[0]], near[late[0] :]]
        sums = merge(stage((0, 0), x, own_x, late), near)
        steps = 4
        parts = [pl.BlockSpec((n, d // steps), lambda i: (0, i)) for n in late]
        return pl.pallas_call(
            _combine_kernel,
            out_shape=jax.ShapeDtypeStruct((t_loc, d), BF16),
            grid=(steps,),
            in_specs=[vmem, vmem] + parts * 2,
            out_specs=pl.BlockSpec((t_loc, d // steps), lambda i: (0, i)),
            name="combine",
        )(hit, gate, *sums, *far)

    rows = P(("ep", "tp"), None)
    return jax.shard_map(
        layer,
        mesh=mesh,
        in_specs=(rows, rows, rows, P(None), P("ep", None, "tp"), P("ep", None, "tp"), P("ep", "tp", None)),
        out_specs=rows,
        check_vma=False,
    )
```

```python
import functools

import jax
import jax.numpy as jnp
from jax import lax
from jax.experimental import pallas as pl
from jax.experimental.pallas import tpu as pltpu
from jax.sharding import PartitionSpec as P


F32 = jnp.float32
BF16 = jnp.bfloat16
VMEM_BYTES = 67_043_328


def _route_kernel(chips, turns, idx_ref, g_ref, cap_ref, x_ref, *refs):
    pos_ref, table_ref, hit_ref, gate_ref, pair_ref, xo_ref, ids_all, held, landed, send_sem, recv_sem, xsend, xrecv, lsem = refs
    core, me = lax.axis_index("ep"), lax.axis_index("tp")
    blocks, top, t = ids_all.shape
    e_all = pos_ref.shape[1]
    here = core * chips + me
    mesh_id = pl.DeviceIdType.MESH
    peers = [
        (k, {"ep": jnp.bitwise_xor(core, k // chips), "tp": jnp.bitwise_xor(me, k % chips)}) for k in range(1, blocks)
    ]
    load = pltpu.make_async_copy(x_ref, held, lsem.at[0])
    load.start()
    barrier = pltpu.get_barrier_semaphore()
    for _, peer in peers:
        pl.semaphore_signal(barrier, inc=1, device_id=peer, device_id_type=mesh_id)
    pl.semaphore_wait(barrier, blocks - 1)
    copies = [
        pltpu.make_async_remote_copy(
            src_ref=idx_ref,
            dst_ref=ids_all.at[here],
            send_sem=send_sem.at[k],
            recv_sem=recv_sem.at[k],
            device_id=peer,
            device_id_type=mesh_id,
        )
        for k, peer in peers
    ]
    for c in copies:
        c.start()
    pieces = xsend.shape[1]
    turn = turns[0] + (turns[1] - turns[0]) * core
    piece = x_ref.shape[0] // pieces

    def tokens(hop, i, src, dst, peer):
        part = pl.ds(i * piece, piece)
        return pltpu.make_async_remote_copy(
            src_ref=src.at[part],
            dst_ref=dst.at[part],
            send_sem=xsend.at[hop, i],
            recv_sem=xrecv.at[hop, i],
            device_id=peer,
            device_id_type=mesh_id,
        )

    arrive = [tokens(0, i, held, landed, {"ep": core, "tp": jnp.bitwise_xor(me, turn)}) for i in range(pieces)]
    forward = [tokens(1, i, landed, xo_ref, {"ep": 1 - core, "tp": me}) for i in range(pieces)]
    keep = [
        pltpu.make_async_copy(
            landed.at[pl.ds(i * piece, piece)], pair_ref.at[pl.ds(i * piece, piece)], lsem.at[2 + i]
        )
        for i in range(pieces)
    ]
    own = pltpu.make_async_copy(held, pair_ref.at[pl.ds(t, t)], lsem.at[1])
    load.wait()
    for c in arrive:
        c.start()
    own.start()
    ids_all[pl.ds(here, 1)] = idx_ref[...][None]
    before = (
        lax.broadcasted_iota(jnp.int32, (t, t), 0) < lax.broadcasted_iota(jnp.int32, (t, t), 1)
    ).astype(F32).astype(BF16)
    ids = lax.broadcasted_iota(jnp.int32, (e_all, t), 0)
    cap = jnp.zeros((e_all, t), jnp.int32)
    for e in range(e_all):
        cap = jnp.where(ids == e, cap_ref[e], cap)
    sub, lane = (lax.broadcasted_iota(jnp.int32, (e_all, 128), i) for i in range(2))
    for c in copies:
        c.wait()

    for b in range(blocks):
        hit = (ids_all[b, 0:1, :] == ids) | (ids_all[b, 1:2, :] == ids)
        one = hit.astype(F32)
        rank = jnp.dot(one.astype(BF16), before, preferred_element_type=F32).astype(jnp.int32)
        total = jnp.sum(one, axis=1, keepdims=True).astype(jnp.int32)
        count = jnp.minimum(jnp.broadcast_to(total, (e_all, t)), cap)
        first = jnp.zeros_like(count)
        for e in range(e_all - 1):
            first = first + jnp.where(ids > e, jnp.broadcast_to(count[e : e + 1, :], count.shape), 0)
        pair = jnp.where(lane == sub, first[:, :128], 0) + jnp.where(lane == sub + e_all, count[:, :128], 0)
        table_ref[pl.ds(b, 1)] = jnp.sum(pair, axis=0, keepdims=True)
        pos_ref[b] = jnp.where(hit & (rank < cap), first + rank, -1)
    pos = pos_ref[here]
    lines = [
        jnp.max(jnp.where(idx_ref[j : j + 1, :] == ids, pos, -1), axis=0, keepdims=True).astype(F32) for j in range(top)
    ]
    lines += [g_ref[j : j + 1, :] for j in range(top)]
    table = jnp.concatenate(lines + [jnp.zeros((8 - 2 * top, t), F32)], axis=0)
    table = jnp.transpose(table)
    gate_ref[...] = table
    row = lax.broadcasted_iota(jnp.int32, hit_ref.shape[1:], 1)
    for j in range(top):
        hit_ref[j] = (row == table[:, j : j + 1].astype(jnp.int32)).astype(F32).astype(BF16)
    for c, f, k in zip(arrive, forward, keep):
        c.wait_recv()
        f.start()
        k.start()
    for c, f, k in zip(arrive, forward, keep):
        c.wait_send()
        k.wait()
        f.wait()
    own.wait()


def _expert_kernel(
    turns, rows0, sizes, cuts, table_ref, pos_ref, xm_hbm, xo_hbm, w1_hbm, w3_hbm, w2_hbm, *refs
):
    outs = refs[:4]
    acc, xbuf, *ws, w2s, wsem, osem, xsem = refs[4:]
    w1s, w3s = ws[: len(ws) // 2], ws[len(ws) // 2 :]
    e_loc, d, _ = w1_hbm.shape
    _, rows, _ = acc.shape
    t = xbuf.shape[1]
    half_d = d // 2
    core, me = lax.axis_index("ep"), lax.axis_index("tp")
    chips = pos_ref.shape[0] // 2
    blocks = []
    for c in (core, 1 - core):
        turn = jnp.where(c == 0, turns[0], turns[1])
        blocks.append(c * chips + jnp.bitwise_xor(me, turn))

    def columns(k):
        def copies(e):
            cols, b = pl.ds(cuts[k], cuts[k + 1] - cuts[k]), e % 2
            return [
                pltpu.make_async_copy(w1_hbm.at[e, :, cols], w1s[k].at[b], wsem.at[b, 2 * k]),
                pltpu.make_async_copy(w3_hbm.at[e, :, cols], w3s[k].at[b], wsem.at[b, 2 * k + 1]),
            ]

        return copies

    def output(k):
        def copies(e):
            cols, b = pl.ds(pl.multiple_of(k * half_d, half_d), half_d), e % 2
            return [pltpu.make_async_copy(w2_hbm.at[e, :, cols], w2s.at[b, k], wsem.at[b, 2 * len(w1s) + k])]

        return copies

    chunks = [columns(k) for k in range(len(w1s))] + [output(k) for k in range(2)]

    def arrive(i, e):
        for c in chunks[i](e):
            c.wait()
        if i == 0:

            @pl.when((e == 0) & (e_loc > 1))
            def _():
                for later in chunks:
                    for c in later(1):
                        c.start()

    def used(i, e):
        @pl.when(e + 2 < e_loc)
        def _():
            for c in chunks[i](e + 2):
                c.start()

    def out_copies(h):
        cols = pl.ds(h * half_d, half_d)
        copies = []
        for i in range(4):
            size = outs[i].shape[0]
            part = pl.ds(0 if i % 2 == 0 else rows - size, size)
            copies.append(pltpu.make_async_copy(acc.at[1 - i // 2, part, cols], outs[i].at[:, cols], osem.at[h, i]))
        return copies

    tokens = [
        pltpu.make_async_copy(ref.at[pl.ds(rows0[i], t)], xbuf.at[i], xsem.at[i]) for i, ref in enumerate((xm_hbm, xo_hbm))
    ]
    for c in tokens:
        c.start()
    for chunk in chunks:
        for c in chunk(0):
            c.start()
    acc[...] = jnp.zeros_like(acc)
    for c in tokens:
        c.wait()

    def step(e, carry):
        expert = core * e_loc + e
        offs = [table_ref[b, expert] for b in blocks]
        cnts = [table_ref[b, 2 * e_loc + expert] for b in blocks]
        need = functools.reduce(jnp.maximum, [jnp.where(k > 0, o - o // 8 * 8 + k, 0) for o, k in zip(offs, cnts)])

        def last(k):
            @pl.when((e == e_loc - 1) & (k == 0))
            def _():
                for c in out_copies(0):
                    c.start()

        def run(m):
            bases = [pl.multiple_of(jnp.minimum(o // 8 * 8, rows - m), 8) for o in offs]
            parts = []
            for s in range(2):
                row = lax.broadcasted_iota(jnp.int32, (m, t), 0) + bases[s]
                hit = (row == pos_ref[blocks[s], pl.ds(expert, 1), :]).astype(F32).astype(BF16)
                parts.append(jnp.dot(hit, xbuf[s], preferred_element_type=F32))
            xs = jnp.concatenate(parts, axis=0).astype(BF16)
            hs = []
            for i, (wa, wb) in enumerate(zip(w1s, w3s)):
                arrive(i, e)
                h1 = jnp.dot(xs, wa[e % 2], preferred_element_type=F32)
                h3 = jnp.dot(xs, wb[e % 2], preferred_element_type=F32)
                hs.append((jax.nn.silu(h1) * h3).astype(BF16))
                used(i, e)
            h = jnp.concatenate(hs, axis=1)

            def project(k, carry):
                for i in range(2):
                    pl.when(k == i)(functools.partial(arrive, len(w1s) + i, e))
                p = jnp.dot(h, w2s[e % 2, k], preferred_element_type=F32)
                cols = pl.ds(pl.multiple_of(k * half_d, half_d), half_d)
                for s in range(2):
                    acc[s, pl.ds(bases[s], m), cols] += p[s * m : (s + 1) * m]
                for i in range(2):
                    pl.when(k == i)(functools.partial(used, len(w1s) + i, e))
                last(k)
                return carry

            lax.fori_loop(0, 2, project, 0)

        @pl.when(need == 0)
        def _():
            for i in range(len(chunks)):
                arrive(i, e)
                used(i, e)
            last(0)

        lo = 0
        for m in sizes:
            pl.when((need > lo) & (need <= m))(functools.partial(run, m))
            lo = m
        return carry

    lax.fori_loop(0, e_loc, step, 0)
    for c in out_copies(1):
        c.start()
    for c in out_copies(0) + out_copies(1):
        c.wait()


def _weigh(hit, gate_ref, y, total=None):
    top = len(hit)
    for j in range(top):
        part = jnp.dot(hit[j], y, preferred_element_type=F32) * gate_ref[:, top + j : top + j + 1]
        total = part if total is None else total + part
    return total


def _combine_kernel(hit_ref, gate_ref, k0_ref, k1_ref, o0_ref, o1_ref, n0_ref, n1_ref, f0_ref, total_ref, sum_ref):
    most = f0_ref.shape[0]
    near = jnp.concatenate([n0_ref[...], n1_ref[...]], axis=0)
    y = (k0_ref[...] + o0_ref[...] + near[:most] + f0_ref[...]).astype(BF16)
    total_ref[...] = _weigh([hit_ref[j, :, :most] for j in range(hit_ref.shape[0])], gate_ref, y)
    sum_ref[...] = k1_ref[...] + o1_ref[...] + near[most:]


def _close_kernel(hit_ref, gate_ref, total_ref, sum_ref, f1_ref, out_ref):
    most = hit_ref.shape[2] - f1_ref.shape[0]
    y = (sum_ref[...] + f1_ref[...]).astype(BF16)
    hit = [hit_ref[j, :, most:] for j in range(hit_ref.shape[0])]
    out_ref[...] = _weigh(hit, gate_ref, y, total_ref[...]).astype(out_ref.dtype)


def solution(mesh):
    chips = mesh.shape["tp"]
    vmem = pl.BlockSpec(memory_space=pltpu.VMEM)
    anym = pl.BlockSpec(memory_space=pl.ANY)
    smem = pl.BlockSpec(memory_space=pltpu.SMEM)

    def layer(x, idx, g, cap, w1, w3, w2):
        t_loc, d = x.shape
        top = idx.shape[1]
        e_all = cap.shape[0]
        e_loc, _, ff = w1.shape
        c = (5 * top * t_loc // (2 * e_all) + 7) // 8 * 8
        rows = top * t_loc
        cuts = (0, 512, ff)
        widths = [b - a for a, b in zip(cuts, cuts[1:])]
        blocks = 2 * chips

        def swap(a):
            return lax.ppermute(a, "ep", [(0, 1), (1, 0)])

        def shift(a, turns):
            pairs = [(2 * k + i, 2 * (k ^ turns[i]) + i) for k in range(chips) for i in range(2)]
            return lax.ppermute(a, ("tp", "ep"), pairs)

        out, back = (1, 2), (2, 1)
        pieces = 4
        pos, groups, hit, gate, pair, x_near = pl.pallas_call(
            functools.partial(_route_kernel, chips, out),
            out_shape=[
                jax.ShapeDtypeStruct((blocks, e_all, t_loc), jnp.int32),
                jax.ShapeDtypeStruct((blocks, 128), jnp.int32),
                jax.ShapeDtypeStruct((top, t_loc, rows), BF16),
                jax.ShapeDtypeStruct((t_loc, 8), F32),
                jax.ShapeDtypeStruct((2 * t_loc, d), BF16),
                jax.ShapeDtypeStruct((t_loc, d), BF16),
            ],
            in_specs=[vmem, vmem, smem, anym],
            out_specs=[vmem] * 4 + [anym] * 2,
            scratch_shapes=[
                pltpu.VMEM((blocks, top, t_loc), jnp.int32),
                pltpu.VMEM((t_loc, d), BF16),
                pltpu.VMEM((t_loc, d), BF16),
                pltpu.SemaphoreType.DMA((blocks,)),
                pltpu.SemaphoreType.DMA((blocks,)),
                pltpu.SemaphoreType.DMA((2, pieces)),
                pltpu.SemaphoreType.DMA((2, pieces)),
                pltpu.SemaphoreType.DMA((2 + pieces,)),
            ],
            compiler_params=pltpu.CompilerParams(collective_id=0, has_side_effects=True, vmem_limit_bytes=VMEM_BYTES),
            name="route",
        )(idx.T, g.T, cap, x)

        sizes = (64, (c + 7 + 7) // 8 * 8)

        def stage(turns, mine, other, split, rows0=(0, 0)):
            return pl.pallas_call(
                functools.partial(_expert_kernel, turns, rows0, sizes, cuts),
                out_shape=[jax.ShapeDtypeStruct((n, d), F32) for n in split * 2],
                in_specs=[smem, vmem] + [anym] * 5,
                out_specs=[anym] * 4,
                scratch_shapes=[
                    pltpu.VMEM((2, rows, d), F32),
                    pltpu.VMEM((2, t_loc, d), BF16),
                    *[pltpu.VMEM((2, d, w), BF16) for w in widths * 2],
                    pltpu.VMEM((2, 2, ff, d // 2), BF16),
                    pltpu.SemaphoreType.DMA((2, 2 * len(widths) + 2)),
                    pltpu.SemaphoreType.DMA((2, 4)),
                    pltpu.SemaphoreType.DMA((2,)),
                ],
                compiler_params=pltpu.CompilerParams(vmem_limit_bytes=VMEM_BYTES),
                cost_estimate=pl.CostEstimate(
                    flops=6 * rows * d * ff, bytes_accessed=6 * e_loc * d * ff + 8 * rows * d, transcendentals=0
                ),
            )(groups, pos, mine, other, w1, w3, w2)

        def merge(parts, *more):
            sums = []
            for q in range(2):
                other = swap(parts[q])
                sums.append(functools.reduce(jnp.add, [m[q] for m in more], parts[2 + q] + other))
            return sums

        early, late = (rows // 8, rows - rows // 8), (rows - rows // 4, rows // 4)
        rest = shift(pair, back)
        rest_other = swap(rest)
        own_x = swap(x)
        near = merge(stage(out, pair, x_near, early))
        near = [shift(a, out) for a in near]
        diag = merge(stage((3, 3), rest, rest_other, late))
        via = [shift(a, out) for a in diag]
        far = merge(stage(back, rest, rest_other, late, (t_loc, t_loc)), via)
        far = [shift(a, back) for a in far]
        own = stage((0, 0), x, own_x, late)
        other = [swap(own[q]) for q in range(2)]

        def by_columns(steps):
            def part(n):
                return pl.BlockSpec((n, d // steps), lambda i: (0, i))

            return dict(grid=(steps,)), part

        grid, part = by_columns(4)
        total, last = pl.pallas_call(
            _combine_kernel,
            out_shape=[jax.ShapeDtypeStruct((t_loc, d), F32), jax.ShapeDtypeStruct((late[1], d), F32)],
            in_specs=[vmem, vmem] + [part(n) for n in late * 2 + early + late[:1]],
            out_specs=[part(t_loc), part(late[1])],
            compiler_params=pltpu.CompilerParams(vmem_limit_bytes=VMEM_BYTES),
            name="combine",
            **grid,
        )(hit, gate, *own[2:], *other, *near, far[0])
        grid, part = by_columns(2)
        return pl.pallas_call(
            _close_kernel,
            out_shape=jax.ShapeDtypeStruct((t_loc, d), BF16),
            in_specs=[vmem, vmem] + [part(n) for n in (t_loc, late[1], late[1])],
            out_specs=part(t_loc),
            name="close",
            **grid,
        )(hit, gate, total, last, far[1])

    rows = P(("ep", "tp"), None)
    return jax.shard_map(
        layer,
        mesh=mesh,
        in_specs=(rows, rows, rows, P(None), P("ep", None, "tp"), P("ep", None, "tp"), P("ep", "tp", None)),
        out_specs=rows,
        check_vma=False,
    )
```

```python
import functools

import jax
import jax.numpy as jnp
from jax import lax
from jax.experimental import pallas as pl
from jax.experimental.pallas import tpu as pltpu
from jax.sharding import PartitionSpec as P


F32 = jnp.float32
BF16 = jnp.bfloat16
VMEM_BYTES = 67_043_328


def _route_kernel(chips, turns, idx_ref, g_ref, cap_ref, x_ref, *refs):
    pos_ref, table_ref, hit_ref, gate_ref, pair_ref, xo_ref, ids_all, held, landed, send_sem, recv_sem, xsend, xrecv, lsem = refs
    core, me = lax.axis_index("ep"), lax.axis_index("tp")
    blocks, top, t = ids_all.shape
    e_all = pos_ref.shape[1]
    here = core * chips + me
    mesh_id = pl.DeviceIdType.MESH
    peers = [
        (k, {"ep": jnp.bitwise_xor(core, k // chips), "tp": jnp.bitwise_xor(me, k % chips)}) for k in range(1, blocks)
    ]
    load = pltpu.make_async_copy(x_ref, held, lsem.at[0])
    load.start()
    barrier = pltpu.get_barrier_semaphore()
    for _, peer in peers:
        pl.semaphore_signal(barrier, inc=1, device_id=peer, device_id_type=mesh_id)
    pl.semaphore_wait(barrier, blocks - 1)
    copies = [
        pltpu.make_async_remote_copy(
            src_ref=idx_ref,
            dst_ref=ids_all.at[here],
            send_sem=send_sem.at[k],
            recv_sem=recv_sem.at[k],
            device_id=peer,
            device_id_type=mesh_id,
        )
        for k, peer in peers
    ]
    pieces = xsend.shape[1]
    turn = turns[0] + (turns[1] - turns[0]) * core
    piece = x_ref.shape[0] // pieces

    def tokens(hop, i, src, dst, peer):
        part = pl.ds(i * piece, piece)
        return pltpu.make_async_remote_copy(
            src_ref=src.at[part],
            dst_ref=dst.at[part],
            send_sem=xsend.at[hop, i],
            recv_sem=xrecv.at[hop, i],
            device_id=peer,
            device_id_type=mesh_id,
        )

    arrive = [tokens(0, i, held, landed, {"ep": core, "tp": jnp.bitwise_xor(me, turn)}) for i in range(pieces)]
    forward = [tokens(1, i, landed, xo_ref, {"ep": 1 - core, "tp": me}) for i in range(pieces)]
    keep = [
        pltpu.make_async_copy(
            landed.at[pl.ds(i * piece, piece)], pair_ref.at[pl.ds(i * piece, piece)], lsem.at[2 + i]
        )
        for i in range(pieces)
    ]
    own = pltpu.make_async_copy(held, pair_ref.at[pl.ds(t, t)], lsem.at[1])
    load.wait()
    arrive[0].start()
    for c in copies:
        c.start()
    for c in arrive[1:]:
        c.start()
    own.start()
    ids_all[pl.ds(here, 1)] = idx_ref[...][None]
    before = (
        lax.broadcasted_iota(jnp.int32, (t, t), 0) < lax.broadcasted_iota(jnp.int32, (t, t), 1)
    ).astype(F32).astype(BF16)
    ids = lax.broadcasted_iota(jnp.int32, (e_all, t), 0)
    cap = jnp.zeros((e_all, t), jnp.int32)
    for e in range(e_all):
        cap = jnp.where(ids == e, cap_ref[e], cap)
    sub, lane = (lax.broadcasted_iota(jnp.int32, (e_all, 128), i) for i in range(2))
    for c in copies:
        c.wait()

    for b in range(blocks):
        hit = (ids_all[b, 0:1, :] == ids) | (ids_all[b, 1:2, :] == ids)
        one = hit.astype(F32)
        rank = jnp.dot(one.astype(BF16), before, preferred_element_type=F32).astype(jnp.int32)
        total = jnp.sum(one, axis=1, keepdims=True).astype(jnp.int32)
        count = jnp.minimum(jnp.broadcast_to(total, (e_all, t)), cap)
        first = jnp.zeros_like(count)
        for e in range(e_all - 1):
            first = first + jnp.where(ids > e, jnp.broadcast_to(count[e : e + 1, :], count.shape), 0)
        pair = jnp.where(lane == sub, first[:, :128], 0) + jnp.where(lane == sub + e_all, count[:, :128], 0)
        table_ref[pl.ds(b, 1)] = jnp.sum(pair, axis=0, keepdims=True)
        pos_ref[b] = jnp.where(hit & (rank < cap), first + rank, -1)
    pos = pos_ref[here]
    lines = [
        jnp.max(jnp.where(idx_ref[j : j + 1, :] == ids, pos, -1), axis=0, keepdims=True).astype(F32) for j in range(top)
    ]
    lines += [g_ref[j : j + 1, :] for j in range(top)]
    table = jnp.concatenate(lines + [jnp.zeros((8 - 2 * top, t), F32)], axis=0)
    table = jnp.transpose(table)
    gate_ref[...] = table
    row = lax.broadcasted_iota(jnp.int32, hit_ref.shape[1:], 1)
    for j in range(top):
        hit_ref[j] = (row == table[:, j : j + 1].astype(jnp.int32)).astype(F32).astype(BF16)
    for c, f, k in zip(arrive, forward, keep):
        c.wait_recv()
        f.start()
        k.start()
    for c, f, k in zip(arrive, forward, keep):
        c.wait_send()
        k.wait()
        f.wait()
    own.wait()


def _expert_kernel(
    turns, rows0, sizes, cuts, table_ref, pos_ref, xm_hbm, xo_hbm, w1_hbm, w3_hbm, w2_hbm, *refs
):
    outs = refs[:4]
    acc, xbuf, *ws, w2s, wsem, osem, xsem = refs[4:]
    w1s, w3s = ws[: len(ws) // 2], ws[len(ws) // 2 :]
    e_loc, d, _ = w1_hbm.shape
    _, rows, _ = acc.shape
    t = xbuf.shape[1]
    half_d = d // 2
    core, me = lax.axis_index("ep"), lax.axis_index("tp")
    chips = pos_ref.shape[0] // 2
    blocks = []
    for c in (core, 1 - core):
        turn = jnp.where(c == 0, turns[0], turns[1])
        blocks.append(c * chips + jnp.bitwise_xor(me, turn))

    def columns(k):
        def copies(e):
            cols, b = pl.ds(cuts[k], cuts[k + 1] - cuts[k]), e % 2
            return [
                pltpu.make_async_copy(w1_hbm.at[e, :, cols], w1s[k].at[b], wsem.at[b, 2 * k]),
                pltpu.make_async_copy(w3_hbm.at[e, :, cols], w3s[k].at[b], wsem.at[b, 2 * k + 1]),
            ]

        return copies

    def output(k):
        def copies(e):
            cols, b = pl.ds(pl.multiple_of(k * half_d, half_d), half_d), e % 2
            return [pltpu.make_async_copy(w2_hbm.at[e, :, cols], w2s.at[b, k], wsem.at[b, 2 * len(w1s) + k])]

        return copies

    chunks = [columns(k) for k in range(len(w1s))] + [output(k) for k in range(2)]

    def arrive(i, e):
        for c in chunks[i](e):
            c.wait()
        if i == 0:

            @pl.when((e == 0) & (e_loc > 1))
            def _():
                for later in chunks:
                    for c in later(1):
                        c.start()

    def used(i, e):
        @pl.when(e + 2 < e_loc)
        def _():
            for c in chunks[i](e + 2):
                c.start()

    def out_copies(h):
        cols = pl.ds(h * half_d, half_d)
        copies = []
        for i in range(4):
            size = outs[i].shape[0]
            part = pl.ds(0 if i % 2 == 0 else rows - size, size)
            copies.append(pltpu.make_async_copy(acc.at[1 - i // 2, part, cols], outs[i].at[:, cols], osem.at[h, i]))
        return copies

    tokens = [
        pltpu.make_async_copy(ref.at[pl.ds(rows0[i], t)], xbuf.at[i], xsem.at[i]) for i, ref in enumerate((xm_hbm, xo_hbm))
    ]
    for c in tokens:
        c.start()
    for chunk in chunks:
        for c in chunk(0):
            c.start()
    acc[...] = jnp.zeros_like(acc)
    for c in tokens:
        c.wait()

    def step(e, carry):
        expert = core * e_loc + e
        offs = [table_ref[b, expert] for b in blocks]
        cnts = [table_ref[b, 2 * e_loc + expert] for b in blocks]
        need = functools.reduce(jnp.maximum, [jnp.where(k > 0, o - o // 8 * 8 + k, 0) for o, k in zip(offs, cnts)])

        def last(k):
            @pl.when((e == e_loc - 1) & (k == 0))
            def _():
                for c in out_copies(0):
                    c.start()

        def run(m):
            tiles = (need + m - 1) // m

            def once(i, carry):
                opens, closes = i == 0, i == tiles - 1
                starts = [o // 8 * 8 + i * m for o in offs]
                bases = [pl.multiple_of(jnp.minimum(b, rows - m), 8) for b in starts]
                parts = []
                for s in range(2):
                    row = lax.broadcasted_iota(jnp.int32, (m, t), 0) + bases[s]
                    hit = (row == pos_ref[blocks[s], pl.ds(expert, 1), :]) & (row >= starts[s])
                    parts.append(jnp.dot(hit.astype(F32).astype(BF16), xbuf[s], preferred_element_type=F32))
                xs = jnp.concatenate(parts, axis=0).astype(BF16)
                hs = []
                for c, (wa, wb) in enumerate(zip(w1s, w3s)):
                    pl.when(opens)(functools.partial(arrive, c, e))
                    h1 = jnp.dot(xs, wa[e % 2], preferred_element_type=F32)
                    h3 = jnp.dot(xs, wb[e % 2], preferred_element_type=F32)
                    hs.append((jax.nn.silu(h1) * h3).astype(BF16))
                    pl.when(closes)(functools.partial(used, c, e))
                h = jnp.concatenate(hs, axis=1)

                def project(k, carry):
                    for c in range(2):
                        pl.when(opens & (k == c))(functools.partial(arrive, len(w1s) + c, e))
                    p = jnp.dot(h, w2s[e % 2, k], preferred_element_type=F32)
                    cols = pl.ds(pl.multiple_of(k * half_d, half_d), half_d)
                    for s in range(2):
                        acc[s, pl.ds(bases[s], m), cols] += p[s * m : (s + 1) * m]
                    for c in range(2):
                        pl.when(closes & (k == c))(functools.partial(used, len(w1s) + c, e))
                    pl.when(closes)(functools.partial(last, k))
                    return carry

                return lax.fori_loop(0, 2, project, carry)

            lax.fori_loop(0, tiles, once, 0)

        @pl.when(need == 0)
        def _():
            for i in range(len(chunks)):
                arrive(i, e)
                used(i, e)
            last(0)

        small, large = sizes
        pl.when((need > 0) & (need <= small))(functools.partial(run, small))
        pl.when(need > small)(functools.partial(run, large))
        return carry

    lax.fori_loop(0, e_loc, step, 0)
    for c in out_copies(1):
        c.start()
    for c in out_copies(0) + out_copies(1):
        c.wait()


def _weigh(hit, gate_ref, y, total=None):
    top = len(hit)
    for j in range(top):
        part = jnp.dot(hit[j], y, preferred_element_type=F32) * gate_ref[:, top + j : top + j + 1]
        total = part if total is None else total + part
    return total


def _combine_kernel(hit_ref, gate_ref, k0_ref, k1_ref, o0_ref, o1_ref, n0_ref, n1_ref, f0_ref, total_ref, sum_ref):
    most = f0_ref.shape[0]
    near = jnp.concatenate([n0_ref[...], n1_ref[...]], axis=0)
    y = (k0_ref[...] + o0_ref[...] + near[:most] + f0_ref[...]).astype(BF16)
    total_ref[...] = _weigh([hit_ref[j, :, :most] for j in range(hit_ref.shape[0])], gate_ref, y)
    sum_ref[...] = k1_ref[...] + o1_ref[...] + near[most:]


def _close_kernel(hit_ref, gate_ref, total_ref, sum_ref, f1_ref, out_ref):
    most = hit_ref.shape[2] - f1_ref.shape[0]
    y = (sum_ref[...] + f1_ref[...]).astype(BF16)
    hit = [hit_ref[j, :, most:] for j in range(hit_ref.shape[0])]
    out_ref[...] = _weigh(hit, gate_ref, y, total_ref[...]).astype(out_ref.dtype)


def solution(mesh):
    chips = mesh.shape["tp"]
    vmem = pl.BlockSpec(memory_space=pltpu.VMEM)
    anym = pl.BlockSpec(memory_space=pl.ANY)
    smem = pl.BlockSpec(memory_space=pltpu.SMEM)

    def layer(x, idx, g, cap, w1, w3, w2):
        t_loc, d = x.shape
        top = idx.shape[1]
        e_all = cap.shape[0]
        e_loc, _, ff = w1.shape
        rows = top * t_loc
        cuts = (0, 512, ff)
        widths = [b - a for a, b in zip(cuts, cuts[1:])]
        blocks = 2 * chips

        def swap(a):
            return lax.ppermute(a, "ep", [(0, 1), (1, 0)])

        def shift(a, turns):
            pairs = [(2 * k + i, 2 * (k ^ turns[i]) + i) for k in range(chips) for i in range(2)]
            return lax.ppermute(a, ("tp", "ep"), pairs)

        out, back = (1, 2), (2, 1)
        pieces = 2
        pos, groups, hit, gate, pair, x_near = pl.pallas_call(
            functools.partial(_route_kernel, chips, out),
            out_shape=[
                jax.ShapeDtypeStruct((blocks, e_all, t_loc), jnp.int32),
                jax.ShapeDtypeStruct((blocks, 128), jnp.int32),
                jax.ShapeDtypeStruct((top, t_loc, rows), BF16),
                jax.ShapeDtypeStruct((t_loc, 8), F32),
                jax.ShapeDtypeStruct((2 * t_loc, d), BF16),
                jax.ShapeDtypeStruct((t_loc, d), BF16),
            ],
            in_specs=[vmem, vmem, smem, anym],
            out_specs=[vmem] * 4 + [anym] * 2,
            scratch_shapes=[
                pltpu.VMEM((blocks, top, t_loc), jnp.int32),
                pltpu.VMEM((t_loc, d), BF16),
                pltpu.VMEM((t_loc, d), BF16),
                pltpu.SemaphoreType.DMA((blocks,)),
                pltpu.SemaphoreType.DMA((blocks,)),
                pltpu.SemaphoreType.DMA((2, pieces)),
                pltpu.SemaphoreType.DMA((2, pieces)),
                pltpu.SemaphoreType.DMA((2 + pieces,)),
            ],
            compiler_params=pltpu.CompilerParams(collective_id=0, has_side_effects=True, vmem_limit_bytes=VMEM_BYTES),
            name="route",
        )(idx.T, g.T, cap, x)

        sizes = (64, 152)

        def stage(turns, mine, other, split, rows0=(0, 0)):
            return pl.pallas_call(
                functools.partial(_expert_kernel, turns, rows0, sizes, cuts),
                out_shape=[jax.ShapeDtypeStruct((n, d), F32) for n in split * 2],
                in_specs=[smem, vmem] + [anym] * 5,
                out_specs=[anym] * 4,
                scratch_shapes=[
                    pltpu.VMEM((2, rows, d), F32),
                    pltpu.VMEM((2, t_loc, d), BF16),
                    *[pltpu.VMEM((2, d, w), BF16) for w in widths * 2],
                    pltpu.VMEM((2, 2, ff, d // 2), BF16),
                    pltpu.SemaphoreType.DMA((2, 2 * len(widths) + 2)),
                    pltpu.SemaphoreType.DMA((2, 4)),
                    pltpu.SemaphoreType.DMA((2,)),
                ],
                compiler_params=pltpu.CompilerParams(vmem_limit_bytes=VMEM_BYTES),
                cost_estimate=pl.CostEstimate(
                    flops=6 * rows * d * ff, bytes_accessed=6 * e_loc * d * ff + 8 * rows * d, transcendentals=0
                ),
            )(groups, pos, mine, other, w1, w3, w2)

        def merge(parts, *more):
            sums = []
            for q in range(2):
                other = swap(parts[q])
                sums.append(functools.reduce(jnp.add, [m[q] for m in more], parts[2 + q] + other))
            return sums

        early, late = (rows // 4, rows - rows // 4), (rows - rows // 4, rows // 4)
        rest = shift(pair, back)
        rest_other = swap(rest)
        own_x = swap(x)
        near = merge(stage(out, pair, x_near, early))
        near = [shift(a, out) for a in near]
        diag = merge(stage((3, 3), rest, rest_other, late))
        via = [shift(a, out) for a in diag]
        far = merge(stage(back, rest, rest_other, late, (t_loc, t_loc)), via)
        far = [shift(a, back) for a in far]
        own = stage((0, 0), x, own_x, late)
        other = [swap(own[q]) for q in range(2)]

        def by_columns(steps):
            def part(n):
                return pl.BlockSpec((n, d // steps), lambda i: (0, i))

            return dict(grid=(steps,)), part

        grid, part = by_columns(4)
        total, last = pl.pallas_call(
            _combine_kernel,
            out_shape=[jax.ShapeDtypeStruct((t_loc, d), F32), jax.ShapeDtypeStruct((late[1], d), F32)],
            in_specs=[vmem, vmem] + [part(n) for n in late * 2 + early + late[:1]],
            out_specs=[part(t_loc), part(late[1])],
            compiler_params=pltpu.CompilerParams(vmem_limit_bytes=VMEM_BYTES),
            name="combine",
            **grid,
        )(hit, gate, *own[2:], *other, *near, far[0])
        grid, part = by_columns(2)
        return pl.pallas_call(
            _close_kernel,
            out_shape=jax.ShapeDtypeStruct((t_loc, d), BF16),
            in_specs=[vmem, vmem] + [part(n) for n in (t_loc, late[1], late[1])],
            out_specs=part(t_loc),
            name="close",
            **grid,
        )(hit, gate, total, last, far[1])

    rows = P(("ep", "tp"), None)
    return jax.shard_map(
        layer,
        mesh=mesh,
        in_specs=(rows, rows, rows, P(None), P("ep", None, "tp"), P("ep", None, "tp"), P("ep", "tp", None)),
        out_specs=rows,
        check_vma=False,
    )
```

```python
import functools

import jax
import jax.numpy as jnp
from jax import lax
from jax.experimental import pallas as pl
from jax.experimental.pallas import tpu as pltpu
from jax.sharding import PartitionSpec as P


F32 = jnp.float32
BF16 = jnp.bfloat16
VMEM_BYTES = 67_043_328


def _route_kernel(chips, turns, idx_ref, g_ref, cap_ref, x_ref, *refs):
    pos_ref, table_ref, hit_ref, gate_ref, pair_ref, xo_ref, ids_all, held, landed, send_sem, recv_sem, xsend, xrecv, lsem = refs
    core, me = lax.axis_index("ep"), lax.axis_index("tp")
    blocks, top, t = ids_all.shape
    e_all = pos_ref.shape[1]
    here = core * chips + me
    mesh_id = pl.DeviceIdType.MESH
    peers = [
        (k, {"ep": jnp.bitwise_xor(core, k // chips), "tp": jnp.bitwise_xor(me, k % chips)}) for k in range(1, blocks)
    ]
    load = pltpu.make_async_copy(x_ref, held, lsem.at[0])
    load.start()
    barrier = pltpu.get_barrier_semaphore()
    for _, peer in peers:
        pl.semaphore_signal(barrier, inc=1, device_id=peer, device_id_type=mesh_id)
    pl.semaphore_wait(barrier, blocks - 1)
    copies = [
        pltpu.make_async_remote_copy(
            src_ref=idx_ref,
            dst_ref=ids_all.at[here],
            send_sem=send_sem.at[k],
            recv_sem=recv_sem.at[k],
            device_id=peer,
            device_id_type=mesh_id,
        )
        for k, peer in peers
    ]
    pieces = xsend.shape[1]
    turn = turns[0] + (turns[1] - turns[0]) * core
    piece = x_ref.shape[0] // pieces

    def tokens(hop, i, src, dst, peer):
        part = pl.ds(i * piece, piece)
        return pltpu.make_async_remote_copy(
            src_ref=src.at[part],
            dst_ref=dst.at[part],
            send_sem=xsend.at[hop, i],
            recv_sem=xrecv.at[hop, i],
            device_id=peer,
            device_id_type=mesh_id,
        )

    arrive = [tokens(0, i, held, landed, {"ep": core, "tp": jnp.bitwise_xor(me, turn)}) for i in range(pieces)]
    forward = [tokens(1, i, landed, xo_ref, {"ep": 1 - core, "tp": me}) for i in range(pieces)]
    keep = [
        pltpu.make_async_copy(
            landed.at[pl.ds(i * piece, piece)], pair_ref.at[pl.ds(i * piece, piece)], lsem.at[2 + i]
        )
        for i in range(pieces)
    ]
    own = pltpu.make_async_copy(held, pair_ref.at[pl.ds(t, t)], lsem.at[1])
    load.wait()
    arrive[0].start()
    for c in copies:
        c.start()
    for c in arrive[1:]:
        c.start()
    own.start()
    ids_all[pl.ds(here, 1)] = idx_ref[...][None]
    before = (
        lax.broadcasted_iota(jnp.int32, (t, t), 0) < lax.broadcasted_iota(jnp.int32, (t, t), 1)
    ).astype(F32).astype(BF16)
    ids = lax.broadcasted_iota(jnp.int32, (e_all, t), 0)
    cap = jnp.zeros((e_all, t), jnp.int32)
    for e in range(e_all):
        cap = jnp.where(ids == e, cap_ref[e], cap)
    sub, lane = (lax.broadcasted_iota(jnp.int32, (e_all, 128), i) for i in range(2))
    for c in copies:
        c.wait()

    for b in range(blocks):
        hit = (ids_all[b, 0:1, :] == ids) | (ids_all[b, 1:2, :] == ids)
        one = hit.astype(F32)
        rank = jnp.dot(one.astype(BF16), before, preferred_element_type=F32).astype(jnp.int32)
        total = jnp.sum(one, axis=1, keepdims=True).astype(jnp.int32)
        count = jnp.minimum(jnp.broadcast_to(total, (e_all, t)), cap)
        first = jnp.zeros_like(count)
        for e in range(e_all - 1):
            first = first + jnp.where(ids > e, jnp.broadcast_to(count[e : e + 1, :], count.shape), 0)
        pair = jnp.where(lane == sub, first[:, :128], 0) + jnp.where(lane == sub + e_all, count[:, :128], 0)
        table_ref[pl.ds(b, 1)] = jnp.sum(pair, axis=0, keepdims=True)
        pos_ref[b] = jnp.where(hit & (rank < cap), first + rank, -1)
    pos = pos_ref[here]
    lines = [
        jnp.max(jnp.where(idx_ref[j : j + 1, :] == ids, pos, -1), axis=0, keepdims=True).astype(F32) for j in range(top)
    ]
    lines += [g_ref[j : j + 1, :] for j in range(top)]
    table = jnp.concatenate(lines + [jnp.zeros((8 - 2 * top, t), F32)], axis=0)
    table = jnp.transpose(table)
    gate_ref[...] = table
    row = lax.broadcasted_iota(jnp.int32, hit_ref.shape[1:], 1)
    for j in range(top):
        hit_ref[j] = (row == table[:, j : j + 1].astype(jnp.int32)).astype(F32).astype(BF16)
    for c, f, k in zip(arrive, forward, keep):
        c.wait_recv()
        f.start()
        k.start()
    for c, f, k in zip(arrive, forward, keep):
        c.wait_send()
        k.wait()
        f.wait()
    own.wait()


def _expert_kernel(
    turns, rows0, sizes, cuts, inits, table_ref, pos_ref, xm_hbm, xo_hbm, w1_hbm, w3_hbm, w2_hbm, *refs
):
    init_hbm, outs = refs[:inits], refs[inits : inits + 4]
    acc, xbuf, *ws, w2s, wsem, osem, xsem = refs[inits + 4 :]
    w1s, w3s = ws[: len(ws) // 2], ws[len(ws) // 2 :]
    e_loc, d, _ = w1_hbm.shape
    _, rows, _ = acc.shape
    t = xbuf.shape[1]
    half_d = d // 2
    core, me = lax.axis_index("ep"), lax.axis_index("tp")
    chips = pos_ref.shape[0] // 2
    blocks = []
    for c in (core, 1 - core):
        turn = jnp.where(c == 0, turns[0], turns[1])
        blocks.append(c * chips + jnp.bitwise_xor(me, turn))

    def columns(k):
        def copies(e):
            cols, b = pl.ds(cuts[k], cuts[k + 1] - cuts[k]), e % 2
            return [
                pltpu.make_async_copy(w1_hbm.at[e, :, cols], w1s[k].at[b], wsem.at[b, 2 * k]),
                pltpu.make_async_copy(w3_hbm.at[e, :, cols], w3s[k].at[b], wsem.at[b, 2 * k + 1]),
            ]

        return copies

    def output(k):
        def copies(e):
            cols, b = pl.ds(pl.multiple_of(k * half_d, half_d), half_d), e % 2
            return [pltpu.make_async_copy(w2_hbm.at[e, :, cols], w2s.at[b, k], wsem.at[b, 2 * len(w1s) + k])]

        return copies

    chunks = [columns(k) for k in range(len(w1s))] + [output(k) for k in range(2)]

    def arrive(i, e):
        for c in chunks[i](e):
            c.wait()
        if i == 0:

            @pl.when((e == 0) & (e_loc > 1))
            def _():
                for later in chunks:
                    for c in later(1):
                        c.start()

    def used(i, e):
        @pl.when(e + 2 < e_loc)
        def _():
            for c in chunks[i](e + 2):
                c.start()

    def out_copies(h):
        cols = pl.ds(h * half_d, half_d)
        copies = []
        for i in range(4):
            size = outs[i].shape[0]
            part = pl.ds(0 if i % 2 == 0 else rows - size, size)
            copies.append(pltpu.make_async_copy(acc.at[1 - i // 2, part, cols], outs[i].at[:, cols], osem.at[h, i]))
        return copies

    tokens = [
        pltpu.make_async_copy(ref.at[pl.ds(rows0[i], t)], xbuf.at[i], xsem.at[i]) for i, ref in enumerate((xm_hbm, xo_hbm))
    ]
    for c in tokens:
        c.start()
    for chunk in chunks:
        for c in chunk(0):
            c.start()
    row = 0
    for i, ref in enumerate(init_hbm):
        tokens.append(pltpu.make_async_copy(ref, acc.at[0, pl.ds(row, ref.shape[0])], xsem.at[2 + i]))
        tokens[-1].start()
        row += ref.shape[0]
    for s in range(1 if inits else 0, 2):
        acc[s] = jnp.zeros(acc.shape[1:], F32)
    for c in tokens:
        c.wait()

    def step(e, carry):
        expert = core * e_loc + e
        offs = [table_ref[b, expert] for b in blocks]
        cnts = [table_ref[b, 2 * e_loc + expert] for b in blocks]
        need = functools.reduce(jnp.maximum, [jnp.where(k > 0, o - o // 8 * 8 + k, 0) for o, k in zip(offs, cnts)])

        def last(k):
            @pl.when((e == e_loc - 1) & (k == 0))
            def _():
                for c in out_copies(0):
                    c.start()

        def run(m):
            tiles = (need + m - 1) // m

            def once(i, carry):
                opens, closes = i == 0, i == tiles - 1
                starts = [o // 8 * 8 + i * m for o in offs]
                bases = [pl.multiple_of(jnp.minimum(b, rows - m), 8) for b in starts]
                parts = []
                for s in range(2):
                    row = lax.broadcasted_iota(jnp.int32, (m, t), 0) + bases[s]
                    hit = (row == pos_ref[blocks[s], pl.ds(expert, 1), :]) & (row >= starts[s])
                    parts.append(jnp.dot(hit.astype(F32).astype(BF16), xbuf[s], preferred_element_type=F32))
                xs = jnp.concatenate(parts, axis=0).astype(BF16)
                hs = []
                for c, (wa, wb) in enumerate(zip(w1s, w3s)):
                    pl.when(opens)(functools.partial(arrive, c, e))
                    h1 = jnp.dot(xs, wa[e % 2], preferred_element_type=F32)
                    h3 = jnp.dot(xs, wb[e % 2], preferred_element_type=F32)
                    hs.append((jax.nn.silu(h1) * h3).astype(BF16))
                    pl.when(closes)(functools.partial(used, c, e))
                h = jnp.concatenate(hs, axis=1)

                def project(k, carry):
                    for c in range(2):
                        pl.when(opens & (k == c))(functools.partial(arrive, len(w1s) + c, e))
                    p = jnp.dot(h, w2s[e % 2, k], preferred_element_type=F32)
                    cols = pl.ds(pl.multiple_of(k * half_d, half_d), half_d)
                    for s in range(2):
                        acc[s, pl.ds(bases[s], m), cols] += p[s * m : (s + 1) * m]
                    for c in range(2):
                        pl.when(closes & (k == c))(functools.partial(used, len(w1s) + c, e))
                    pl.when(closes)(functools.partial(last, k))
                    return carry

                return lax.fori_loop(0, 2, project, carry)

            lax.fori_loop(0, tiles, once, 0)

        @pl.when(need == 0)
        def _():
            for i in range(len(chunks)):
                arrive(i, e)
                used(i, e)
            last(0)

        small, large = sizes
        pl.when((need > 0) & (need <= small))(functools.partial(run, small))
        pl.when(need > small)(functools.partial(run, large))
        return carry

    lax.fori_loop(0, e_loc, step, 0)
    for c in out_copies(1):
        c.start()
    for c in out_copies(0) + out_copies(1):
        c.wait()


def _weigh(hit, gate_ref, y, total=None):
    top = len(hit)
    for j in range(top):
        part = jnp.dot(hit[j], y, preferred_element_type=F32) * gate_ref[:, top + j : top + j + 1]
        total = part if total is None else total + part
    return total


def _combine_kernel(hit_ref, gate_ref, k0_ref, k1_ref, o0_ref, o1_ref, f0_ref, total_ref, sum_ref):
    most = f0_ref.shape[0]
    y = (k0_ref[...] + o0_ref[...] + f0_ref[...]).astype(BF16)
    total_ref[...] = _weigh([hit_ref[j, :, :most] for j in range(hit_ref.shape[0])], gate_ref, y)
    sum_ref[...] = k1_ref[...] + o1_ref[...]


def _close_kernel(hit_ref, gate_ref, total_ref, sum_ref, f1_ref, out_ref):
    most = hit_ref.shape[2] - f1_ref.shape[0]
    y = (sum_ref[...] + f1_ref[...]).astype(BF16)
    hit = [hit_ref[j, :, most:] for j in range(hit_ref.shape[0])]
    out_ref[...] = _weigh(hit, gate_ref, y, total_ref[...]).astype(out_ref.dtype)


def solution(mesh):
    chips = mesh.shape["tp"]
    vmem = pl.BlockSpec(memory_space=pltpu.VMEM)
    anym = pl.BlockSpec(memory_space=pl.ANY)
    smem = pl.BlockSpec(memory_space=pltpu.SMEM)

    def layer(x, idx, g, cap, w1, w3, w2):
        t_loc, d = x.shape
        top = idx.shape[1]
        e_all = cap.shape[0]
        e_loc, _, ff = w1.shape
        rows = top * t_loc
        cuts = (0, 512, ff)
        widths = [b - a for a, b in zip(cuts, cuts[1:])]
        blocks = 2 * chips

        def swap(a):
            return lax.ppermute(a, "ep", [(0, 1), (1, 0)])

        def shift(a, turns):
            pairs = [(2 * k + i, 2 * (k ^ turns[i]) + i) for k in range(chips) for i in range(2)]
            return lax.ppermute(a, ("tp", "ep"), pairs)

        out, back = (1, 2), (2, 1)
        pieces = 2
        pos, groups, hit, gate, pair, x_near = pl.pallas_call(
            functools.partial(_route_kernel, chips, out),
            out_shape=[
                jax.ShapeDtypeStruct((blocks, e_all, t_loc), jnp.int32),
                jax.ShapeDtypeStruct((blocks, 128), jnp.int32),
                jax.ShapeDtypeStruct((top, t_loc, rows), BF16),
                jax.ShapeDtypeStruct((t_loc, 8), F32),
                jax.ShapeDtypeStruct((2 * t_loc, d), BF16),
                jax.ShapeDtypeStruct((t_loc, d), BF16),
            ],
            in_specs=[vmem, vmem, smem, anym],
            out_specs=[vmem] * 4 + [anym] * 2,
            scratch_shapes=[
                pltpu.VMEM((blocks, top, t_loc), jnp.int32),
                pltpu.VMEM((t_loc, d), BF16),
                pltpu.VMEM((t_loc, d), BF16),
                pltpu.SemaphoreType.DMA((blocks,)),
                pltpu.SemaphoreType.DMA((blocks,)),
                pltpu.SemaphoreType.DMA((2, pieces)),
                pltpu.SemaphoreType.DMA((2, pieces)),
                pltpu.SemaphoreType.DMA((2 + pieces,)),
            ],
            compiler_params=pltpu.CompilerParams(collective_id=0, has_side_effects=True, vmem_limit_bytes=VMEM_BYTES),
            name="route",
        )(idx.T, g.T, cap, x)

        sizes = (64, 152)

        def stage(turns, mine, other, split, rows0=(0, 0), init=()):
            return pl.pallas_call(
                functools.partial(_expert_kernel, turns, rows0, sizes, cuts, len(init)),
                out_shape=[jax.ShapeDtypeStruct((n, d), F32) for n in split * 2],
                in_specs=[smem, vmem] + [anym] * (5 + len(init)),
                out_specs=[anym] * 4,
                scratch_shapes=[
                    pltpu.VMEM((2, rows, d), F32),
                    pltpu.VMEM((2, t_loc, d), BF16),
                    *[pltpu.VMEM((2, d, w), BF16) for w in widths * 2],
                    pltpu.VMEM((2, 2, ff, d // 2), BF16),
                    pltpu.SemaphoreType.DMA((2, 2 * len(widths) + 2)),
                    pltpu.SemaphoreType.DMA((2, 4)),
                    pltpu.SemaphoreType.DMA((2 + len(init),)),
                ],
                compiler_params=pltpu.CompilerParams(vmem_limit_bytes=VMEM_BYTES),
                cost_estimate=pl.CostEstimate(
                    flops=6 * rows * d * ff, bytes_accessed=6 * e_loc * d * ff + 8 * rows * d, transcendentals=0
                ),
            )(groups, pos, mine, other, w1, w3, w2, *init)

        def merge(parts, *more):
            sums = []
            for q in range(2):
                other = swap(parts[q])
                sums.append(functools.reduce(jnp.add, [m[q] for m in more], parts[2 + q] + other))
            return sums

        early, late = (rows // 4, rows - rows // 4), (rows - rows // 4, rows // 4)
        rest = shift(pair, back)
        rest_other = swap(rest)
        own_x = swap(x)
        near = merge(stage(out, pair, x_near, early))
        near = [shift(a, out) for a in near]
        diag = merge(stage((3, 3), rest, rest_other, late))
        via = [shift(a, out) for a in diag]
        far = merge(stage(back, rest, rest_other, late, (t_loc, t_loc)), via)
        far = [shift(a, back) for a in far]
        own = stage((0, 0), x, own_x, late, init=near)
        other = [swap(own[q]) for q in range(2)]

        def by_columns(steps):
            def part(n):
                return pl.BlockSpec((n, d // steps), lambda i: (0, i))

            return dict(grid=(steps,)), part

        grid, part = by_columns(4)
        total, last = pl.pallas_call(
            _combine_kernel,
            out_shape=[jax.ShapeDtypeStruct((t_loc, d), F32), jax.ShapeDtypeStruct((late[1], d), F32)],
            in_specs=[vmem, vmem] + [part(n) for n in late * 2 + late[:1]],
            out_specs=[part(t_loc), part(late[1])],
            compiler_params=pltpu.CompilerParams(vmem_limit_bytes=VMEM_BYTES),
            name="combine",
            **grid,
        )(hit, gate, *own[2:], *other, far[0])
        grid, part = by_columns(2)
        return pl.pallas_call(
            _close_kernel,
            out_shape=jax.ShapeDtypeStruct((t_loc, d), BF16),
            in_specs=[vmem, vmem] + [part(n) for n in (t_loc, late[1], late[1])],
            out_specs=part(t_loc),
            name="close",
            **grid,
        )(hit, gate, total, last, far[1])

    rows = P(("ep", "tp"), None)
    return jax.shard_map(
        layer,
        mesh=mesh,
        in_specs=(rows, rows, rows, P(None), P("ep", None, "tp"), P("ep", None, "tp"), P("ep", "tp", None)),
        out_specs=rows,
        check_vma=False,
    )
```

```python
import functools

import jax
import jax.numpy as jnp
from jax import lax
from jax.experimental import pallas as pl
from jax.experimental.pallas import tpu as pltpu
from jax.sharding import PartitionSpec as P


F32 = jnp.float32
BF16 = jnp.bfloat16
VMEM_BYTES = 67_043_328


def _route_kernel(chips, turns, idx_ref, g_ref, cap_ref, x_ref, *refs):
    pos_ref, table_ref, hit_ref, gate_ref, pair_ref, xo_ref, ids_all, held, landed, send_sem, recv_sem, xsend, xrecv, lsem = refs
    core, me = lax.axis_index("ep"), lax.axis_index("tp")
    blocks, top, t = ids_all.shape
    e_all = pos_ref.shape[1]
    here = core * chips + me
    mesh_id = pl.DeviceIdType.MESH
    peers = [
        (k, {"ep": jnp.bitwise_xor(core, k // chips), "tp": jnp.bitwise_xor(me, k % chips)}) for k in range(1, blocks)
    ]
    load = pltpu.make_async_copy(x_ref, held, lsem.at[0])
    load.start()
    barrier = pltpu.get_barrier_semaphore()
    for _, peer in peers:
        pl.semaphore_signal(barrier, inc=1, device_id=peer, device_id_type=mesh_id)
    pl.semaphore_wait(barrier, blocks - 1)
    copies = [
        pltpu.make_async_remote_copy(
            src_ref=idx_ref,
            dst_ref=ids_all.at[here],
            send_sem=send_sem.at[k],
            recv_sem=recv_sem.at[k],
            device_id=peer,
            device_id_type=mesh_id,
        )
        for k, peer in peers
    ]
    pieces = xsend.shape[1]
    turn = turns[0] + (turns[1] - turns[0]) * core
    piece = x_ref.shape[0] // pieces

    def tokens(hop, i, src, dst, peer):
        part = pl.ds(i * piece, piece)
        return pltpu.make_async_remote_copy(
            src_ref=src.at[part],
            dst_ref=dst.at[part],
            send_sem=xsend.at[hop, i],
            recv_sem=xrecv.at[hop, i],
            device_id=peer,
            device_id_type=mesh_id,
        )

    arrive = [tokens(0, i, held, landed, {"ep": core, "tp": jnp.bitwise_xor(me, turn)}) for i in range(pieces)]
    forward = [tokens(1, i, landed, xo_ref, {"ep": 1 - core, "tp": me}) for i in range(pieces)]
    keep = [
        pltpu.make_async_copy(
            landed.at[pl.ds(i * piece, piece)], pair_ref.at[pl.ds(i * piece, piece)], lsem.at[2 + i]
        )
        for i in range(pieces)
    ]
    own = pltpu.make_async_copy(held, pair_ref.at[pl.ds(t, t)], lsem.at[1])
    load.wait()
    for c in copies:
        c.start()
    for c in arrive:
        c.start()
    own.start()
    ids_all[pl.ds(here, 1)] = idx_ref[...][None]
    before = (
        lax.broadcasted_iota(jnp.int32, (t, t), 0) < lax.broadcasted_iota(jnp.int32, (t, t), 1)
    ).astype(F32).astype(BF16)
    ids = lax.broadcasted_iota(jnp.int32, (e_all, t), 0)
    cap = jnp.zeros((e_all, t), jnp.int32)
    for e in range(e_all):
        cap = jnp.where(ids == e, cap_ref[e], cap)
    sub, lane = (lax.broadcasted_iota(jnp.int32, (e_all, 128), i) for i in range(2))
    for c in copies:
        c.wait()

    for b in range(blocks):
        hit = (ids_all[b, 0:1, :] == ids) | (ids_all[b, 1:2, :] == ids)
        one = hit.astype(F32)
        rank = jnp.dot(one.astype(BF16), before, preferred_element_type=F32).astype(jnp.int32)
        total = jnp.sum(one, axis=1, keepdims=True).astype(jnp.int32)
        count = jnp.minimum(jnp.broadcast_to(total, (e_all, t)), cap)
        first = jnp.zeros_like(count)
        for e in range(e_all - 1):
            first = first + jnp.where(ids > e, jnp.broadcast_to(count[e : e + 1, :], count.shape), 0)
        pair = jnp.where(lane == sub, first[:, :128], 0) + jnp.where(lane == sub + e_all, count[:, :128], 0)
        table_ref[pl.ds(b, 1)] = jnp.sum(pair, axis=0, keepdims=True)
        pos_ref[b] = jnp.where(hit & (rank < cap), first + rank, -1)
    pos = pos_ref[here]
    lines = [
        jnp.max(jnp.where(idx_ref[j : j + 1, :] == ids, pos, -1), axis=0, keepdims=True).astype(F32) for j in range(top)
    ]
    lines += [g_ref[j : j + 1, :] for j in range(top)]
    table = jnp.concatenate(lines + [jnp.zeros((8 - 2 * top, t), F32)], axis=0)
    table = jnp.transpose(table)
    gate_ref[...] = table
    row = lax.broadcasted_iota(jnp.int32, hit_ref.shape[1:], 1)
    for j in range(top):
        hit_ref[j] = (row == table[:, j : j + 1].astype(jnp.int32)).astype(F32).astype(BF16)
    for c, f, k in zip(arrive, forward, keep):
        c.wait_recv()
        f.start()
        k.start()
    for c, f, k in zip(arrive, forward, keep):
        c.wait_send()
        k.wait()
        f.wait()
    own.wait()


def _expert_kernel(
    turns, rows0, sizes, cuts, inits, table_ref, pos_ref, xm_hbm, xo_hbm, w1_hbm, w3_hbm, w2_hbm, *refs
):
    init_hbm, outs = refs[:inits], refs[inits : inits + 4]
    acc, xbuf, *ws, w2s, wsem, osem, xsem = refs[inits + 4 :]
    w1s, w3s = ws[: len(ws) // 2], ws[len(ws) // 2 :]
    e_loc, d, _ = w1_hbm.shape
    _, rows, _ = acc.shape
    t = xbuf.shape[1]
    half_d = d // 2
    core, me = lax.axis_index("ep"), lax.axis_index("tp")
    chips = pos_ref.shape[0] // 2
    blocks = []
    for c in (core, 1 - core):
        turn = jnp.where(c == 0, turns[0], turns[1])
        blocks.append(c * chips + jnp.bitwise_xor(me, turn))

    def columns(k):
        def copies(e):
            cols, b = pl.ds(cuts[k], cuts[k + 1] - cuts[k]), e % 2
            return [
                pltpu.make_async_copy(w1_hbm.at[e, :, cols], w1s[k].at[b], wsem.at[b, 2 * k]),
                pltpu.make_async_copy(w3_hbm.at[e, :, cols], w3s[k].at[b], wsem.at[b, 2 * k + 1]),
            ]

        return copies

    def output(k):
        def copies(e):
            cols, b = pl.ds(pl.multiple_of(k * half_d, half_d), half_d), e % 2
            return [pltpu.make_async_copy(w2_hbm.at[e, :, cols], w2s.at[b, k], wsem.at[b, 2 * len(w1s) + k])]

        return copies

    chunks = [columns(k) for k in range(len(w1s))] + [output(k) for k in range(2)]

    def arrive(i, e):
        for c in chunks[i](e):
            c.wait()
        if i == 0:

            @pl.when(e == 0)
            def _():
                for later in chunks[len(w1s) :]:
                    for c in later(0):
                        c.start()

        if i == 1:

            @pl.when((e == 0) & (e_loc > 1))
            def _():
                for later in chunks:
                    for c in later(1):
                        c.start()

    def used(i, e):
        @pl.when(e + 2 < e_loc)
        def _():
            for c in chunks[i](e + 2):
                c.start()

    def out_copies(h):
        cols = pl.ds(h * half_d, half_d)
        copies = []
        for i in range(4):
            size = outs[i].shape[0]
            part = pl.ds(0 if i % 2 == 0 else rows - size, size)
            copies.append(pltpu.make_async_copy(acc.at[1 - i // 2, part, cols], outs[i].at[:, cols], osem.at[h, i]))
        return copies

    tokens = [
        pltpu.make_async_copy(ref.at[pl.ds(rows0[i], t)], xbuf.at[i], xsem.at[i]) for i, ref in enumerate((xm_hbm, xo_hbm))
    ]
    for c in tokens:
        c.start()
    for c in chunks[0](0):
        c.start()
    row = 0
    for i, ref in enumerate(init_hbm):
        tokens.append(pltpu.make_async_copy(ref, acc.at[0, pl.ds(row, ref.shape[0])], xsem.at[2 + i]))
        tokens[-1].start()
        row += ref.shape[0]
    for s in range(1 if inits else 0, 2):
        acc[s] = jnp.zeros(acc.shape[1:], F32)
    for c in tokens[:2]:
        c.wait()
    for chunk in chunks[1 : len(w1s)]:
        for c in chunk(0):
            c.start()
    for c in tokens[2:]:
        c.wait()

    def step(e, carry):
        expert = core * e_loc + e
        offs = [table_ref[b, expert] for b in blocks]
        cnts = [table_ref[b, 2 * e_loc + expert] for b in blocks]
        need = functools.reduce(jnp.maximum, [jnp.where(k > 0, o - o // 8 * 8 + k, 0) for o, k in zip(offs, cnts)])

        def last(k):
            @pl.when((e == e_loc - 1) & (k == 0))
            def _():
                for c in out_copies(0):
                    c.start()

        def run(m, tiles, skip, opening, closing):
            def once(i, carry):
                opens, closes = opening & (i == 0), closing & (i == tiles - 1)
                starts = [o // 8 * 8 + skip + i * m for o in offs]
                bases = [pl.multiple_of(jnp.minimum(b, rows - m), 8) for b in starts]
                parts = []
                for s in range(2):
                    row = lax.broadcasted_iota(jnp.int32, (m, t), 0) + bases[s]
                    hit = (row == pos_ref[blocks[s], pl.ds(expert, 1), :]) & (row >= starts[s])
                    parts.append(jnp.dot(hit.astype(F32).astype(BF16), xbuf[s], preferred_element_type=F32))
                xs = jnp.concatenate(parts, axis=0).astype(BF16)
                hs = []
                for c, (wa, wb) in enumerate(zip(w1s, w3s)):
                    pl.when(opens)(functools.partial(arrive, c, e))
                    h1 = jnp.dot(xs, wa[e % 2], preferred_element_type=F32)
                    h3 = jnp.dot(xs, wb[e % 2], preferred_element_type=F32)
                    hs.append((jax.nn.silu(h1) * h3).astype(BF16))
                    pl.when(closes)(functools.partial(used, c, e))
                h = jnp.concatenate(hs, axis=1)

                def project(k, carry):
                    for c in range(2):
                        pl.when(opens & (k == c))(functools.partial(arrive, len(w1s) + c, e))
                    p = jnp.dot(h, w2s[e % 2, k], preferred_element_type=F32)
                    cols = pl.ds(pl.multiple_of(k * half_d, half_d), half_d)
                    for s in range(2):
                        acc[s, pl.ds(bases[s], m), cols] += p[s * m : (s + 1) * m]
                    for c in range(2):
                        pl.when(closes & (k == c))(functools.partial(used, len(w1s) + c, e))
                    pl.when(closes)(functools.partial(last, k))
                    return carry

                return lax.fori_loop(0, 2, project, carry)

            lax.fori_loop(0, tiles, once, 0)

        @pl.when(need == 0)
        def _():
            for i in range(len(chunks)):
                arrive(i, e)
                used(i, e)
            last(0)

        small, large = sizes

        @pl.when(need > small)
        def _():
            run(large, 1, 0, need > 0, need <= large)

        @pl.when((need > 0) & ((need <= small) | (need > large)))
        def _():
            skip = jnp.where(need <= small, 0, large)
            run(small, (need - skip + small - 1) // small, skip, need <= small, need > 0)

        return carry

    lax.fori_loop(0, e_loc, step, 0)
    for c in out_copies(1):
        c.start()
    for c in out_copies(0) + out_copies(1):
        c.wait()


def _weigh(hit, gate_ref, y, total=None):
    top = len(hit)
    for j in range(top):
        part = jnp.dot(hit[j], y, preferred_element_type=F32) * gate_ref[:, top + j : top + j + 1]
        total = part if total is None else total + part
    return total


def _combine_kernel(hit_ref, gate_ref, k0_ref, k1_ref, o0_ref, o1_ref, f0_ref, total_ref, sum_ref):
    most = f0_ref.shape[0]
    y = (k0_ref[...] + o0_ref[...] + f0_ref[...]).astype(BF16)
    total_ref[...] = _weigh([hit_ref[j, :, :most] for j in range(hit_ref.shape[0])], gate_ref, y)
    sum_ref[...] = k1_ref[...] + o1_ref[...]


def _close_kernel(hit_ref, gate_ref, total_ref, sum_ref, f1_ref, out_ref):
    y = (sum_ref[...] + f1_ref[...]).astype(BF16)
    hit = [hit_ref[j] for j in range(hit_ref.shape[0])]
    out_ref[...] = _weigh(hit, gate_ref, y, total_ref[...]).astype(out_ref.dtype)


def solution(mesh):
    chips = mesh.shape["tp"]
    vmem = pl.BlockSpec(memory_space=pltpu.VMEM)
    anym = pl.BlockSpec(memory_space=pl.ANY)
    smem = pl.BlockSpec(memory_space=pltpu.SMEM)

    def layer(x, idx, g, cap, w1, w3, w2):
        t_loc, d = x.shape
        top = idx.shape[1]
        e_all = cap.shape[0]
        e_loc, _, ff = w1.shape
        rows = top * t_loc
        cuts = (0, 512, ff)
        widths = [b - a for a, b in zip(cuts, cuts[1:])]
        blocks = 2 * chips

        def swap(a):
            return lax.ppermute(a, "ep", [(0, 1), (1, 0)])

        def shift(a, turns):
            pairs = [(2 * k + i, 2 * (k ^ turns[i]) + i) for k in range(chips) for i in range(2)]
            return lax.ppermute(a, ("tp", "ep"), pairs)

        out, back = (1, 2), (2, 1)
        pieces = 4
        pos, groups, hit, gate, pair, x_near = pl.pallas_call(
            functools.partial(_route_kernel, chips, out),
            out_shape=[
                jax.ShapeDtypeStruct((blocks, e_all, t_loc), jnp.int32),
                jax.ShapeDtypeStruct((blocks, 128), jnp.int32),
                jax.ShapeDtypeStruct((top, t_loc, rows), BF16),
                jax.ShapeDtypeStruct((t_loc, 8), F32),
                jax.ShapeDtypeStruct((2 * t_loc, d), BF16),
                jax.ShapeDtypeStruct((t_loc, d), BF16),
            ],
            in_specs=[vmem, vmem, smem, anym],
            out_specs=[vmem] * 4 + [anym] * 2,
            scratch_shapes=[
                pltpu.VMEM((blocks, top, t_loc), jnp.int32),
                pltpu.VMEM((t_loc, d), BF16),
                pltpu.VMEM((t_loc, d), BF16),
                pltpu.SemaphoreType.DMA((blocks,)),
                pltpu.SemaphoreType.DMA((blocks,)),
                pltpu.SemaphoreType.DMA((2, pieces)),
                pltpu.SemaphoreType.DMA((2, pieces)),
                pltpu.SemaphoreType.DMA((2 + pieces,)),
            ],
            compiler_params=pltpu.CompilerParams(collective_id=0, has_side_effects=True, vmem_limit_bytes=VMEM_BYTES),
            name="route",
        )(idx.T, g.T, cap, x)

        sizes = (64, 152)

        def stage(turns, mine, other, split, rows0=(0, 0), init=()):
            return pl.pallas_call(
                functools.partial(_expert_kernel, turns, rows0, sizes, cuts, len(init)),
                out_shape=[jax.ShapeDtypeStruct((n, d), F32) for n in split * 2],
                in_specs=[smem, vmem] + [anym] * (5 + len(init)),
                out_specs=[anym] * 4,
                scratch_shapes=[
                    pltpu.VMEM((2, rows, d), F32),
                    pltpu.VMEM((2, t_loc, d), BF16),
                    *[pltpu.VMEM((2, d, w), BF16) for w in widths * 2],
                    pltpu.VMEM((2, 2, ff, d // 2), BF16),
                    pltpu.SemaphoreType.DMA((2, 2 * len(widths) + 2)),
                    pltpu.SemaphoreType.DMA((2, 4)),
                    pltpu.SemaphoreType.DMA((2 + len(init),)),
                ],
                compiler_params=pltpu.CompilerParams(vmem_limit_bytes=VMEM_BYTES),
                cost_estimate=pl.CostEstimate(
                    flops=6 * rows * d * ff, bytes_accessed=6 * e_loc * d * ff + 8 * rows * d, transcendentals=0
                ),
            )(groups, pos, mine, other, w1, w3, w2, *init)

        def merge(parts, *more):
            sums = []
            for q in range(2):
                other = swap(parts[q])
                sums.append(functools.reduce(jnp.add, [m[q] for m in more], parts[2 + q] + other))
            return sums

        early, late = (rows // 4, rows - rows // 4), (rows - rows // 4, rows // 4)
        rest = shift(pair, back)
        rest_other = swap(rest)
        own_x = swap(x)
        near = merge(stage(out, pair, x_near, early))
        near = [shift(a, out) for a in near]
        diag = merge(stage((3, 3), rest, rest_other, late))
        via = [shift(a, out) for a in diag]
        far = merge(stage(back, rest, rest_other, late, (t_loc, t_loc)), via)
        far = [shift(a, back) for a in far]
        own = stage((0, 0), x, own_x, late, init=near)
        other = [swap(own[q]) for q in range(2)]

        def by_columns(steps):
            def part(n):
                return pl.BlockSpec((n, d // steps), lambda i: (0, i))

            return dict(grid=(steps,)), part

        grid, part = by_columns(4)
        total, last = pl.pallas_call(
            _combine_kernel,
            out_shape=[jax.ShapeDtypeStruct((t_loc, d), F32), jax.ShapeDtypeStruct((late[1], d), F32)],
            in_specs=[vmem, vmem] + [part(n) for n in late * 2 + late[:1]],
            out_specs=[part(t_loc), part(late[1])],
            compiler_params=pltpu.CompilerParams(vmem_limit_bytes=VMEM_BYTES),
            name="combine",
            **grid,
        )(hit, gate, *own[2:], *other, far[0])
        grid, part = by_columns(2)
        return pl.pallas_call(
            _close_kernel,
            out_shape=jax.ShapeDtypeStruct((t_loc, d), BF16),
            in_specs=[pl.BlockSpec((top, t_loc, late[1]), lambda i: (0, 0, late[0] // late[1])), vmem]
            + [part(n) for n in (t_loc, late[1], late[1])],
            out_specs=part(t_loc),
            name="close",
            **grid,
        )(hit, gate, total, last, far[1])

    rows = P(("ep", "tp"), None)
    return jax.shard_map(
        layer,
        mesh=mesh,
        in_specs=(rows, rows, rows, P(None), P("ep", None, "tp"), P("ep", None, "tp"), P("ep", "tp", None)),
        out_specs=rows,
        check_vma=False,
    )
```

```python
import functools

import jax
import jax.numpy as jnp
from jax import lax
from jax.experimental import pallas as pl
from jax.experimental.pallas import tpu as pltpu
from jax.sharding import PartitionSpec as P


F32 = jnp.float32
BF16 = jnp.bfloat16
VMEM_BYTES = 67_043_328


def _route_kernel(chips, turns, idx_ref, g_ref, cap_ref, x_ref, *refs):
    pos_ref, table_ref, hit_ref, gate_ref, pair_ref, xo_ref, ids_all, held, landed, send_sem, recv_sem, xsend, xrecv, lsem = refs
    core, me = lax.axis_index("ep"), lax.axis_index("tp")
    blocks, top, t = ids_all.shape
    e_all = pos_ref.shape[1]
    here = core * chips + me
    mesh_id = pl.DeviceIdType.MESH
    peers = [
        (k, {"ep": jnp.bitwise_xor(core, k // chips), "tp": jnp.bitwise_xor(me, k % chips)}) for k in range(1, blocks)
    ]
    load = pltpu.make_async_copy(x_ref, held, lsem.at[0])
    load.start()
    barrier = pltpu.get_barrier_semaphore()
    for _, peer in peers:
        pl.semaphore_signal(barrier, inc=1, device_id=peer, device_id_type=mesh_id)
    pl.semaphore_wait(barrier, blocks - 1)
    copies = [
        pltpu.make_async_remote_copy(
            src_ref=idx_ref,
            dst_ref=ids_all.at[here],
            send_sem=send_sem.at[k],
            recv_sem=recv_sem.at[k],
            device_id=peer,
            device_id_type=mesh_id,
        )
        for k, peer in peers
    ]
    pieces = xsend.shape[1]
    turn = turns[0] + (turns[1] - turns[0]) * core
    piece = x_ref.shape[0] // pieces

    def tokens(hop, i, src, dst, peer):
        part = pl.ds(i * piece, piece)
        return pltpu.make_async_remote_copy(
            src_ref=src.at[part],
            dst_ref=dst.at[part],
            send_sem=xsend.at[hop, i],
            recv_sem=xrecv.at[hop, i],
            device_id=peer,
            device_id_type=mesh_id,
        )

    arrive = [tokens(0, i, held, landed, {"ep": core, "tp": jnp.bitwise_xor(me, turn)}) for i in range(pieces)]
    forward = [tokens(1, i, landed, xo_ref, {"ep": 1 - core, "tp": me}) for i in range(pieces)]
    keep = [
        pltpu.make_async_copy(
            landed.at[pl.ds(i * piece, piece)], pair_ref.at[pl.ds(i * piece, piece)], lsem.at[2 + i]
        )
        for i in range(pieces)
    ]
    own = pltpu.make_async_copy(held, pair_ref.at[pl.ds(t, t)], lsem.at[1])
    load.wait()
    for c in copies:
        c.start()
    for c in arrive:
        c.start()
    own.start()
    ids_all[pl.ds(here, 1)] = idx_ref[...][None]
    before = (
        lax.broadcasted_iota(jnp.int32, (t, t), 0) < lax.broadcasted_iota(jnp.int32, (t, t), 1)
    ).astype(F32).astype(BF16)
    ids = lax.broadcasted_iota(jnp.int32, (e_all, t), 0)
    cap = jnp.zeros((e_all, t), jnp.int32)
    for e in range(e_all):
        cap = jnp.where(ids == e, cap_ref[e], cap)
    sub, lane = (lax.broadcasted_iota(jnp.int32, (e_all, 128), i) for i in range(2))
    for c in copies:
        c.wait()

    for b in range(blocks):
        hit = (ids_all[b, 0:1, :] == ids) | (ids_all[b, 1:2, :] == ids)
        one = hit.astype(F32)
        rank = jnp.dot(one.astype(BF16), before, preferred_element_type=F32).astype(jnp.int32)
        total = jnp.sum(one, axis=1, keepdims=True).astype(jnp.int32)
        count = jnp.minimum(jnp.broadcast_to(total, (e_all, t)), cap)
        first = jnp.zeros_like(count)
        for e in range(e_all - 1):
            first = first + jnp.where(ids > e, jnp.broadcast_to(count[e : e + 1, :], count.shape), 0)
        pair = jnp.where(lane == sub, first[:, :128], 0) + jnp.where(lane == sub + e_all, count[:, :128], 0)
        table_ref[pl.ds(b, 1)] = jnp.sum(pair, axis=0, keepdims=True)
        pos_ref[b] = jnp.where(hit & (rank < cap), first + rank, -1)
    pos = pos_ref[here]
    lines = [
        jnp.max(jnp.where(idx_ref[j : j + 1, :] == ids, pos, -1), axis=0, keepdims=True).astype(F32) for j in range(top)
    ]
    lines += [g_ref[j : j + 1, :] for j in range(top)]
    table = jnp.concatenate(lines + [jnp.zeros((8 - 2 * top, t), F32)], axis=0)
    table = jnp.transpose(table)
    gate_ref[...] = table
    row = lax.broadcasted_iota(jnp.int32, hit_ref.shape[1:], 1)
    for j in range(top):
        hit_ref[j] = (row == table[:, j : j + 1].astype(jnp.int32)).astype(F32).astype(BF16)
    for c, f, k in zip(arrive, forward, keep):
        c.wait_recv()
        f.start()
        k.start()
    for c, f, k in zip(arrive, forward, keep):
        c.wait_send()
        k.wait()
        f.wait()
    own.wait()


def _expert_kernel(
    turns, rows0, sizes, cuts, inits, table_ref, pos_ref, xm_hbm, xo_hbm, w1_hbm, w3_hbm, w2_hbm, *refs
):
    init_hbm, outs = refs[:inits], refs[inits : inits + 4]
    acc, xbuf, *ws, w2s, wsem, osem, xsem = refs[inits + 4 :]
    w1s, w3s = ws[: len(ws) // 2], ws[len(ws) // 2 :]
    e_loc, d, _ = w1_hbm.shape
    _, rows, _ = acc.shape
    t = xbuf.shape[1]
    half_d = d // 2
    core, me = lax.axis_index("ep"), lax.axis_index("tp")
    chips = pos_ref.shape[0] // 2
    blocks = []
    for c in (core, 1 - core):
        turn = jnp.where(c == 0, turns[0], turns[1])
        blocks.append(c * chips + jnp.bitwise_xor(me, turn))

    def columns(k):
        def copies(e):
            cols, b = pl.ds(cuts[k], cuts[k + 1] - cuts[k]), e % 2
            return [
                pltpu.make_async_copy(w1_hbm.at[e, :, cols], w1s[k].at[b], wsem.at[b, 2 * k]),
                pltpu.make_async_copy(w3_hbm.at[e, :, cols], w3s[k].at[b], wsem.at[b, 2 * k + 1]),
            ]

        return copies

    def output(k):
        def copies(e):
            cols, b = pl.ds(pl.multiple_of(k * half_d, half_d), half_d), e % 2
            return [pltpu.make_async_copy(w2_hbm.at[e, :, cols], w2s.at[b, k], wsem.at[b, 2 * len(w1s) + k])]

        return copies

    chunks = [columns(k) for k in range(len(w1s))] + [output(k) for k in range(2)]

    def arrive(i, e):
        for c in chunks[i](e):
            c.wait()
        if i == 0:

            @pl.when(e == 0)
            def _():
                for later in chunks[len(w1s) :]:
                    for c in later(0):
                        c.start()

        if i == 1:

            @pl.when((e == 0) & (e_loc > 1))
            def _():
                for later in chunks:
                    for c in later(1):
                        c.start()

    def used(i, e):
        @pl.when(e + 2 < e_loc)
        def _():
            for c in chunks[i](e + 2):
                c.start()

    def out_copies(h):
        cols = pl.ds(h * half_d, half_d)
        copies = []
        for i in range(4):
            size = outs[i].shape[0]
            part = pl.ds(0 if i % 2 == 0 else rows - size, size)
            copies.append(pltpu.make_async_copy(acc.at[1 - i // 2, part, cols], outs[i].at[:, cols], osem.at[h, i]))
        return copies

    tokens = [
        pltpu.make_async_copy(ref.at[pl.ds(rows0[i], t)], xbuf.at[i], xsem.at[i]) for i, ref in enumerate((xm_hbm, xo_hbm))
    ]
    for c in tokens:
        c.start()
    for chunk in chunks[: len(w1s)]:
        for c in chunk(0):
            c.start()
    row = 0
    for i, ref in enumerate(init_hbm):
        tokens.append(pltpu.make_async_copy(ref, acc.at[0, pl.ds(row, ref.shape[0])], xsem.at[2 + i]))
        tokens[-1].start()
        row += ref.shape[0]
    for s in range(1 if inits else 0, 2):
        acc[s] = jnp.zeros(acc.shape[1:], F32)
    for c in tokens:
        c.wait()

    def step(e, carry):
        expert = core * e_loc + e
        offs = [table_ref[b, expert] for b in blocks]
        cnts = [table_ref[b, 2 * e_loc + expert] for b in blocks]
        need = functools.reduce(jnp.maximum, [jnp.where(k > 0, o - o // 8 * 8 + k, 0) for o, k in zip(offs, cnts)])

        def last(k):
            @pl.when((e == e_loc - 1) & (k == 0))
            def _():
                for c in out_copies(0):
                    c.start()

        def run(m, tiles, skip, opening, closing):
            def once(i, carry):
                opens, closes = opening & (i == 0), closing & (i == tiles - 1)
                starts = [o // 8 * 8 + skip + i * m for o in offs]
                bases = [pl.multiple_of(jnp.minimum(b, rows - m), 8) for b in starts]
                parts = []
                for s in range(2):
                    row = lax.broadcasted_iota(jnp.int32, (m, t), 0) + bases[s]
                    hit = (row == pos_ref[blocks[s], pl.ds(expert, 1), :]) & (row >= starts[s])
                    parts.append(jnp.dot(hit.astype(F32).astype(BF16), xbuf[s], preferred_element_type=F32))
                xs = jnp.concatenate(parts, axis=0).astype(BF16)
                hs = []
                for c, (wa, wb) in enumerate(zip(w1s, w3s)):
                    pl.when(opens)(functools.partial(arrive, c, e))
                    h1 = jnp.dot(xs, wa[e % 2], preferred_element_type=F32)
                    h3 = jnp.dot(xs, wb[e % 2], preferred_element_type=F32)
                    hs.append((jax.nn.silu(h1) * h3).astype(BF16))
                    pl.when(closes)(functools.partial(used, c, e))
                h = jnp.concatenate(hs, axis=1)

                def project(k, carry):
                    for c in range(2):
                        pl.when(opens & (k == c))(functools.partial(arrive, len(w1s) + c, e))
                    p = jnp.dot(h, w2s[e % 2, k], preferred_element_type=F32)
                    cols = pl.ds(pl.multiple_of(k * half_d, half_d), half_d)
                    for s in range(2):
                        acc[s, pl.ds(bases[s], m), cols] += p[s * m : (s + 1) * m]
                    for c in range(2):
                        pl.when(closes & (k == c))(functools.partial(used, len(w1s) + c, e))
                    pl.when(closes)(functools.partial(last, k))
                    return carry

                return lax.fori_loop(0, 2, project, carry)

            lax.fori_loop(0, tiles, once, 0)

        @pl.when(need == 0)
        def _():
            for i in range(len(chunks)):
                arrive(i, e)
                used(i, e)
            last(0)

        small, large = sizes

        @pl.when(need > small)
        def _():
            run(large, 1, 0, need > 0, need <= large)

        @pl.when((need > 0) & ((need <= small) | (need > large)))
        def _():
            skip = jnp.where(need <= small, 0, large)
            run(small, (need - skip + small - 1) // small, skip, need <= small, need > 0)

        return carry

    lax.fori_loop(0, e_loc, step, 0)
    for c in out_copies(1):
        c.start()
    for c in out_copies(0) + out_copies(1):
        c.wait()


def _weigh(hit, gate_ref, y, total=None):
    top = len(hit)
    for j in range(top):
        part = jnp.dot(hit[j], y, preferred_element_type=F32) * gate_ref[:, top + j : top + j + 1]
        total = part if total is None else total + part
    return total


def _combine_kernel(hit_ref, gate_ref, k0_ref, k1_ref, o0_ref, o1_ref, f0_ref, total_ref, sum_ref):
    most = f0_ref.shape[0]
    y = (k0_ref[...] + o0_ref[...] + f0_ref[...]).astype(BF16)
    total_ref[...] = _weigh([hit_ref[j, :, :most] for j in range(hit_ref.shape[0])], gate_ref, y)
    sum_ref[...] = k1_ref[...] + o1_ref[...]


def _close_kernel(hit_ref, gate_ref, total_ref, sum_ref, f1_ref, out_ref):
    most = hit_ref.shape[2] - f1_ref.shape[0]
    y = (sum_ref[...] + f1_ref[...]).astype(BF16)
    hit = [hit_ref[j, :, most:] for j in range(hit_ref.shape[0])]
    out_ref[...] = _weigh(hit, gate_ref, y, total_ref[...]).astype(out_ref.dtype)


def solution(mesh):
    chips = mesh.shape["tp"]
    vmem = pl.BlockSpec(memory_space=pltpu.VMEM)
    anym = pl.BlockSpec(memory_space=pl.ANY)
    smem = pl.BlockSpec(memory_space=pltpu.SMEM)

    def layer(x, idx, g, cap, w1, w3, w2):
        t_loc, d = x.shape
        top = idx.shape[1]
        e_all = cap.shape[0]
        e_loc, _, ff = w1.shape
        rows = top * t_loc
        cuts = (0, 512, ff)
        widths = [b - a for a, b in zip(cuts, cuts[1:])]
        blocks = 2 * chips

        def swap(a):
            return lax.ppermute(a, "ep", [(0, 1), (1, 0)])

        def shift(a, turns):
            pairs = [(2 * k + i, 2 * (k ^ turns[i]) + i) for k in range(chips) for i in range(2)]
            return lax.ppermute(a, ("tp", "ep"), pairs)

        out, back = (1, 2), (2, 1)
        pieces = 4
        pos, groups, hit, gate, pair, x_near = pl.pallas_call(
            functools.partial(_route_kernel, chips, out),
            out_shape=[
                jax.ShapeDtypeStruct((blocks, e_all, t_loc), jnp.int32),
                jax.ShapeDtypeStruct((blocks, 128), jnp.int32),
                jax.ShapeDtypeStruct((top, t_loc, rows), BF16),
                jax.ShapeDtypeStruct((t_loc, 8), F32),
                jax.ShapeDtypeStruct((2 * t_loc, d), BF16),
                jax.ShapeDtypeStruct((t_loc, d), BF16),
            ],
            in_specs=[vmem, vmem, smem, anym],
            out_specs=[vmem] * 4 + [anym] * 2,
            scratch_shapes=[
                pltpu.VMEM((blocks, top, t_loc), jnp.int32),
                pltpu.VMEM((t_loc, d), BF16),
                pltpu.VMEM((t_loc, d), BF16),
                pltpu.SemaphoreType.DMA((blocks,)),
                pltpu.SemaphoreType.DMA((blocks,)),
                pltpu.SemaphoreType.DMA((2, pieces)),
                pltpu.SemaphoreType.DMA((2, pieces)),
                pltpu.SemaphoreType.DMA((2 + pieces,)),
            ],
            compiler_params=pltpu.CompilerParams(collective_id=0, has_side_effects=True, vmem_limit_bytes=VMEM_BYTES),
            name="route",
        )(idx.T, g.T, cap, x)

        sizes = (64, 160)

        def stage(turns, mine, other, split, rows0=(0, 0), init=()):
            return pl.pallas_call(
                functools.partial(_expert_kernel, turns, rows0, sizes, cuts, len(init)),
                out_shape=[jax.ShapeDtypeStruct((n, d), F32) for n in split * 2],
                in_specs=[smem, vmem] + [anym] * (5 + len(init)),
                out_specs=[anym] * 4,
                scratch_shapes=[
                    pltpu.VMEM((2, rows, d), F32),
                    pltpu.VMEM((2, t_loc, d), BF16),
                    *[pltpu.VMEM((2, d, w), BF16) for w in widths * 2],
                    pltpu.VMEM((2, 2, ff, d // 2), BF16),
                    pltpu.SemaphoreType.DMA((2, 2 * len(widths) + 2)),
                    pltpu.SemaphoreType.DMA((2, 4)),
                    pltpu.SemaphoreType.DMA((2 + len(init),)),
                ],
                compiler_params=pltpu.CompilerParams(vmem_limit_bytes=VMEM_BYTES),
                cost_estimate=pl.CostEstimate(
                    flops=6 * rows * d * ff, bytes_accessed=6 * e_loc * d * ff + 8 * rows * d, transcendentals=0
                ),
            )(groups, pos, mine, other, w1, w3, w2, *init)

        def merge(parts, *more):
            sums = []
            for q in range(2):
                other = swap(parts[q])
                sums.append(functools.reduce(jnp.add, [m[q] for m in more], parts[2 + q] + other))
            return sums

        early, late = (rows // 4, rows - rows // 4), (rows - rows // 4, rows // 4)
        rest = shift(pair, back)
        rest_other = swap(rest)
        own_x = swap(x)
        near = merge(stage(out, pair, x_near, early))
        near = [shift(a, out) for a in near]
        diag = merge(stage((3, 3), rest, rest_other, late))
        via = [shift(a, out) for a in diag]
        far = merge(stage(back, rest, rest_other, late, (t_loc, t_loc)), via)
        far = [shift(a, back) for a in far]
        own = stage((0, 0), x, own_x, late, init=near)
        other = [swap(own[q]) for q in range(2)]

        def by_columns(steps):
            def part(n):
                return pl.BlockSpec((n, d // steps), lambda i: (0, i))

            return dict(grid=(steps,)), part

        grid, part = by_columns(4)
        total, last = pl.pallas_call(
            _combine_kernel,
            out_shape=[jax.ShapeDtypeStruct((t_loc, d), F32), jax.ShapeDtypeStruct((late[1], d), F32)],
            in_specs=[vmem, vmem] + [part(n) for n in late * 2 + late[:1]],
            out_specs=[part(t_loc), part(late[1])],
            compiler_params=pltpu.CompilerParams(vmem_limit_bytes=VMEM_BYTES),
            name="combine",
            **grid,
        )(hit, gate, *own[2:], *other, far[0])
        grid, part = by_columns(2)
        return pl.pallas_call(
            _close_kernel,
            out_shape=jax.ShapeDtypeStruct((t_loc, d), BF16),
            in_specs=[vmem, vmem] + [part(n) for n in (t_loc, late[1], late[1])],
            out_specs=part(t_loc),
            name="close",
            **grid,
        )(hit, gate, total, last, far[1])

    rows = P(("ep", "tp"), None)
    return jax.shard_map(
        layer,
        mesh=mesh,
        in_specs=(rows, rows, rows, P(None), P("ep", None, "tp"), P("ep", None, "tp"), P("ep", "tp", None)),
        out_specs=rows,
        check_vma=False,
    )
```
